8 devices in a mesh: dom: 2 (over z, y), ens: 4 (over x, core).
Axes of the slice: x: 2, y: 2, z: 1, core: 2. Of those that a mesh axis runs over, the one named last changes fastest.
Arguments:
- ens_state: bfloat16 [64, 128, 32, 227], P('ens', None, 'dom')
- w_in: bfloat16 [454, 512], replicated
- w_out: bfloat16 [512, 227], replicated
- obs_op: bfloat16 [227, 32], replicated
- obs_val: float32 [32, 4, 2, 16, 32], P(None, None, 'dom')
- obs_wt: float32 [32, 4, 2, 16, 32], P(None, None, 'dom')
Outputs:
- output: bfloat16 [128, 32, 64, 227], P('ens', 'dom')
All inputs are finite; a program needn't handle non-finite values.
Results may differ from the reference program's by a relative error of at most 0.001.
Values are sent between devices in bfloat16 or wider.
A program may use at most 1 GiB of HBM per device.

```python
import jax
import jax.numpy as jnp
from jax import lax

E = 64
NY = 128
NX = 32
C = 227
F = 512
O = 32
BR = 4
BC = 16
NS_STEPS = 18


def setup_inputs(seed: int = 0) -> dict:
    keys = jax.random.split(jax.random.key(seed), 7)
    mean_field = jax.random.normal(keys[0], (NY, NX, C), jnp.float32)
    perturb = 0.3 * jax.random.normal(keys[1], (E, NY, NX, C), jnp.float32)
    ens_state = (mean_field[None] + perturb).astype(jnp.bfloat16)
    row_scale = jnp.concatenate([jnp.full((C, 1), (2.0 * C) ** -0.5, jnp.float32), jnp.full((C, 1), 0.25 * C ** -0.5, jnp.float32)], axis=0)
    w_in = (row_scale * jax.random.normal(keys[2], (2 * C, F), jnp.float32)).astype(jnp.bfloat16)
    w_out = (0.5 * F ** -0.5 * jax.random.normal(keys[3], (F, C), jnp.float32)).astype(jnp.bfloat16)
    obs_op = (C ** -0.5 * jax.random.normal(keys[4], (C, O), jnp.float32)).astype(jnp.bfloat16)
    obs_grid = jnp.einsum("ijc,co->ijo", mean_field, obs_op.astype(jnp.float32)) + 0.4 * jax.random.normal(keys[5], (NY, NX, O), jnp.float32)
    obs_val = obs_grid.reshape(NY // BR, BR, NX // BC, BC, O)
    wt_scale = E / (0.16 * BR * BC * O)
    obs_wt = wt_scale * jax.random.uniform(keys[6], (NY // BR, BR, NX // BC, BC, O), jnp.float32, 0.25, 1.75)
    return {"ens_state": ens_state, "w_in": w_in, "w_out": w_out, "obs_op": obs_op, "obs_val": obs_val, "obs_wt": obs_wt}


def reference(ens_state, w_in, w_out, obs_op, obs_val, obs_wt):
    def member_forecast(member):
        member_f32 = member.astype(jnp.float32)
        north_val = jnp.concatenate([member_f32[:1], member_f32[:-1]], axis=0)
        south_val = jnp.concatenate([member_f32[1:], member_f32[-1:]], axis=0)
        west_val = jnp.roll(member_f32, 1, axis=1)
        east_val = jnp.roll(member_f32, -1, axis=1)
        lap_field = (north_val + south_val + west_val + east_val - 4.0 * member_f32).astype(jnp.bfloat16)
        joined = jnp.concatenate([member, lap_field], axis=-1)

        def row_forecast(grid_row):
            hidden = jnp.dot(grid_row, w_in, preferred_element_type=jnp.float32)
            gelu_out = jax.nn.gelu(hidden, approximate=True).astype(jnp.bfloat16)
            increment = jnp.dot(gelu_out, w_out, preferred_element_type=jnp.float32)
            return (grid_row[:, :C].astype(jnp.float32) + increment).astype(jnp.bfloat16)

        return lax.map(row_forecast, joined)

    forecast = lax.map(member_forecast, ens_state)
    patch_rows = NY // BR
    patch_cols = NX // BC
    patches = forecast.reshape(E, patch_rows, BR, patch_cols, BC, C).transpose(1, 3, 0, 2, 4, 5).reshape(patch_rows * patch_cols, E, BR * BC, C)
    obs_patches = obs_val.transpose(0, 2, 1, 3, 4).reshape(patch_rows * patch_cols, BR * BC * O)
    wt_patches = obs_wt.transpose(0, 2, 1, 3, 4).reshape(patch_rows * patch_cols, BR * BC * O)
    identity = jnp.eye(E, dtype=jnp.float32)
    op_f32 = obs_op.astype(jnp.float32)

    def patch_analysis(operands):
        patch_fc, patch_obs, patch_wt = operands
        fc_f32 = patch_fc.astype(jnp.float32)
        mean_fc = jnp.mean(fc_f32, axis=0)
        anomaly = fc_f32 - mean_fc
        obs_fc = jnp.einsum("kbc,co->kbo", fc_f32, op_f32).reshape(E, BR * BC * O)
        obs_mean = jnp.mean(obs_fc, axis=0)
        obs_anom = obs_fc - obs_mean
        weighted = obs_anom * patch_wt
        a_mat = (E - 1.0) * identity + jnp.dot(weighted, obs_anom.T)
        a_trace = jnp.trace(a_mat)

        def newton_step(step_idx, carry):
            sqrt_est, inv_est = carry
            mixer = 1.5 * identity - 0.5 * jnp.dot(inv_est, sqrt_est)
            return jnp.dot(sqrt_est, mixer), jnp.dot(mixer, inv_est)

        sqrt_est, inv_est = lax.fori_loop(0, NS_STEPS, newton_step, (a_mat / a_trace, identity))
        inv_root = inv_est / jnp.sqrt(a_trace)
        post_cov = jnp.dot(inv_root, inv_root)
        w_mean = jnp.dot(post_cov, jnp.dot(weighted, patch_obs - obs_mean))
        transform = jnp.sqrt(E - 1.0) * inv_root + w_mean[:, None]
        return (mean_fc + jnp.einsum("kbc,ke->ebc", anomaly, transform)).astype(jnp.bfloat16)

    result = lax.map(patch_analysis, (patches, obs_patches, wt_patches))
    return result.reshape(patch_rows, patch_cols, E, BR, BC, C).transpose(0, 3, 1, 4, 2, 5).reshape(NY, NX, E, C)
```

```python
import functools
import math
import jax
import jax.numpy as jnp
from jax import lax
from jax.experimental import pallas as pl
from jax.experimental.pallas import tpu as pltpu
from jax.sharding import PartitionSpec as P

NS_STEPS = 18
MESH = pl.DeviceIdType.MESH
CP = 256
NT = (((1,), (1,)), ((), ()))


NN = (((1,), (0,)), ((), ()))


def split3(a):
    hi = a.astype(jnp.bfloat16)
    rem = a - hi.astype(jnp.float32)
    mid = rem.astype(jnp.bfloat16)
    low = (rem - mid.astype(jnp.float32)).astype(jnp.bfloat16)
    return hi, mid, low


def f32dot(a, b, dims=NN):
    ah, am, al = split3(a)
    bh, bm, bl = split3(b)
    n = a.shape[0]

    def dot(u, v):
        return lax.dot_general(u, v, dims, preferred_element_type=jnp.float32)
    by_hi = dot(jnp.concatenate([ah, am, al], axis=0), bh)
    by_mid = dot(jnp.concatenate([ah, am], axis=0), bm)
    by_low = dot(ah, bl)
    small = (by_low + by_hi[2 * n:]) + by_mid[n:]
    return (small + (by_mid[:n] + by_hi[n:2 * n])) + by_hi[:n]


def exchange_kernel(dims, x_hbm, wi_ref, wo_ref, op_ref, yo_ref, wt_ref, g_hbm, tt_ref,
                    xv, xs, xl, ts, sb, gath, gsend, grecv, wobs, yp, cm,
                    xsem, gssem, grsem, ssem, rsem, gsem):
    members, rows, columns, channels, patches, dev_rows, ens_size = dims
    rest = channels - 128
    units = patches * ens_size
    total_m = members * ens_size
    me = lax.axis_index("ens")
    mydom = lax.axis_index("dom")
    my_x, my_core = me // 2, me % 2

    def dest_of(dslot):
        dx = (my_x + 1 - dslot // 2) % 2
        dc = (my_core + (dslot + 1) // 2) % 2
        return dx * 2 + dc

    barrier = pltpu.get_barrier_semaphore()
    for dslot in range(3):
        pl.semaphore_signal(barrier, inc=1, device_id={"ens": dest_of(dslot)}, device_id_type=MESH)
    pl.semaphore_signal(barrier, inc=1, device_id={"dom": 1 - mydom}, device_id_type=MESH)
    pl.semaphore_wait(barrier, 4)

    def x_copies(unit, action):
        patch, dslot = unit // ens_size, unit % ens_size
        slot = unit % 2
        first = dest_of(dslot) * dev_rows + patch * 4
        north = jnp.maximum(first - 1, 0)
        south = jnp.minimum(first + 4, rows - 1)
        for idx, (src, num, dst) in enumerate(((first, 4, 1), (north, 1, 0), (south, 1, 5))):
            copy = pltpu.make_async_copy(x_hbm.at[:, pl.ds(src, num)], xv.at[slot, :, pl.ds(dst, num)], xsem.at[slot, idx])
            action(copy)

    def ghost_copy(unit):
        return pltpu.make_async_remote_copy(
            src_ref=gsend.at[unit], dst_ref=grecv.at[unit], send_sem=gssem.at[unit], recv_sem=grsem.at[unit],
            device_id={"dom": 1 - mydom}, device_id_type=MESH)

    def unit_copy(patch, dslot):
        return pltpu.make_async_remote_copy(
            src_ref=sb.at[patch * 3 + dslot], dst_ref=gath.at[patch, :, :, pl.ds(me * members, members)],
            send_sem=ssem.at[patch, dslot], recv_sem=rsem.at[patch, dslot],
            device_id={"ens": dest_of(dslot)}, device_id_type=MESH)

    def gath_copy(patch):
        return pltpu.make_async_copy(gath.at[patch], g_hbm.at[patch], gsem.at[patch])

    x_copies(0, lambda c: c.start())

    xs[...] = jnp.zeros_like(xs)
    wobs[...] = jnp.zeros_like(wobs)
    for j in range(8):
        place = (lax.broadcasted_iota(jnp.int32, (32, CP), 1) == lax.broadcasted_iota(jnp.int32, (32, CP), 0) + 32 * j)
        wobs[j * CP:(j + 1) * CP, :] = jnp.dot(op_ref[...], place.astype(jnp.bfloat16), preferred_element_type=jnp.float32).astype(jnp.bfloat16)

    def prepare(unit):
        slot = unit % 2

        @pl.when(unit + 1 < units)
        def _():
            x_copies(unit + 1, lambda c: c.start())
        x_copies(unit, lambda c: c.wait())

        def convert(r, carry):
            for m in range(members):
                v = xv[slot, m, r]
                xs[slot, 0, r, 32 * m + 8:32 * m + 24, :] = v[:, :128].astype(jnp.float32)
                xs[slot, 1, r, 32 * m + 8:32 * m + 24, 0:rest] = v[:, 128:].astype(jnp.float32)
            return carry
        lax.fori_loop(0, 6, convert, 0)

        def edges(r, carry):
            for h in range(2):
                gsend[unit, 0, r, :, h * 128:h * 128 + 128] = xs[slot, h, r + 1, pl.ds(23, members, stride=32), :].astype(jnp.bfloat16)
                gsend[unit, 1, r, :, h * 128:h * 128 + 128] = xs[slot, h, r + 1, pl.ds(8, members, stride=32), :].astype(jnp.bfloat16)
            return carry
        lax.fori_loop(0, 4, edges, 0)
        ghost_copy(unit).start()

    def forecast(unit):
        patch, dslot = unit // ens_size, unit % ens_size
        slot = unit % 2
        out_slot = jnp.where(dslot < 3, patch * 3 + dslot, patches * 3)
        ghost_copy(unit).wait_recv()

        def block(r, carry):
            for h in range(2):
                xs[slot, h, r + 1, pl.ds(7, members, stride=32), :] = grecv[unit, 0, r, :, h * 128:h * 128 + 128].astype(jnp.float32)
                xs[slot, h, r + 1, pl.ds(24, members, stride=32), :] = grecv[unit, 1, r, :, h * 128:h * 128 + 128].astype(jnp.float32)
            for m in range(members):
                b = 32 * m
                for h in range(2):
                    cur = xs[slot, h, r + 1, b + 8:b + 24, :]
                    north = xs[slot, h, r, b + 8:b + 24, :]
                    south = xs[slot, h, r + 2, b + 8:b + 24, :]
                    west = xs[slot, h, r + 1, b + 7:b + 23, :]
                    east = xs[slot, h, r + 1, b + 9:b + 25, :]
                    lap = north + south + west + east - 4.0 * cur
                    xl[16 * m:16 * m + 16, h * 128:h * 128 + 128] = cur.astype(jnp.bfloat16)
                    xl[16 * m:16 * m + 16, CP + h * 128:CP + h * 128 + 128] = lap.astype(jnp.bfloat16)
            hidden = jnp.dot(xl[...], wi_ref[...], preferred_element_type=jnp.float32)
            gel = jax.nn.gelu(hidden, approximate=True).astype(jnp.bfloat16)
            inc = jnp.dot(gel, wo_ref[...], preferred_element_type=jnp.float32)
            for m in range(members):
                for h in range(2):
                    ts[h, 16 * m:16 * m + 16, :] = xs[slot, h, r + 1, 32 * m + 8:32 * m + 24, :] + inc[16 * m:16 * m + 16, h * 128:h * 128 + 128]
            for col in range(columns):
                for h in range(2):
                    sb[out_slot, r, col, :, h * 128:h * 128 + 128] = ts[h, pl.ds(col, members, stride=16), :].astype(jnp.bfloat16)
            return carry
        lax.fori_loop(0, 4, block, 0)

        @pl.when(dslot < 3)
        def _():
            unit_copy(patch, dslot).start()

        @pl.when(dslot == 3)
        def _():
            def own(r, carry):
                gath[patch, r, :, pl.ds(pl.multiple_of(me * members, members), members), :] = sb[patches * 3, r]
                return carry
            lax.fori_loop(0, 4, own, 0)

    def analysis(patch):
        for dslot in range(3):
            unit_copy(patch, dslot).wait_recv()
        gath_copy(patch).start()
        eye = (lax.broadcasted_iota(jnp.int32, (total_m, total_m), 0) == lax.broadcasted_iota(jnp.int32, (total_m, total_m), 1)).astype(jnp.float32)
        csum = jnp.zeros((total_m, CP), jnp.float32)
        for half in range(2):
            lhs = jnp.concatenate([gath[patch, :, half * 8 + j].reshape(4 * total_m, CP) for j in range(8)], axis=1)
            yb = jnp.dot(lhs, wobs[...], preferred_element_type=jnp.float32)
            for r in range(4):
                g = half * 4 + r
                y = yb[r * total_m:(r + 1) * total_m]
                ybar = jnp.sum(y, axis=0, keepdims=True) * (1.0 / total_m)
                y = y - ybar
                c = y * wt_ref[patch, g:g + 1, :]
                csum = csum + c * (yo_ref[patch, g:g + 1, :] - ybar)
                yp[g] = y
                cm[g] = c
        a_mat = (total_m - 1.0) * eye
        for g in range(8):
            a_mat = a_mat + f32dot(cm[g], yp[g], NT)
        trace = jnp.sum(jnp.sum(a_mat * eye, axis=0, keepdims=True), axis=1, keepdims=True)

        def newton(step, carry):
            y, z = carry
            mix = 1.5 * eye - 0.5 * f32dot(z, y)
            return f32dot(y, mix), f32dot(mix, z)
        _, inv = lax.fori_loop(0, NS_STEPS, newton, (a_mat / trace, eye))
        root = inv / jnp.sqrt(trace)
        rhs = jnp.broadcast_to(jnp.sum(csum, axis=1, keepdims=True), (total_m, total_m))
        wbar = f32dot(root, f32dot(root, rhs))
        trans = math.sqrt(total_m - 1.0) * root + wbar
        trans = trans + (1.0 - jnp.sum(trans, axis=0, keepdims=True)) * (1.0 / total_m)
        tt_ref[patch] = trans.T

    def step(v, carry):
        @pl.when(v < units)
        def _():
            prepare(v)

        @pl.when((v >= 1) & (v <= units))
        def _():
            forecast(v - 1)

        @pl.when((v >= 12) & (v % 4 == 0))
        def _():
            analysis(v // 4 - 3)
        return carry
    lax.fori_loop(0, units + 9, step, 0)

    def finish(patch, carry):
        for dslot in range(3):
            unit_copy(patch, dslot).wait_send()
        for dslot in range(4):
            ghost_copy(patch * 4 + dslot).wait_send()
        gath_copy(patch).wait()
        return carry
    lax.fori_loop(0, patches, finish, 0)


def update_kernel(tt_ref, g_ref, out_ref):
    t = tt_ref[0]
    hi = t.astype(jnp.bfloat16)
    r1 = t - hi.astype(jnp.float32)
    mid = r1.astype(jnp.bfloat16)
    low = (r1 - mid.astype(jnp.float32)).astype(jnp.bfloat16)
    lhs = jnp.concatenate([hi, mid, low], axis=0)
    n = t.shape[0]
    for col in range(g_ref.shape[2]):
        res = jnp.dot(lhs, g_ref[0, 0, col], preferred_element_type=jnp.float32)
        val = (res[2 * n:] + res[n:2 * n]) + res[:n]
        out_ref[0, col] = val[:, :out_ref.shape[3]].astype(jnp.bfloat16)


def solution(mesh):
    ens_size = mesh.shape["ens"]
    obs_spec = P(None, None, "dom", None, None)

    def local_step(ens_state, w_in, w_out, obs_op, obs_val, obs_wt):
        members, rows, columns, channels = ens_state.shape
        hidden = w_in.shape[1]
        total_m = members * ens_size
        dev_rows = rows // ens_size
        patches = dev_rows // 4
        units = patches * ens_size
        obs = obs_op.shape[1]
        pad = ((0, CP - channels), (0, 0))
        wi = jnp.concatenate([jnp.pad(w_in[:channels], pad), jnp.pad(w_in[channels:], pad)], axis=0)
        wo = jnp.pad(w_out, ((0, 0), (0, CP - channels)))
        op = jnp.pad(obs_op, pad)
        start = lax.axis_index("ens") * patches

        def arrange(v):
            v = lax.dynamic_slice_in_dim(v, start, patches, axis=0)
            v = v.reshape(patches, 4, 2, 8 * obs).transpose(0, 2, 1, 3)
            return v.reshape(patches, 8, 8 * obs)
        yo, wt = arrange(obs_val), arrange(obs_wt)
        dims = (members, rows, columns, channels, patches, dev_rows, ens_size)
        vmem = pl.BlockSpec(memory_space=pltpu.VMEM)
        anym = pl.BlockSpec(memory_space=pl.ANY)
        bf, f32 = jnp.bfloat16, jnp.float32
        dma = pltpu.SemaphoreType.DMA
        gathered, trans = pl.pallas_call(
            functools.partial(exchange_kernel, dims),
            out_shape=(jax.ShapeDtypeStruct((patches, 4, columns, total_m, CP), bf),
                       jax.ShapeDtypeStruct((patches, total_m, total_m), f32)),
            in_specs=[anym, vmem, vmem, vmem, vmem, vmem],
            out_specs=(anym, vmem),
            scratch_shapes=[
                pltpu.VMEM((2, members, 6, columns, channels), bf),
                pltpu.VMEM((2, 2, 6, members * 32, 128), f32),
                pltpu.VMEM((members * columns, 2 * CP), bf),
                pltpu.VMEM((2, members * columns, 128), f32),
                pltpu.VMEM((patches * 3 + 1, 4, columns, members, CP), bf),
                pltpu.VMEM((patches, 4, columns, total_m, CP), bf),
                pltpu.VMEM((units, 2, 4, members, CP), bf),
                pltpu.VMEM((units, 2, 4, members, CP), bf),
                pltpu.VMEM((8 * CP, CP), bf),
                pltpu.VMEM((8, total_m, CP), f32),
                pltpu.VMEM((8, total_m, CP), f32),
                dma((2, 3)), dma((units,)), dma((units,)), dma((patches, 3)), dma((patches, 3)), dma((patches,)),
            ],
            compiler_params=pltpu.CompilerParams(collective_id=0, has_side_effects=True, vmem_limit_bytes=62 * 1024 * 1024),
        )(ens_state, wi, wo, op, yo, wt)
        return pl.pallas_call(
            update_kernel,
            grid=(patches, 4),
            out_shape=jax.ShapeDtypeStruct((dev_rows, columns, total_m, channels), bf),
            in_specs=[pl.BlockSpec((1, total_m, total_m), lambda p, r: (p, 0, 0)),
                      pl.BlockSpec((1, 1, columns, total_m, CP), lambda p, r: (p, r, 0, 0, 0))],
            out_specs=pl.BlockSpec((1, columns, total_m, channels), lambda p, r: (p * 4 + r, 0, 0, 0)),
            compiler_params=pltpu.CompilerParams(dimension_semantics=("arbitrary", "arbitrary")),
        )(trans, gathered)

    return jax.shard_map(local_step, mesh=mesh, in_specs=(P("ens", None, "dom", None), P(), P(), P(), obs_spec, obs_spec), out_specs=P("ens", "dom", None, None), check_vma=False)
```

```python
import functools
import math
import jax
import jax.numpy as jnp
from jax import lax
from jax.experimental import pallas as pl
from jax.experimental.pallas import tpu as pltpu
from jax.sharding import PartitionSpec as P

NS_STEPS = 18
MESH = pl.DeviceIdType.MESH
CP = 256
NT = (((1,), (1,)), ((), ()))


NN = (((1,), (0,)), ((), ()))


def split3(a):
    hi = a.astype(jnp.bfloat16)
    rem = a - hi.astype(jnp.float32)
    mid = rem.astype(jnp.bfloat16)
    low = (rem - mid.astype(jnp.float32)).astype(jnp.bfloat16)
    return hi, mid, low


def f32dot(a, b, dims=NN):
    ah, am, al = split3(a)
    bh, bm, bl = split3(b)
    n = a.shape[0]

    def dot(u, v):
        return lax.dot_general(u, v, dims, preferred_element_type=jnp.float32)
    by_hi = dot(jnp.concatenate([ah, am, al], axis=0), bh)
    by_mid = dot(jnp.concatenate([ah, am], axis=0), bm)
    by_low = dot(ah, bl)
    small = (by_low + by_hi[2 * n:]) + by_mid[n:]
    return (small + (by_mid[:n] + by_hi[n:2 * n])) + by_hi[:n]


def exchange_kernel(dims, x_hbm, wi_ref, wo_ref, op_ref, yo_hbm, wt_hbm, g_hbm, tt_ref,
                    xv, xs, xl, ts, t2, sb1, sb2, rb, gath, gsend, grecv, wi, wo, wf, wobs, obs_raw, obs_row, yp, cm,
                    xsem, gssem, grsem, ssem, rsem, gsem, osem):
    members, rows, columns, channels, patches, dev_rows, ens_size = dims
    rest = channels - 128
    units = patches * ens_size
    total_m = members * ens_size
    me = lax.axis_index("ens")
    mydom = lax.axis_index("dom")
    my_x, my_core = me // 2, me % 2
    mine = pl.ds(pl.multiple_of(me * members, members), members)

    def dest_of(dslot):
        dx = (my_x + 1 - dslot // 2) % 2
        dc = (my_core + (dslot + 1) // 2) % 2
        return dx * 2 + dc

    def x_copies(unit, action):
        patch, dslot = unit // ens_size, unit % ens_size
        slot = unit % 2
        first = dest_of(dslot) * dev_rows + patch * 4
        north = jnp.maximum(first - 1, 0)
        south = jnp.minimum(first + 4, rows - 1)
        for idx, (src, num, dst) in enumerate(((first, 4, 1), (north, 1, 0), (south, 1, 5))):
            copy = pltpu.make_async_copy(x_hbm.at[:, pl.ds(src, num)], xv.at[slot, :, pl.ds(dst, num)], xsem.at[slot, idx])
            action(copy)

    def ghost_copy(unit):
        return pltpu.make_async_remote_copy(
            src_ref=gsend.at[unit], dst_ref=grecv.at[unit], send_sem=gssem.at[unit], recv_sem=grsem.at[unit],
            device_id={"dom": 1 - mydom}, device_id_type=MESH)

    def unit_copies(patch, dslot):
        dev = {"ens": dest_of(dslot)}
        first = pltpu.make_async_remote_copy(
            src_ref=sb1.at[patch * 3 + dslot], dst_ref=gath.at[patch, :, :, mine, pl.ds(0, 128)],
            send_sem=ssem.at[patch, dslot, 0], recv_sem=rsem.at[patch, dslot, 0],
            device_id=dev, device_id_type=MESH)
        second = pltpu.make_async_remote_copy(
            src_ref=sb2.at[patch * 3 + dslot], dst_ref=rb.at[patch * 3 + dslot],
            send_sem=ssem.at[patch, dslot, 1], recv_sem=rsem.at[patch, dslot, 1],
            device_id=dev, device_id_type=MESH)
        return first, second

    def gath_copy(patch):
        return pltpu.make_async_copy(gath.at[patch], g_hbm.at[patch], gsem.at[patch])

    obs_copies = [pltpu.make_async_copy(ref.at[pl.ds(me * patches, patches)], obs_raw.at[i], osem.at[i]) for i, ref in enumerate((yo_hbm, wt_hbm))]

    x_copies(0, lambda c: c.start())
    for copy in obs_copies:
        copy.start()
    barrier = pltpu.get_barrier_semaphore()
    for dslot in range(3):
        pl.semaphore_signal(barrier, inc=1, device_id={"ens": dest_of(dslot)}, device_id_type=MESH)
    pl.semaphore_signal(barrier, inc=1, device_id={"dom": 1 - mydom}, device_id_type=MESH)

    xs[:, 1] = jnp.zeros((2, 6, members * 32, 128), jnp.float32)
    wf[...] = jnp.zeros_like(wf)
    wf[0:channels, :] = wo_ref[...].astype(jnp.float32)
    wo[...] = wf[0:CP, :].T.astype(jnp.bfloat16)
    wf[0:2 * channels, :] = wi_ref[...].astype(jnp.float32)
    keep = lax.broadcasted_iota(jnp.int32, (CP, 512), 0) < channels
    wi[0:CP, :] = jnp.where(keep, wf[0:CP, :], 0.0).astype(jnp.bfloat16)
    wi[CP:2 * CP, :] = wf[channels:channels + CP, :].astype(jnp.bfloat16)
    pl.semaphore_wait(barrier, 4)

    lane = lax.broadcasted_iota(jnp.int32, (members, 128), 1)

    def setup():
        wf[0:128, 0:CP] = jnp.zeros((128, CP), jnp.float32)
        wf[0:32, 0:channels] = op_ref[...].astype(jnp.float32)
        opt = wf[0:128, 0:CP].T.astype(jnp.bfloat16)
        for j in range(8):
            place = (lax.broadcasted_iota(jnp.int32, (128, CP), 1) == lax.broadcasted_iota(jnp.int32, (128, CP), 0) + 32 * j)
            wobs[j * CP:(j + 1) * CP, :] = jnp.dot(opt, place.astype(jnp.bfloat16), preferred_element_type=jnp.float32).astype(jnp.bfloat16)
        for copy in obs_copies:
            copy.wait()
        sub8 = lax.broadcasted_iota(jnp.int32, (8, 128), 0)
        lane8 = lax.broadcasted_iota(jnp.int32, (8, 128), 1) // 32
        wf[0:8, 0:128] = jnp.zeros((8, 128), jnp.float32)

        def rows_of(patch, carry):
            for i in range(2):
                for g in range(8):
                    wf[0:8, 0:32] = obs_raw[i, patch, g % 4, 0, (g // 4) * 8:(g // 4) * 8 + 8, :]
                    v = wf[0:8, 0:128]
                    v = v + pltpu.roll(v, 32, 1)
                    v = v + pltpu.roll(v, 64, 1)
                    for q in range(2):
                        obs_row[i, patch, g:g + 1, q * 128:q * 128 + 128] = jnp.sum(jnp.where(sub8 == lane8 + 4 * q, v, 0.0), axis=0, keepdims=True)
            return carry
        lax.fori_loop(0, patches, rows_of, 0)

    def prepare(unit):
        slot = unit % 2

        @pl.when(unit + 1 < units)
        def _():
            x_copies(unit + 1, lambda c: c.start())
        x_copies(unit, lambda c: c.wait())

        def convert(r, carry):
            for m in range(members):
                v = xv[slot, m, r]
                xs[slot, 0, r, 32 * m + 8:32 * m + 24, :] = v[:, :128].astype(jnp.float32)
                xs[slot, 1, r, 32 * m + 8:32 * m + 24, 0:rest] = v[:, 128:].astype(jnp.float32)
            return carry
        lax.fori_loop(0, 6, convert, 0)

        def edges(r, carry):
            for h in range(2):
                gsend[unit, 0, r, :, h * 128:h * 128 + 128] = xs[slot, h, r + 1, pl.ds(23, members, stride=32), :].astype(jnp.bfloat16)
                gsend[unit, 1, r, :, h * 128:h * 128 + 128] = xs[slot, h, r + 1, pl.ds(8, members, stride=32), :].astype(jnp.bfloat16)
            return carry
        lax.fori_loop(0, 4, edges, 0)
        ghost_copy(unit).start()

    def forecast(unit):
        patch, dslot = unit // ens_size, unit % ens_size
        slot = unit % 2
        out_slot = jnp.where(dslot < 3, patch * 3 + dslot, patches * 3)
        ghost_copy(unit).wait_recv()

        def block(r, carry):
            for h in range(2):
                xs[slot, h, r + 1, pl.ds(7, members, stride=32), :] = grecv[unit, 0, r, :, h * 128:h * 128 + 128].astype(jnp.float32)
                xs[slot, h, r + 1, pl.ds(24, members, stride=32), :] = grecv[unit, 1, r, :, h * 128:h * 128 + 128].astype(jnp.float32)
            for m in range(members):
                b = 32 * m
                for h in range(2):
                    cur = xs[slot, h, r + 1, b + 8:b + 24, :]
                    north = xs[slot, h, r, b + 8:b + 24, :]
                    south = xs[slot, h, r + 2, b + 8:b + 24, :]
                    west = xs[slot, h, r + 1, b + 7:b + 23, :]
                    east = xs[slot, h, r + 1, b + 9:b + 25, :]
                    lap = north + south + west + east - 4.0 * cur
                    xl[16 * m:16 * m + 16, h * 128:h * 128 + 128] = cur.astype(jnp.bfloat16)
                    xl[16 * m:16 * m + 16, CP + h * 128:CP + h * 128 + 128] = lap.astype(jnp.bfloat16)
            hidden = jnp.dot(xl[...], wi[...], preferred_element_type=jnp.float32)
            gel = jax.nn.gelu(hidden, approximate=True).astype(jnp.bfloat16)
            inc = jnp.dot(gel, wo[...], preferred_element_type=jnp.float32)
            for m in range(members):
                for h in range(2):
                    ts[h, 16 * m:16 * m + 16, :] = xs[slot, h, r + 1, 32 * m + 8:32 * m + 24, :] + inc[16 * m:16 * m + 16, h * 128:h * 128 + 128]
            for col in range(columns):
                sb1[out_slot, r, col] = ts[0, pl.ds(col, members, stride=16), :].astype(jnp.bfloat16)
                t2[r, col] = ts[1, pl.ds(col, members, stride=16), :]
            return carry
        lax.fori_loop(0, 4, block, 0)

        @pl.when(dslot < 3)
        def _():
            def pack(pair, carry):
                left = jnp.zeros((members, 128), jnp.float32)
                for k in range(8):
                    r, c0 = pair * 2 + k // 4, (k % 4) * 4
                    v = [t2[r, c0 + i] for i in range(4)]
                    for i in range(3):
                        sb2[out_slot, pair * 25 + k * 3 + i] = jnp.where(lane < 96, v[i], pltpu.roll(v[3], 96 - 32 * i, 1)).astype(jnp.bfloat16)
                    for i in range(4):
                        left = left + pltpu.roll(jnp.where(lane >= 96, v[i], 0.0), (32 + 3 * (4 * k + i)) % 128, 1)
                sb2[out_slot, pair * 25 + 24] = left.astype(jnp.bfloat16)
                return carry
            lax.fori_loop(0, 2, pack, 0)
            for copy in unit_copies(patch, dslot):
                copy.start()

        @pl.when(dslot == 3)
        def _():
            def own(r, carry):
                for col in range(columns):
                    gath[patch, r, col, mine, 0:128] = sb1[patches * 3, r, col]
                    gath[patch, r, col, mine, 128:256] = t2[r, col].astype(jnp.bfloat16)
                return carry
            lax.fori_loop(0, 4, own, 0)

    def unpack(patch, dslot):
        src = pl.ds(pl.multiple_of(dest_of(dslot) * members, members), members)
        box = patch * 3 + dslot

        def half(pair, carry):
            left = rb[box, pair * 25 + 24].astype(jnp.float32)
            for k in range(8):
                r, c0 = pair * 2 + k // 4, (k % 4) * 4
                p = [rb[box, pair * 25 + k * 3 + i].astype(jnp.float32) for i in range(3)]
                tail = [jnp.where(lane < 99, pltpu.roll(left, (96 - 3 * (4 * k + i)) % 128, 1), 0.0) for i in range(4)]
                for i in range(3):
                    gath[patch, r, c0 + i, src, 128:256] = jnp.where(lane < 96, p[i], tail[i]).astype(jnp.bfloat16)
                last = jnp.where(lane < 64, jnp.where(lane < 32, pltpu.roll(p[0], 32, 1), pltpu.roll(p[1], 64, 1)),
                                 jnp.where(lane < 96, pltpu.roll(p[2], 96, 1), tail[3]))
                gath[patch, r, c0 + 3, src, 128:256] = last.astype(jnp.bfloat16)
            return carry
        lax.fori_loop(0, 2, half, 0)

    def analysis(patch):
        def arrive(dslot, carry):
            for copy in unit_copies(patch, dslot):
                copy.wait_recv()
            unpack(patch, dslot)
            return carry
        lax.fori_loop(0, 3, lambda i, c: arrive(2 - i, c), 0)
        gath_copy(patch).start()
        eye = (lax.broadcasted_iota(jnp.int32, (total_m, total_m), 0) == lax.broadcasted_iota(jnp.int32, (total_m, total_m), 1)).astype(jnp.float32)
        csum = jnp.zeros((total_m, CP), jnp.float32)
        for half in range(2):
            lhs = jnp.concatenate([gath[patch, :, half * 8 + j].reshape(4 * total_m, CP) for j in range(8)], axis=1)
            yb = jnp.dot(lhs, wobs[...], preferred_element_type=jnp.float32)
            for r in range(4):
                g = half * 4 + r
                y = yb[r * total_m:(r + 1) * total_m]
                ybar = jnp.sum(y, axis=0, keepdims=True) * (1.0 / total_m)
                y = y - ybar
                c = y * obs_row[1, patch, g:g + 1, :]
                csum = csum + c * (obs_row[0, patch, g:g + 1, :] - ybar)
                yp[g] = y
                cm[g] = c
        a_mat = (total_m - 1.0) * eye
        for g in range(8):
            a_mat = a_mat + f32dot(cm[g], yp[g], NT)
        trace = jnp.sum(jnp.sum(a_mat * eye, axis=0, keepdims=True), axis=1, keepdims=True)

        def newton(step, carry):
            y, z = carry
            mix = 1.5 * eye - 0.5 * f32dot(z, y)
            return f32dot(y, mix), f32dot(mix, z)
        _, inv = lax.fori_loop(0, NS_STEPS, newton, (a_mat / trace, eye))
        root = inv / jnp.sqrt(trace)
        rhs = jnp.broadcast_to(jnp.sum(csum, axis=1, keepdims=True), (total_m, total_m))
        wbar = f32dot(root, f32dot(root, rhs))
        trans = math.sqrt(total_m - 1.0) * root + wbar
        trans = trans + (1.0 - jnp.sum(trans, axis=0, keepdims=True)) * (1.0 / total_m)
        tt_ref[patch] = trans.T

    def step(v, carry):
        @pl.when(v < units)
        def _():
            prepare(v)

        @pl.when((v >= 1) & (v <= units))
        def _():
            forecast(v - 1)

        @pl.when(v == 3)
        def _():
            setup()

        @pl.when((v >= 12) & (v % 4 == 0))
        def _():
            analysis(v // 4 - 3)
        return carry
    lax.fori_loop(0, units + 9, step, 0)

    def finish(patch, carry):
        for dslot in range(3):
            for copy in unit_copies(patch, dslot):
                copy.wait_send()
        for dslot in range(4):
            ghost_copy(patch * 4 + dslot).wait_send()
        gath_copy(patch).wait()
        return carry
    lax.fori_loop(0, patches, finish, 0)


def update_kernel(tt_ref, g_ref, out_ref):
    hi, mid, low = split3(tt_ref[0])
    n = tt_ref.shape[1]
    zero = jnp.zeros((n, n), jnp.float32)
    lhs = jnp.concatenate([
        jnp.concatenate([hi.astype(jnp.float32), mid.astype(jnp.float32)], axis=1),
        jnp.concatenate([low.astype(jnp.float32), zero], axis=1)], axis=0).astype(jnp.bfloat16)
    for col in range(g_ref.shape[2]):
        g = g_ref[0, 0, col]
        res = jnp.dot(lhs, jnp.concatenate([g, g], axis=0), preferred_element_type=jnp.float32)
        val = res[n:] + res[:n]
        out_ref[0, col] = val[:, :out_ref.shape[3]].astype(jnp.bfloat16)


def solution(mesh):
    ens_size = mesh.shape["ens"]
    obs_spec = P(None, None, "dom", None, None)

    def local_step(ens_state, w_in, w_out, obs_op, obs_val, obs_wt):
        members, rows, columns, channels = ens_state.shape
        total_m = members * ens_size
        dev_rows = rows // ens_size
        patches = dev_rows // 4
        units = patches * ens_size
        dims = (members, rows, columns, channels, patches, dev_rows, ens_size)
        vmem = pl.BlockSpec(memory_space=pltpu.VMEM)
        anym = pl.BlockSpec(memory_space=pl.ANY)
        bf, f32 = jnp.bfloat16, jnp.float32
        dma = pltpu.SemaphoreType.DMA
        gathered, trans = pl.pallas_call(
            functools.partial(exchange_kernel, dims),
            out_shape=(jax.ShapeDtypeStruct((patches, 4, columns, total_m, CP), bf),
                       jax.ShapeDtypeStruct((patches, total_m, total_m), f32)),
            in_specs=[anym, vmem, vmem, vmem, anym, anym],
            out_specs=(anym, vmem),
            scratch_shapes=[
                pltpu.VMEM((2, members, 6, columns, channels), bf),
                pltpu.VMEM((2, 2, 6, members * 32, 128), f32),
                pltpu.VMEM((members * columns, 2 * CP), bf),
                pltpu.VMEM((2, members * columns, 128), f32),
                pltpu.VMEM((4, columns, members, 128), f32),
                pltpu.VMEM((patches * 3 + 1, 4, columns, members, 128), bf),
                pltpu.VMEM((patches * 3, 50, members, 128), bf),
                pltpu.VMEM((patches * 3, 50, members, 128), bf),
                pltpu.VMEM((patches, 4, columns, total_m, CP), bf),
                pltpu.VMEM((units, 2, 4, members, CP), bf),
                pltpu.VMEM((units, 2, 4, members, CP), bf),
                pltpu.VMEM((2 * CP, 512), bf),
                pltpu.VMEM((512, CP), bf),
                pltpu.VMEM((488, 512), f32),
                pltpu.VMEM((8 * CP, CP), bf),
                pltpu.VMEM((2, patches, 4, 1, columns, 32), f32),
                pltpu.VMEM((2, patches, 8, CP), f32),
                pltpu.VMEM((8, total_m, CP), f32),
                pltpu.VMEM((8, total_m, CP), f32),
                dma((2, 3)), dma((units,)), dma((units,)), dma((patches, 3, 2)), dma((patches, 3, 2)), dma((patches,)), dma((2,)),
            ],
            compiler_params=pltpu.CompilerParams(collective_id=0, has_side_effects=True, vmem_limit_bytes=62 * 1024 * 1024),
        )(ens_state, w_in, w_out.T, obs_op.T, obs_val, obs_wt)
        return pl.pallas_call(
            update_kernel,
            grid=(patches, 4),
            out_shape=jax.ShapeDtypeStruct((dev_rows, columns, total_m, channels), bf),
            in_specs=[pl.BlockSpec((1, total_m, total_m), lambda p, r: (p, 0, 0)),
                      pl.BlockSpec((1, 1, columns, total_m, CP), lambda p, r: (p, r, 0, 0, 0))],
            out_specs=pl.BlockSpec((1, columns, total_m, channels), lambda p, r: (p * 4 + r, 0, 0, 0)),
            compiler_params=pltpu.CompilerParams(dimension_semantics=("arbitrary", "arbitrary")),
        )(trans, gathered)

    return jax.shard_map(local_step, mesh=mesh, in_specs=(P("ens", None, "dom", None), P(), P(), P(), obs_spec, obs_spec), out_specs=P("ens", "dom", None, None), check_vma=False)
```

```python
import functools
import math
import jax
import jax.numpy as jnp
from jax import lax
from jax.experimental import pallas as pl
from jax.experimental.pallas import tpu as pltpu
from jax.sharding import PartitionSpec as P

NS_STEPS = 18
MESH = pl.DeviceIdType.MESH
CP = 256
NT = (((1,), (1,)), ((), ()))


NN = (((1,), (0,)), ((), ()))


def gelu(x):
    scale = math.sqrt(2.0 / math.pi)
    return (0.5 * x) * (1.0 + jnp.tanh(x * (scale + (scale * 0.044715) * (x * x))))


def split3(a):
    hi = a.astype(jnp.bfloat16)
    rem = a - hi.astype(jnp.float32)
    mid = rem.astype(jnp.bfloat16)
    low = (rem - mid.astype(jnp.float32)).astype(jnp.bfloat16)
    return hi, mid, low


def f32dot(a, b, dims=NN):
    ah, am, al = split3(a)
    bh, bm, bl = split3(b)
    n = a.shape[0]

    def dot(u, v):
        return lax.dot_general(u, v, dims, preferred_element_type=jnp.float32)
    by_hi = dot(jnp.concatenate([ah, am, al], axis=0), bh)
    by_mid = dot(jnp.concatenate([ah, am], axis=0), bm)
    by_low = dot(ah, bl)
    small = (by_low + by_hi[2 * n:]) + by_mid[n:]
    return (small + (by_mid[:n] + by_hi[n:2 * n])) + by_hi[:n]


def pair_lhs(a):
    hi, mid, low = split3(a)
    first = lax.broadcasted_iota(jnp.int32, a.shape, 1) < a.shape[1] // 2
    hi, mid, low = (v.astype(jnp.float32) for v in (hi, mid, low))
    lead = jnp.where(first, hi, mid).astype(jnp.bfloat16)
    return jnp.concatenate([lead, lead, jnp.where(first, hi, low).astype(jnp.bfloat16)], axis=1)


def pair_rhs(b):
    hi, mid, low = split3(b)
    return jnp.concatenate([hi, hi, mid, mid, low, hi], axis=0)


def twin_dot(lhs, rhs):
    k = rhs.shape[1]
    acc = jnp.dot(lhs[:, 2*k:], rhs[2*k:], preferred_element_type=jnp.float32)
    acc = acc + jnp.dot(lhs[:, k:2*k], rhs[k:2*k], preferred_element_type=jnp.float32)
    return acc + jnp.dot(lhs[:, :k], rhs[:k], preferred_element_type=jnp.float32)


def exchange_kernel(dims, x_hbm, wi_ref, wo_ref, op_ref, yo_hbm, wt_hbm, g_hbm, tt_ref,
                    xv, xs, xl, ts, t2, sb1, sb2, rb, gath, gsend, grecv, wi, wo, wf, wobs, obs_raw, obs_row, yp, cm, amat, cvec,
                    xsem, gssem, grsem, ssem, rsem, gsem, osem):
    members, rows, columns, channels, patches, dev_rows, ens_size = dims
    rest = channels - 128
    units = patches * ens_size
    total_m = members * ens_size
    me = lax.axis_index("ens")
    mydom = lax.axis_index("dom")
    my_x, my_core = me // 2, me % 2
    mine = pl.ds(pl.multiple_of(me * members, members), members)

    def dest_of(dslot):
        dx = (my_x + 1 - dslot // 2) % 2
        dc = (my_core + (dslot + 1) // 2) % 2
        return dx * 2 + dc

    def x_copies(unit, action):
        patch, dslot = unit // ens_size, unit % ens_size
        slot = unit % 2
        first = dest_of(dslot) * dev_rows + patch * 4
        north = jnp.maximum(first - 1, 0)
        south = jnp.minimum(first + 4, rows - 1)
        for idx, (src, num, dst) in enumerate(((first, 4, 1), (north, 1, 0), (south, 1, 5))):
            copy = pltpu.make_async_copy(x_hbm.at[:, pl.ds(src, num)], xv.at[slot, :, pl.ds(dst, num)], xsem.at[slot, idx])
            action(copy)

    def ghost_copy(unit):
        return pltpu.make_async_remote_copy(
            src_ref=gsend.at[unit], dst_ref=grecv.at[unit], send_sem=gssem.at[unit], recv_sem=grsem.at[unit],
            device_id={"dom": 1 - mydom}, device_id_type=MESH)

    def unit_copies(patch, dslot):
        dev = {"ens": dest_of(dslot)}
        first = pltpu.make_async_remote_copy(
            src_ref=sb1.at[patch * 3 + dslot], dst_ref=gath.at[patch, :, :, mine, pl.ds(0, 128)],
            send_sem=ssem.at[patch, dslot, 0], recv_sem=rsem.at[patch, dslot, 0],
            device_id=dev, device_id_type=MESH)
        second = pltpu.make_async_remote_copy(
            src_ref=sb2.at[patch * 3 + dslot], dst_ref=rb.at[patch * 3 + dslot],
            send_sem=ssem.at[patch, dslot, 1], recv_sem=rsem.at[patch, dslot, 1],
            device_id=dev, device_id_type=MESH)
        return first, second

    def gath_copy(patch):
        return pltpu.make_async_copy(gath.at[patch], g_hbm.at[patch], gsem.at[patch])

    obs_copies = [pltpu.make_async_copy(ref.at[pl.ds(me * patches, patches)], obs_raw.at[i], osem.at[i]) for i, ref in enumerate((yo_hbm, wt_hbm))]

    x_copies(0, lambda c: c.start())
    for copy in obs_copies:
        copy.start()
    barrier = pltpu.get_barrier_semaphore()
    for dslot in range(3):
        pl.semaphore_signal(barrier, inc=1, device_id={"ens": dest_of(dslot)}, device_id_type=MESH)
    pl.semaphore_signal(barrier, inc=1, device_id={"dom": 1 - mydom}, device_id_type=MESH)

    xs[:, 1] = jnp.zeros((2, 6, members * 32, 128), jnp.float32)
    wf[...] = jnp.zeros_like(wf)
    wf[0:channels, :] = wo_ref[...].astype(jnp.float32)
    wo[...] = wf[0:CP, :].T.astype(jnp.bfloat16)
    wf[0:2 * channels, :] = wi_ref[...].astype(jnp.float32)
    keep = lax.broadcasted_iota(jnp.int32, (CP, 512), 0) < channels
    wi[0:CP, :] = jnp.where(keep, wf[0:CP, :], 0.0).astype(jnp.bfloat16)
    wi[CP:2 * CP, :] = wf[channels:channels + CP, :].astype(jnp.bfloat16)
    pl.semaphore_wait(barrier, 4)

    lane = lax.broadcasted_iota(jnp.int32, (members, 128), 1)

    def setup():
        wf[0:128, 0:CP] = jnp.zeros((128, CP), jnp.float32)
        wf[0:32, 0:channels] = op_ref[...].astype(jnp.float32)
        opt = wf[0:128, 0:CP].T.astype(jnp.bfloat16)
        for j in range(8):
            place = (lax.broadcasted_iota(jnp.int32, (128, CP), 1) == lax.broadcasted_iota(jnp.int32, (128, CP), 0) + 32 * j)
            wobs[j * CP:(j + 1) * CP, :] = jnp.dot(opt, place.astype(jnp.bfloat16), preferred_element_type=jnp.float32).astype(jnp.bfloat16)
        for copy in obs_copies:
            copy.wait()
        sub8 = lax.broadcasted_iota(jnp.int32, (8, 128), 0)
        lane8 = lax.broadcasted_iota(jnp.int32, (8, 128), 1) // 32
        wf[0:8, 0:128] = jnp.zeros((8, 128), jnp.float32)

        def rows_of(patch, carry):
            for i in range(2):
                for g in range(8):
                    wf[0:8, 0:32] = obs_raw[i, patch, g % 4, 0, (g // 4) * 8:(g // 4) * 8 + 8, :]
                    v = wf[0:8, 0:128]
                    v = v + pltpu.roll(v, 32, 1)
                    v = v + pltpu.roll(v, 64, 1)
                    for q in range(2):
                        obs_row[i, patch, g:g + 1, q * 128:q * 128 + 128] = jnp.sum(jnp.where(sub8 == lane8 + 4 * q, v, 0.0), axis=0, keepdims=True)
            return carry
        lax.fori_loop(0, patches, rows_of, 0)

    def prepare(unit):
        slot = unit % 2

        @pl.when(unit + 1 < units)
        def _():
            x_copies(unit + 1, lambda c: c.start())
        x_copies(unit, lambda c: c.wait())

        def convert(r, carry):
            for m in range(members):
                v = xv[slot, m, r]
                xs[slot, 0, r, 32 * m + 8:32 * m + 24, :] = v[:, :128].astype(jnp.float32)
                xs[slot, 1, r, 32 * m + 8:32 * m + 24, 0:rest] = v[:, 128:].astype(jnp.float32)
            return carry
        lax.fori_loop(0, 6, convert, 0)

        def edges(r, carry):
            for h in range(2):
                gsend[unit, 0, r, :, h * 128:h * 128 + 128] = xs[slot, h, r + 1, pl.ds(23, members, stride=32), :].astype(jnp.bfloat16)
                gsend[unit, 1, r, :, h * 128:h * 128 + 128] = xs[slot, h, r + 1, pl.ds(8, members, stride=32), :].astype(jnp.bfloat16)
            return carry
        lax.fori_loop(0, 4, edges, 0)
        ghost_copy(unit).start()

    def forecast(unit):
        patch, dslot = unit // ens_size, unit % ens_size
        slot = unit % 2
        out_slot = jnp.where(dslot < 3, patch * 3 + dslot, patches * 3)
        ghost_copy(unit).wait_recv()

        def block(r, carry):
            for h in range(2):
                xs[slot, h, r + 1, pl.ds(7, members, stride=32), :] = grecv[unit, 0, r, :, h * 128:h * 128 + 128].astype(jnp.float32)
                xs[slot, h, r + 1, pl.ds(24, members, stride=32), :] = grecv[unit, 1, r, :, h * 128:h * 128 + 128].astype(jnp.float32)
            for m in range(members):
                b = 32 * m
                for h in range(2):
                    cur = xs[slot, h, r + 1, b + 8:b + 24, :]
                    north = xs[slot, h, r, b + 8:b + 24, :]
                    south = xs[slot, h, r + 2, b + 8:b + 24, :]
                    west = xs[slot, h, r + 1, b + 7:b + 23, :]
                    east = xs[slot, h, r + 1, b + 9:b + 25, :]
                    lap = north + south + west + east - 4.0 * cur
                    xl[16 * m:16 * m + 16, h * 128:h * 128 + 128] = cur.astype(jnp.bfloat16)
                    xl[16 * m:16 * m + 16, CP + h * 128:CP + h * 128 + 128] = lap.astype(jnp.bfloat16)
            hidden = jnp.dot(xl[...], wi[...], preferred_element_type=jnp.float32)
            gel = gelu(hidden).astype(jnp.bfloat16)
            inc = jnp.dot(gel, wo[...], preferred_element_type=jnp.float32)
            for m in range(members):
                for h in range(2):
                    ts[h, 16 * m:16 * m + 16, :] = xs[slot, h, r + 1, 32 * m + 8:32 * m + 24, :] + inc[16 * m:16 * m + 16, h * 128:h * 128 + 128]
            for col in range(columns):
                sb1[out_slot, r, col] = ts[0, pl.ds(col, members, stride=16), :].astype(jnp.bfloat16)
                t2[r, col] = ts[1, pl.ds(col, members, stride=16), :]
            return carry
        lax.fori_loop(0, 4, block, 0)

        @pl.when(dslot < 3)
        def _():
            def pack(pair, carry):
                left = jnp.zeros((members, 128), jnp.float32)
                for k in range(8):
                    r, c0 = pair * 2 + k // 4, (k % 4) * 4
                    v = [t2[r, c0 + i] for i in range(4)]
                    for i in range(3):
                        sb2[out_slot, pair * 25 + k * 3 + i] = jnp.where(lane < 96, v[i], pltpu.roll(v[3], 96 - 32 * i, 1)).astype(jnp.bfloat16)
                    for i in range(4):
                        left = left + pltpu.roll(jnp.where(lane >= 96, v[i], 0.0), (32 + 3 * (4 * k + i)) % 128, 1)
                sb2[out_slot, pair * 25 + 24] = left.astype(jnp.bfloat16)
                return carry
            lax.fori_loop(0, 2, pack, 0)
            for copy in unit_copies(patch, dslot):
                copy.start()

        @pl.when(dslot == 3)
        def _():
            def own(r, carry):
                for col in range(columns):
                    gath[patch, r, col, mine, 0:128] = sb1[patches * 3, r, col]
                    gath[patch, r, col, mine, 128:256] = t2[r, col].astype(jnp.bfloat16)
                return carry
            lax.fori_loop(0, 4, own, 0)

    def unpack(patch, dslot):
        src = pl.ds(pl.multiple_of(dest_of(dslot) * members, members), members)
        box = patch * 3 + dslot

        def half(pair, carry):
            left = rb[box, pair * 25 + 24].astype(jnp.float32)
            for k in range(8):
                r, c0 = pair * 2 + k // 4, (k % 4) * 4
                p = [rb[box, pair * 25 + k * 3 + i].astype(jnp.float32) for i in range(3)]
                tail = [jnp.where(lane < 99, pltpu.roll(left, (96 - 3 * (4 * k + i)) % 128, 1), 0.0) for i in range(4)]
                for i in range(3):
                    gath[patch, r, c0 + i, src, 128:256] = jnp.where(lane < 96, p[i], tail[i]).astype(jnp.bfloat16)
                last = jnp.where(lane < 64, jnp.where(lane < 32, pltpu.roll(p[0], 32, 1), pltpu.roll(p[1], 64, 1)),
                                 jnp.where(lane < 96, pltpu.roll(p[2], 96, 1), tail[3]))
                gath[patch, r, c0 + 3, src, 128:256] = last.astype(jnp.bfloat16)
            return carry
        lax.fori_loop(0, 2, half, 0)

    def analysis(patch):
        def arrive(dslot, carry):
            for copy in unit_copies(patch, dslot):
                copy.wait_recv()
            unpack(patch, dslot)
            return carry
        lax.fori_loop(0, 3, lambda i, c: arrive(2 - i, c), 0)
        gath_copy(patch).start()
        eye = (lax.broadcasted_iota(jnp.int32, (total_m, total_m), 0) == lax.broadcasted_iota(jnp.int32, (total_m, total_m), 1)).astype(jnp.float32)
        csum = jnp.zeros((total_m, CP), jnp.float32)
        for half in range(2):
            lhs = jnp.concatenate([gath[patch, :, half * 8 + j].reshape(4 * total_m, CP) for j in range(8)], axis=1)
            yb = jnp.dot(lhs, wobs[...], preferred_element_type=jnp.float32)
            for r in range(4):
                g = half * 4 + r
                y = yb[r * total_m:(r + 1) * total_m]
                ybar = jnp.sum(y, axis=0, keepdims=True) * (1.0 / total_m)
                y = y - ybar
                c = y * obs_row[1, patch, g:g + 1, :]
                csum = csum + c * (obs_row[0, patch, g:g + 1, :] - ybar)
                yp[g] = y
                cm[g] = c
        a_mat = (total_m - 1.0) * eye
        for g in range(8):
            a_mat = a_mat + f32dot(cm[g], yp[g], NT)
        amat[patch % 2, :, 0:total_m] = a_mat
        amat[patch % 2, :, total_m:2 * total_m] = a_mat
        cvec[patch % 2] = jnp.broadcast_to(jnp.sum(csum, axis=1, keepdims=True), (total_m, 2 * total_m))

    def solve(patch):
        row = lax.broadcasted_iota(jnp.int32, (total_m, 2 * total_m), 0)
        col = lax.broadcasted_iota(jnp.int32, (total_m, 2 * total_m), 1)
        eye = ((row == col) | (row + total_m == col)).astype(jnp.float32)
        mats = [amat[i] for i in range(2)]
        traces = [0.5 * jnp.sum(jnp.sum(a * eye, axis=0, keepdims=True), axis=1, keepdims=True) for a in mats]

        def newton(step, carry):
            out = []
            for y, z in carry:
                mix = 1.5 * eye - 0.5 * twin_dot(pair_lhs(z), pair_rhs(y))
                out.append((twin_dot(pair_lhs(y), pair_rhs(mix)), twin_dot(pair_lhs(mix), pair_rhs(z))))
            return tuple(out)
        pairs = lax.fori_loop(0, NS_STEPS, newton, tuple((a / t, eye) for a, t in zip(mats, traces)))
        for i in range(2):
            root = pairs[i][1] / jnp.sqrt(traces[i])
            left = pair_lhs(root)
            wbar = twin_dot(left, pair_rhs(twin_dot(left, pair_rhs(cvec[i]))))
            trans = math.sqrt(total_m - 1.0) * root + wbar
            trans = trans + (1.0 - jnp.sum(trans, axis=0, keepdims=True)) * (1.0 / total_m)
            tt_ref[patch + i] = trans[:, 0:total_m].T

    def step(v, carry):
        @pl.when(v < units)
        def _():
            prepare(v)

        @pl.when((v >= 1) & (v <= units))
        def _():
            forecast(v - 1)

        @pl.when(v == 3)
        def _():
            setup()

        @pl.when((v >= 12) & (v % 4 == 0))
        def _():
            analysis(v // 4 - 3)

        @pl.when((v >= 12) & (v % 8 == 0))
        def _():
            solve(v // 4 - 4)
        return carry
    lax.fori_loop(0, units + 9, step, 0)

    def finish(patch, carry):
        for dslot in range(3):
            for copy in unit_copies(patch, dslot):
                copy.wait_send()
        for dslot in range(4):
            ghost_copy(patch * 4 + dslot).wait_send()
        gath_copy(patch).wait()
        return carry
    lax.fori_loop(0, patches, finish, 0)


def update_kernel(tt_ref, g_ref, out_ref):
    hi, mid, low = split3(tt_ref[0])
    n = tt_ref.shape[1]
    zero = jnp.zeros((n, n), jnp.float32)
    lhs = jnp.concatenate([
        jnp.concatenate([hi.astype(jnp.float32), mid.astype(jnp.float32)], axis=1),
        jnp.concatenate([low.astype(jnp.float32), zero], axis=1)], axis=0).astype(jnp.bfloat16)

    def row(r, carry):
        for col in range(g_ref.shape[2]):
            g = g_ref[0, r, col]
            res = jnp.dot(lhs, jnp.concatenate([g, g], axis=0), preferred_element_type=jnp.float32)
            val = res[n:] + res[:n]
            out_ref[r, col] = val[:, :out_ref.shape[3]].astype(jnp.bfloat16)
        return carry
    lax.fori_loop(0, g_ref.shape[1], row, 0)


def solution(mesh):
    ens_size = mesh.shape["ens"]
    obs_spec = P(None, None, "dom", None, None)

    def local_step(ens_state, w_in, w_out, obs_op, obs_val, obs_wt):
        members, rows, columns, channels = ens_state.shape
        total_m = members * ens_size
        dev_rows = rows // ens_size
        patches = dev_rows // 4
        units = patches * ens_size
        dims = (members, rows, columns, channels, patches, dev_rows, ens_size)
        vmem = pl.BlockSpec(memory_space=pltpu.VMEM)
        anym = pl.BlockSpec(memory_space=pl.ANY)
        bf, f32 = jnp.bfloat16, jnp.float32
        dma = pltpu.SemaphoreType.DMA
        gathered, trans = pl.pallas_call(
            functools.partial(exchange_kernel, dims),
            out_shape=(jax.ShapeDtypeStruct((patches, 4, columns, total_m, CP), bf),
                       jax.ShapeDtypeStruct((patches, total_m, total_m), f32)),
            in_specs=[anym, vmem, vmem, vmem, anym, anym],
            out_specs=(anym, vmem),
            scratch_shapes=[
                pltpu.VMEM((2, members, 6, columns, channels), bf),
                pltpu.VMEM((2, 2, 6, members * 32, 128), f32),
                pltpu.VMEM((members * columns, 2 * CP), bf),
                pltpu.VMEM((2, members * columns, 128), f32),
                pltpu.VMEM((4, columns, members, 128), f32),
                pltpu.VMEM((patches * 3 + 1, 4, columns, members, 128), bf),
                pltpu.VMEM((patches * 3, 50, members, 128), bf),
                pltpu.VMEM((patches * 3, 50, members, 128), bf),
                pltpu.VMEM((patches, 4, columns, total_m, CP), bf),
                pltpu.VMEM((units, 2, 4, members, CP), bf),
                pltpu.VMEM((units, 2, 4, members, CP), bf),
                pltpu.VMEM((2 * CP, 512), bf),
                pltpu.VMEM((512, CP), bf),
                pltpu.VMEM((488, 512), f32),
                pltpu.VMEM((8 * CP, CP), bf),
                pltpu.VMEM((2, patches, 4, 1, columns, 32), f32),
                pltpu.VMEM((2, patches, 8, CP), f32),
                pltpu.VMEM((8, total_m, CP), f32),
                pltpu.VMEM((8, total_m, CP), f32),
                pltpu.VMEM((2, total_m, 2 * total_m), f32),
                pltpu.VMEM((2, total_m, 2 * total_m), f32),
                dma((2, 3)), dma((units,)), dma((units,)), dma((patches, 3, 2)), dma((patches, 3, 2)), dma((patches,)), dma((2,)),
            ],
            compiler_params=pltpu.CompilerParams(collective_id=0, has_side_effects=True, vmem_limit_bytes=62 * 1024 * 1024),
        )(ens_state, w_in, w_out.T, obs_op.T, obs_val, obs_wt)
        return pl.pallas_call(
            update_kernel,
            grid=(patches,),
            out_shape=jax.ShapeDtypeStruct((dev_rows, columns, total_m, channels), bf),
            in_specs=[pl.BlockSpec((1, total_m, total_m), lambda p: (p, 0, 0)),
                      pl.BlockSpec((1, 4, columns, total_m, CP), lambda p: (p, 0, 0, 0, 0))],
            out_specs=pl.BlockSpec((4, columns, total_m, channels), lambda p: (p, 0, 0, 0)),
            compiler_params=pltpu.CompilerParams(dimension_semantics=("arbitrary",)),
        )(trans, gathered)

    return jax.shard_map(local_step, mesh=mesh, in_specs=(P("ens", None, "dom", None), P(), P(), P(), obs_spec, obs_spec), out_specs=P("ens", "dom", None, None), check_vma=False)
```

```python
import functools
import math
import jax
import jax.numpy as jnp
from jax import lax
from jax.experimental import pallas as pl
from jax.experimental.pallas import tpu as pltpu
from jax.sharding import PartitionSpec as P

NS_STEPS = 18
MESH = pl.DeviceIdType.MESH
CP = 256
NT = (((1,), (1,)), ((), ()))


NN = (((1,), (0,)), ((), ()))


def gelu(x):
    scale = math.sqrt(2.0 / math.pi)
    return (0.5 * x) * (1.0 + jnp.tanh(x * (scale + (scale * 0.044715) * (x * x))))


def split3(a):
    hi = a.astype(jnp.bfloat16)
    rem = a - hi.astype(jnp.float32)
    mid = rem.astype(jnp.bfloat16)
    low = (rem - mid.astype(jnp.float32)).astype(jnp.bfloat16)
    return hi, mid, low


def f32dot(a, b, dims=NN):
    ah, am, al = split3(a)
    bh, bm, bl = split3(b)
    n = a.shape[0]

    def dot(u, v):
        return lax.dot_general(u, v, dims, preferred_element_type=jnp.float32)
    by_hi = dot(jnp.concatenate([ah, am, al], axis=0), bh)
    by_mid = dot(jnp.concatenate([ah, am], axis=0), bm)
    by_low = dot(ah, bl)
    small = (by_low + by_hi[2 * n:]) + by_mid[n:]
    return (small + (by_mid[:n] + by_hi[n:2 * n])) + by_hi[:n]


def pair_lhs(a):
    hi, mid, low = split3(a)
    first = lax.broadcasted_iota(jnp.int32, a.shape, 1) < a.shape[1] // 2
    hi, mid, low = (v.astype(jnp.float32) for v in (hi, mid, low))
    lead = jnp.where(first, hi, mid).astype(jnp.bfloat16)
    return jnp.concatenate([lead, lead, jnp.where(first, hi, low).astype(jnp.bfloat16)], axis=1)


def pair_rhs(b):
    hi, mid, low = split3(b)
    return jnp.concatenate([hi, hi, mid, mid, low, hi], axis=0)


def twin_dot(lhs, rhs):
    k = rhs.shape[1]
    acc = jnp.dot(lhs[:, 2*k:], rhs[2*k:], preferred_element_type=jnp.float32)
    acc = acc + jnp.dot(lhs[:, k:2*k], rhs[k:2*k], preferred_element_type=jnp.float32)
    return acc + jnp.dot(lhs[:, :k], rhs[:k], preferred_element_type=jnp.float32)


def exchange_kernel(dims, xt_hbm, wi_ref, wo_ref, op_ref, yo_hbm, wt_hbm, g_hbm, tt_ref,
                    xn, xb, xs, xl, ts, t2, sb1, sb2, rb, gath, gsend, grecv, wi, wo, wf, wobs, obs_raw, obs_row, yp, cm, amat, cvec,
                    xsem, gssem, grsem, ssem, rsem, gsem, osem):
    members, rows, columns, channels, patches, dev_rows, ens_size = dims
    units = patches * ens_size
    total_m = members * ens_size
    me = lax.axis_index("ens")
    mydom = lax.axis_index("dom")
    my_x, my_core = me // 2, me % 2
    mine = pl.ds(pl.multiple_of(me * members, members), members)

    def dest_of(dslot):
        dx = (my_x + 1 - dslot // 2) % 2
        dc = (my_core + (dslot + 1) // 2) % 2
        return dx * 2 + dc

    def x_copy(m):
        return pltpu.make_async_copy(xt_hbm.at[m], xn.at[m % 2], xsem.at[m % 2])

    def ghost_copy(unit):
        return pltpu.make_async_remote_copy(
            src_ref=gsend.at[unit], dst_ref=grecv.at[unit], send_sem=gssem.at[unit], recv_sem=grsem.at[unit],
            device_id={"dom": 1 - mydom}, device_id_type=MESH)

    def unit_copies(patch, dslot):
        dev = {"ens": dest_of(dslot)}
        first = pltpu.make_async_remote_copy(
            src_ref=sb1.at[(patch % 3) * 3 + dslot], dst_ref=gath.at[patch, :, :, mine, pl.ds(0, 128)],
            send_sem=ssem.at[patch, dslot, 0], recv_sem=rsem.at[patch, dslot, 0],
            device_id=dev, device_id_type=MESH)
        second = pltpu.make_async_remote_copy(
            src_ref=sb2.at[(patch % 3) * 3 + dslot], dst_ref=rb.at[patch * 3 + dslot],
            send_sem=ssem.at[patch, dslot, 1], recv_sem=rsem.at[patch, dslot, 1],
            device_id=dev, device_id_type=MESH)
        return first, second

    def gath_copy(patch):
        return pltpu.make_async_copy(gath.at[patch], g_hbm.at[patch], gsem.at[patch])

    obs_copies = [pltpu.make_async_copy(ref.at[pl.ds(me * patches, patches)], obs_raw.at[i], osem.at[i]) for i, ref in enumerate((yo_hbm, wt_hbm))]

    x_copy(0).start()
    for copy in obs_copies:
        copy.start()
    barrier = pltpu.get_barrier_semaphore()
    for dslot in range(3):
        pl.semaphore_signal(barrier, inc=1, device_id={"ens": dest_of(dslot)}, device_id_type=MESH)
    pl.semaphore_signal(barrier, inc=1, device_id={"dom": 1 - mydom}, device_id_type=MESH)

    xs[0, 1, 3, 16 * (channels % 32):512, :] = jnp.zeros((512 - 16 * (channels % 32), 128), jnp.float32)
    wf[...] = jnp.zeros_like(wf)
    wf[0:channels, :] = wo_ref[...].astype(jnp.float32)
    wo[...] = wf[0:CP, :].T.astype(jnp.bfloat16)
    wf[0:2 * channels, :] = wi_ref[...].astype(jnp.float32)
    keep = lax.broadcasted_iota(jnp.int32, (CP, 512), 0) < channels
    wi[0:CP, :] = jnp.where(keep, wf[0:CP, :], 0.0).astype(jnp.bfloat16)
    wi[CP:2 * CP, :] = wf[channels:channels + CP, :].astype(jnp.bfloat16)
    turn = (lax.broadcasted_iota(jnp.int32, (128, 128), 0) == lax.broadcasted_iota(jnp.int32, (128, 128), 1)).astype(jnp.float32).astype(jnp.bfloat16)

    def relayout(m, carry):
        @pl.when(m + 1 < members)
        def _():
            x_copy(m + 1).start()
        x_copy(m).wait()

        def widen(b, c2):
            for cc in range(32):
                xs[0, b // 4, b % 4, 16 * cc:16 * cc + 16, :] = xn[m % 2, b * 32 + cc].astype(jnp.float32)
            return c2
        lax.fori_loop(0, channels // 32, widen, 0)
        for cc in range(channels % 32):
            xs[0, 1, 3, 16 * cc:16 * cc + 16, :] = xn[m % 2, channels - channels % 32 + cc].astype(jnp.float32)
        for col in range(columns):
            part = jnp.concatenate([xs[0, h, j, pl.ds(col, 32, stride=16), :] for h in range(2) for j in range(4)], axis=0)
            out = lax.dot_general(turn, part.astype(jnp.bfloat16), NT, preferred_element_type=jnp.float32)
            for h in range(2):
                for j in range(4):
                    xs[1, h, j, pl.ds(col, 32, stride=16), :] = out[32 * j:32 * j + 32, h * 128:h * 128 + 128]

        def narrow(j, c2):
            for rr in range(32):
                for h in range(2):
                    xb[m, 32 * j + rr, :, h * 128:h * 128 + 128] = xs[1, h, j, 16 * rr:16 * rr + 16, :].astype(jnp.bfloat16)
            return c2
        lax.fori_loop(0, 4, narrow, 0)
        return carry
    lax.fori_loop(0, members, relayout, 0)
    pl.semaphore_wait(barrier, 4)

    lane = lax.broadcasted_iota(jnp.int32, (members, 128), 1)

    def setup():
        wf[0:128, 0:CP] = jnp.zeros((128, CP), jnp.float32)
        wf[0:32, 0:channels] = op_ref[...].astype(jnp.float32)
        opt = wf[0:128, 0:CP].T.astype(jnp.bfloat16)
        for j in range(8):
            place = (lax.broadcasted_iota(jnp.int32, (128, CP), 1) == lax.broadcasted_iota(jnp.int32, (128, CP), 0) + 32 * j)
            wobs[j * CP:(j + 1) * CP, :] = jnp.dot(opt, place.astype(jnp.bfloat16), preferred_element_type=jnp.float32).astype(jnp.bfloat16)
        for copy in obs_copies:
            copy.wait()
        sub8 = lax.broadcasted_iota(jnp.int32, (8, 128), 0)
        lane8 = lax.broadcasted_iota(jnp.int32, (8, 128), 1) // 32
        wf[0:8, 0:128] = jnp.zeros((8, 128), jnp.float32)

        def rows_of(patch, carry):
            for i in range(2):
                for g in range(8):
                    wf[0:8, 0:32] = obs_raw[i, patch, g % 4, 0, (g // 4) * 8:(g // 4) * 8 + 8, :]
                    v = wf[0:8, 0:128]
                    v = v + pltpu.roll(v, 32, 1)
                    v = v + pltpu.roll(v, 64, 1)
                    for q in range(2):
                        obs_row[i, patch, g:g + 1, q * 128:q * 128 + 128] = jnp.sum(jnp.where(sub8 == lane8 + 4 * q, v, 0.0), axis=0, keepdims=True)
            return carry
        lax.fori_loop(0, patches, rows_of, 0)

    def prepare(unit):
        slot = unit % 2
        patch, dslot = unit // ens_size, unit % ens_size
        first = dest_of(dslot) * dev_rows + patch * 4

        def convert(r, carry):
            row = jnp.minimum(jnp.maximum(first + r - 1, 0), rows - 1)
            for m in range(members):
                for h in range(2):
                    xs[slot, h, r, 32 * m + 8:32 * m + 24, :] = xb[m, row, :, h * 128:h * 128 + 128].astype(jnp.float32)
            return carry
        lax.fori_loop(0, 6, convert, 0)

        def edges(r, carry):
            for h in range(2):
                gsend[unit, 0, r, :, h * 128:h * 128 + 128] = xs[slot, h, r + 1, pl.ds(23, members, stride=32), :].astype(jnp.bfloat16)
                gsend[unit, 1, r, :, h * 128:h * 128 + 128] = xs[slot, h, r + 1, pl.ds(8, members, stride=32), :].astype(jnp.bfloat16)
            return carry
        lax.fori_loop(0, 4, edges, 0)
        ghost_copy(unit).start()

    def forecast(unit):
        patch, dslot = unit // ens_size, unit % ens_size
        slot = unit % 2
        out_slot = jnp.where(dslot < 3, (patch % 3) * 3 + dslot, 9)

        @pl.when((dslot < 3) & (patch >= 3))
        def _():
            for copy in unit_copies(patch - 3, dslot):
                copy.wait_send()
        ghost_copy(unit).wait_recv()

        def block(r, carry):
            for h in range(2):
                xs[slot, h, r + 1, pl.ds(7, members, stride=32), :] = grecv[unit, 0, r, :, h * 128:h * 128 + 128].astype(jnp.float32)
                xs[slot, h, r + 1, pl.ds(24, members, stride=32), :] = grecv[unit, 1, r, :, h * 128:h * 128 + 128].astype(jnp.float32)
            for m in range(members):
                b = 32 * m
                for h in range(2):
                    cur = xs[slot, h, r + 1, b + 8:b + 24, :]
                    north = xs[slot, h, r, b + 8:b + 24, :]
                    south = xs[slot, h, r + 2, b + 8:b + 24, :]
                    west = xs[slot, h, r + 1, b + 7:b + 23, :]
                    east = xs[slot, h, r + 1, b + 9:b + 25, :]
                    lap = north + south + west + east - 4.0 * cur
                    xl[16 * m:16 * m + 16, h * 128:h * 128 + 128] = cur.astype(jnp.bfloat16)
                    xl[16 * m:16 * m + 16, CP + h * 128:CP + h * 128 + 128] = lap.astype(jnp.bfloat16)
            hidden = jnp.dot(xl[...], wi[...], preferred_element_type=jnp.float32)
            gel = gelu(hidden).astype(jnp.bfloat16)
            inc = jnp.dot(gel, wo[...], preferred_element_type=jnp.float32)
            for m in range(members):
                for h in range(2):
                    ts[h, 16 * m:16 * m + 16, :] = xs[slot, h, r + 1, 32 * m + 8:32 * m + 24, :] + inc[16 * m:16 * m + 16, h * 128:h * 128 + 128]
            for col in range(columns):
                sb1[out_slot, r, col] = ts[0, pl.ds(col, members, stride=16), :].astype(jnp.bfloat16)
                t2[r, col] = ts[1, pl.ds(col, members, stride=16), :]
            return carry
        lax.fori_loop(0, 4, block, 0)

        @pl.when(dslot < 3)
        def _():
            def pack(pair, carry):
                left = jnp.zeros((members, 128), jnp.float32)
                for k in range(8):
                    r, c0 = pair * 2 + k // 4, (k % 4) * 4
                    v = [t2[r, c0 + i] for i in range(4)]
                    for i in range(3):
                        sb2[out_slot, pair * 25 + k * 3 + i] = jnp.where(lane < 96, v[i], pltpu.roll(v[3], 96 - 32 * i, 1)).astype(jnp.bfloat16)
                    for i in range(4):
                        left = left + pltpu.roll(jnp.where(lane >= 96, v[i], 0.0), (32 + 3 * (4 * k + i)) % 128, 1)
                sb2[out_slot, pair * 25 + 24] = left.astype(jnp.bfloat16)
                return carry
            lax.fori_loop(0, 2, pack, 0)
            for copy in unit_copies(patch, dslot):
                copy.start()

        @pl.when(dslot == 3)
        def _():
            def own(r, carry):
                for col in range(columns):
                    gath[patch, r, col, mine, 0:128] = sb1[9, r, col]
                    gath[patch, r, col, mine, 128:256] = t2[r, col].astype(jnp.bfloat16)
                return carry
            lax.fori_loop(0, 4, own, 0)

    def unpack(patch, dslot):
        src = pl.ds(pl.multiple_of(dest_of(dslot) * members, members), members)
        box = patch * 3 + dslot

        def half(pair, carry):
            left = rb[box, pair * 25 + 24].astype(jnp.float32)
            for k in range(8):
                r, c0 = pair * 2 + k // 4, (k % 4) * 4
                p = [rb[box, pair * 25 + k * 3 + i].astype(jnp.float32) for i in range(3)]
                tail = [jnp.where(lane < 99, pltpu.roll(left, (96 - 3 * (4 * k + i)) % 128, 1), 0.0) for i in range(4)]
                for i in range(3):
                    gath[patch, r, c0 + i, src, 128:256] = jnp.where(lane < 96, p[i], tail[i]).astype(jnp.bfloat16)
                last = jnp.where(lane < 64, jnp.where(lane < 32, pltpu.roll(p[0], 32, 1), pltpu.roll(p[1], 64, 1)),
                                 jnp.where(lane < 96, pltpu.roll(p[2], 96, 1), tail[3]))
                gath[patch, r, c0 + 3, src, 128:256] = last.astype(jnp.bfloat16)
            return carry
        lax.fori_loop(0, 2, half, 0)

    def analysis(patch):
        def arrive(dslot, carry):
            for copy in unit_copies(patch, dslot):
                copy.wait_recv()
            unpack(patch, dslot)
            return carry
        lax.fori_loop(0, 3, lambda i, c: arrive(2 - i, c), 0)
        gath_copy(patch).start()
        eye = (lax.broadcasted_iota(jnp.int32, (total_m, total_m), 0) == lax.broadcasted_iota(jnp.int32, (total_m, total_m), 1)).astype(jnp.float32)
        csum = jnp.zeros((total_m, CP), jnp.float32)
        for half in range(2):
            lhs = jnp.concatenate([gath[patch, :, half * 8 + j].reshape(4 * total_m, CP) for j in range(8)], axis=1)
            yb = jnp.dot(lhs, wobs[...], preferred_element_type=jnp.float32)
            for r in range(4):
                g = half * 4 + r
                y = yb[r * total_m:(r + 1) * total_m]
                ybar = jnp.sum(y, axis=0, keepdims=True) * (1.0 / total_m)
                y = y - ybar
                c = y * obs_row[1, patch, g:g + 1, :]
                csum = csum + c * (obs_row[0, patch, g:g + 1, :] - ybar)
                yp[g] = y
                cm[g] = c
        a_mat = (total_m - 1.0) * eye
        for g in range(8):
            a_mat = a_mat + f32dot(cm[g], yp[g], NT)
        amat[patch % 2, :, 0:total_m] = a_mat
        amat[patch % 2, :, total_m:2 * total_m] = a_mat
        cvec[patch % 2] = jnp.broadcast_to(jnp.sum(csum, axis=1, keepdims=True), (total_m, 2 * total_m))

    def solve(patch):
        row = lax.broadcasted_iota(jnp.int32, (total_m, 2 * total_m), 0)
        col = lax.broadcasted_iota(jnp.int32, (total_m, 2 * total_m), 1)
        eye = ((row == col) | (row + total_m == col)).astype(jnp.float32)
        mats = [amat[i] for i in range(2)]
        traces = [0.5 * jnp.sum(jnp.sum(a * eye, axis=0, keepdims=True), axis=1, keepdims=True) for a in mats]

        def newton(step, carry):
            out = []
            for y, z in carry:
                mix = 1.5 * eye - 0.5 * twin_dot(pair_lhs(z), pair_rhs(y))
                out.append((twin_dot(pair_lhs(y), pair_rhs(mix)), twin_dot(pair_lhs(mix), pair_rhs(z))))
            return tuple(out)
        pairs = lax.fori_loop(0, NS_STEPS, newton, tuple((a / t, eye) for a, t in zip(mats, traces)))
        for i in range(2):
            root = pairs[i][1] / jnp.sqrt(traces[i])
            left = pair_lhs(root)
            wbar = twin_dot(left, pair_rhs(twin_dot(left, pair_rhs(cvec[i]))))
            trans = math.sqrt(total_m - 1.0) * root + wbar
            trans = trans + (1.0 - jnp.sum(trans, axis=0, keepdims=True)) * (1.0 / total_m)
            tt_ref[patch + i] = trans[:, 0:total_m].T

    def step(v, carry):
        @pl.when(v < units)
        def _():
            prepare(v)

        @pl.when((v >= 1) & (v <= units))
        def _():
            forecast(v - 1)

        @pl.when(v == 3)
        def _():
            setup()

        @pl.when((v >= 12) & (v % 4 == 0))
        def _():
            analysis(v // 4 - 3)

        @pl.when((v >= 12) & (v % 8 == 0))
        def _():
            solve(v // 4 - 4)
        return carry
    lax.fori_loop(0, units + 9, step, 0)

    def finish(patch, carry):
        @pl.when(patch >= patches - 3)
        def _():
            for dslot in range(3):
                for copy in unit_copies(patch, dslot):
                    copy.wait_send()
        for dslot in range(4):
            ghost_copy(patch * 4 + dslot).wait_send()
        gath_copy(patch).wait()
        return carry
    lax.fori_loop(0, patches, finish, 0)


def update_kernel(tt_ref, g_ref, out_ref):
    hi, mid, low = split3(tt_ref[0])
    n = tt_ref.shape[1]
    zero = jnp.zeros((n, n), jnp.float32)
    lhs = jnp.concatenate([
        jnp.concatenate([hi.astype(jnp.float32), mid.astype(jnp.float32)], axis=1),
        jnp.concatenate([low.astype(jnp.float32), zero], axis=1)], axis=0).astype(jnp.bfloat16)

    def row(r, carry):
        for col in range(g_ref.shape[2]):
            g = g_ref[0, r, col]
            res = jnp.dot(lhs, jnp.concatenate([g, g], axis=0), preferred_element_type=jnp.float32)
            val = res[n:] + res[:n]
            out_ref[r, col] = val[:, :out_ref.shape[3]].astype(jnp.bfloat16)
        return carry
    lax.fori_loop(0, g_ref.shape[1], row, 0)


def solution(mesh):
    ens_size = mesh.shape["ens"]
    obs_spec = P(None, None, "dom", None, None)

    def local_step(ens_state, w_in, w_out, obs_op, obs_val, obs_wt):
        members, rows, columns, channels = ens_state.shape
        total_m = members * ens_size
        dev_rows = rows // ens_size
        patches = dev_rows // 4
        units = patches * ens_size
        dims = (members, rows, columns, channels, patches, dev_rows, ens_size)
        vmem = pl.BlockSpec(memory_space=pltpu.VMEM)
        anym = pl.BlockSpec(memory_space=pl.ANY)
        bf, f32 = jnp.bfloat16, jnp.float32
        dma = pltpu.SemaphoreType.DMA
        gathered, trans = pl.pallas_call(
            functools.partial(exchange_kernel, dims),
            out_shape=(jax.ShapeDtypeStruct((patches, 4, columns, total_m, CP), bf),
                       jax.ShapeDtypeStruct((patches, total_m, total_m), f32)),
            in_specs=[anym, vmem, vmem, vmem, anym, anym],
            out_specs=(anym, vmem),
            scratch_shapes=[
                pltpu.VMEM((2, channels, columns, rows), bf),
                pltpu.VMEM((members, rows, columns, CP), bf),
                pltpu.VMEM((2, 2, 6, members * 32, 128), f32),
                pltpu.VMEM((members * columns, 2 * CP), bf),
                pltpu.VMEM((2, members * columns, 128), f32),
                pltpu.VMEM((4, columns, members, 128), f32),
                pltpu.VMEM((10, 4, columns, members, 128), bf),
                pltpu.VMEM((9, 50, members, 128), bf),
                pltpu.VMEM((patches * 3, 50, members, 128), bf),
                pltpu.VMEM((patches, 4, columns, total_m, CP), bf),
                pltpu.VMEM((units, 2, 4, members, CP), bf),
                pltpu.VMEM((units, 2, 4, members, CP), bf),
                pltpu.VMEM((2 * CP, 512), bf),
                pltpu.VMEM((512, CP), bf),
                pltpu.VMEM((488, 512), f32),
                pltpu.VMEM((8 * CP, CP), bf),
                pltpu.VMEM((2, patches, 4, 1, columns, 32), f32),
                pltpu.VMEM((2, patches, 8, CP), f32),
                pltpu.VMEM((8, total_m, CP), f32),
                pltpu.VMEM((8, total_m, CP), f32),
                pltpu.VMEM((2, total_m, 2 * total_m), f32),
                pltpu.VMEM((2, total_m, 2 * total_m), f32),
                dma((2,)), dma((units,)), dma((units,)), dma((patches, 3, 2)), dma((patches, 3, 2)), dma((patches,)), dma((2,)),
            ],
            compiler_params=pltpu.CompilerParams(collective_id=0, has_side_effects=True, vmem_limit_bytes=62 * 1024 * 1024),
        )(ens_state.transpose(0, 3, 2, 1), w_in, w_out.T, obs_op.T, obs_val, obs_wt)
        return pl.pallas_call(
            update_kernel,
            grid=(patches,),
            out_shape=jax.ShapeDtypeStruct((dev_rows, columns, total_m, channels), bf),
            in_specs=[pl.BlockSpec((1, total_m, total_m), lambda p: (p, 0, 0)),
                      pl.BlockSpec((1, 4, columns, total_m, CP), lambda p: (p, 0, 0, 0, 0))],
            out_specs=pl.BlockSpec((4, columns, total_m, channels), lambda p: (p, 0, 0, 0)),
            compiler_params=pltpu.CompilerParams(dimension_semantics=("arbitrary",)),
        )(trans, gathered)

    return jax.shard_map(local_step, mesh=mesh, in_specs=(P("ens", None, "dom", None), P(), P(), P(), obs_spec, obs_spec), out_specs=P("ens", "dom", None, None), check_vma=False)
```

```python
import functools
import math
import jax
import jax.numpy as jnp
from jax import lax
from jax.experimental import pallas as pl
from jax.experimental.pallas import tpu as pltpu
from jax.sharding import PartitionSpec as P

NS_STEPS = 18
MESH = pl.DeviceIdType.MESH
CP = 256
NT = (((1,), (1,)), ((), ()))


NN = (((1,), (0,)), ((), ()))


def gelu(x):
    scale = math.sqrt(2.0 / math.pi)
    return (0.5 * x) * (1.0 + jnp.tanh(x * (scale + (scale * 0.044715) * (x * x))))


def split3(a):
    hi = a.astype(jnp.bfloat16)
    rem = a - hi.astype(jnp.float32)
    mid = rem.astype(jnp.bfloat16)
    low = (rem - mid.astype(jnp.float32)).astype(jnp.bfloat16)
    return hi, mid, low


def f32dot(a, b, dims=NN):
    ah, am, al = split3(a)
    bh, bm, bl = split3(b)
    n = a.shape[0]

    def dot(u, v):
        return lax.dot_general(u, v, dims, preferred_element_type=jnp.float32)
    by_hi = dot(jnp.concatenate([ah, am, al], axis=0), bh)
    by_mid = dot(jnp.concatenate([ah, am], axis=0), bm)
    by_low = dot(ah, bl)
    small = (by_low + by_hi[2 * n:]) + by_mid[n:]
    return (small + (by_mid[:n] + by_hi[n:2 * n])) + by_hi[:n]


def pair_lhs(a):
    hi, mid, low = split3(a)
    first = lax.broadcasted_iota(jnp.int32, a.shape, 1) < a.shape[1] // 2
    hi, mid, low = (v.astype(jnp.float32) for v in (hi, mid, low))
    lead = jnp.where(first, hi, mid).astype(jnp.bfloat16)
    return jnp.concatenate([lead, lead, jnp.where(first, hi, low).astype(jnp.bfloat16)], axis=1)


def pair_rhs(b):
    hi, mid, low = split3(b)
    return jnp.concatenate([hi, hi, mid, mid, low, hi], axis=0)


def twin_dot(lhs, rhs):
    k = rhs.shape[1]
    acc = jnp.dot(lhs[:, 2*k:], rhs[2*k:], preferred_element_type=jnp.float32)
    acc = acc + jnp.dot(lhs[:, k:2*k], rhs[k:2*k], preferred_element_type=jnp.float32)
    return acc + jnp.dot(lhs[:, :k], rhs[:k], preferred_element_type=jnp.float32)


def exchange_kernel(dims, xt_hbm, wi_ref, wo_ref, op_ref, yo_hbm, wt_hbm, g_hbm, tt_ref,
                    xn, xb, xs, xl, ts, t2, sb1, sb2, rb, gath, gsend, grecv, wi, wo, wf, wobs, obs_raw, obs_row, yp, cm, amat, cvec,
                    xsem, gssem, grsem, ssem, rsem, gsem, osem):
    members, rows, columns, channels, patches, dev_rows, ens_size = dims
    units = patches * ens_size
    total_m = members * ens_size
    me = lax.axis_index("ens")
    mydom = lax.axis_index("dom")
    my_x, my_core = me // 2, me % 2
    mine = pl.ds(pl.multiple_of(me * members, members), members)

    def dest_of(dslot):
        dx = (my_x + 1 - dslot // 2) % 2
        dc = (my_core + (dslot + 1) // 2) % 2
        return dx * 2 + dc

    def x_copy(m):
        return pltpu.make_async_copy(xt_hbm.at[m], xn.at[m % 2], xsem.at[m % 2])

    def ghost_copy(unit):
        return pltpu.make_async_remote_copy(
            src_ref=gsend.at[unit], dst_ref=grecv.at[unit], send_sem=gssem.at[unit], recv_sem=grsem.at[unit],
            device_id={"dom": 1 - mydom}, device_id_type=MESH)

    def unit_copies(patch, dslot):
        dev = {"ens": dest_of(dslot)}
        first = pltpu.make_async_remote_copy(
            src_ref=sb1.at[(patch % 3) * 3 + dslot], dst_ref=gath.at[patch, :, :, mine, pl.ds(0, 128)],
            send_sem=ssem.at[patch, dslot, 0], recv_sem=rsem.at[patch, dslot, 0],
            device_id=dev, device_id_type=MESH)
        second = pltpu.make_async_remote_copy(
            src_ref=sb2.at[(patch % 3) * 3 + dslot], dst_ref=rb.at[patch * 3 + dslot],
            send_sem=ssem.at[patch, dslot, 1], recv_sem=rsem.at[patch, dslot, 1],
            device_id=dev, device_id_type=MESH)
        return first, second

    def gath_copy(patch):
        return pltpu.make_async_copy(gath.at[patch], g_hbm.at[patch], gsem.at[patch])

    obs_copies = [pltpu.make_async_copy(ref.at[pl.ds(me * patches, patches)], obs_raw.at[i], osem.at[i]) for i, ref in enumerate((yo_hbm, wt_hbm))]

    x_copy(0).start()
    for copy in obs_copies:
        copy.start()
    barrier = pltpu.get_barrier_semaphore()
    for dslot in range(3):
        pl.semaphore_signal(barrier, inc=1, device_id={"ens": dest_of(dslot)}, device_id_type=MESH)
    pl.semaphore_signal(barrier, inc=1, device_id={"dom": 1 - mydom}, device_id_type=MESH)

    xs[0, 1, 3, 17 * (channels % 32):544, :] = jnp.zeros((544 - 17 * (channels % 32), 128), jnp.float32)
    wf[...] = jnp.zeros_like(wf)
    wf[0:channels, :] = wo_ref[...].astype(jnp.float32)
    wo[...] = wf[0:CP, :].T.astype(jnp.bfloat16)
    wf[0:2 * channels, :] = wi_ref[...].astype(jnp.float32)
    keep = lax.broadcasted_iota(jnp.int32, (CP, 512), 0) < channels
    wi[0:CP, :] = jnp.where(keep, wf[0:CP, :], 0.0).astype(jnp.bfloat16)
    wi[CP:2 * CP, :] = wf[channels:channels + CP, :].astype(jnp.bfloat16)
    turn = (lax.broadcasted_iota(jnp.int32, (128, 128), 0) == lax.broadcasted_iota(jnp.int32, (128, 128), 1)).astype(jnp.float32).astype(jnp.bfloat16)

    def relayout(m, carry):
        @pl.when(m + 1 < members)
        def _():
            x_copy(m + 1).start()
        x_copy(m).wait()

        def widen(b, c2):
            for cc in range(32):
                xs[0, b // 4, b % 4, 17 * cc:17 * cc + 16, :] = xn[m % 2, b * 32 + cc].astype(jnp.float32)
            return c2
        lax.fori_loop(0, channels // 32, widen, 0)
        for cc in range(channels % 32):
            xs[0, 1, 3, 17 * cc:17 * cc + 16, :] = xn[m % 2, channels - channels % 32 + cc].astype(jnp.float32)
        for col in range(columns):
            part = jnp.concatenate([xs[0, h, j, pl.ds(col, 32, stride=17), :] for h in range(2) for j in range(4)], axis=0)
            out = lax.dot_general(turn, part.astype(jnp.bfloat16), NT, preferred_element_type=jnp.float32)
            for h in range(2):
                for j in range(4):
                    xs[1, h, j, pl.ds(col, 32, stride=17), :] = out[32 * j:32 * j + 32, h * 128:h * 128 + 128]

        def narrow(j, c2):
            for rr in range(32):
                for h in range(2):
                    xb[m, 32 * j + rr, :, h * 128:h * 128 + 128] = xs[1, h, j, 17 * rr:17 * rr + 16, :].astype(jnp.bfloat16)
            return c2
        lax.fori_loop(0, 4, narrow, 0)
        return carry
    lax.fori_loop(0, members, relayout, 0)
    pl.semaphore_wait(barrier, 4)

    lane = lax.broadcasted_iota(jnp.int32, (members, 128), 1)

    def setup():
        wf[0:128, 0:CP] = jnp.zeros((128, CP), jnp.float32)
        wf[0:32, 0:channels] = op_ref[...].astype(jnp.float32)
        opt = wf[0:128, 0:CP].T.astype(jnp.bfloat16)
        for j in range(8):
            place = (lax.broadcasted_iota(jnp.int32, (128, CP), 1) == lax.broadcasted_iota(jnp.int32, (128, CP), 0) + 32 * j)
            wobs[j * CP:(j + 1) * CP, :] = jnp.dot(opt, place.astype(jnp.bfloat16), preferred_element_type=jnp.float32).astype(jnp.bfloat16)
        for copy in obs_copies:
            copy.wait()
        sub8 = lax.broadcasted_iota(jnp.int32, (8, 128), 0)
        lane8 = lax.broadcasted_iota(jnp.int32, (8, 128), 1) // 32
        wf[0:8, 0:128] = jnp.zeros((8, 128), jnp.float32)

        def rows_of(patch, carry):
            for i in range(2):
                for g in range(8):
                    wf[0:8, 0:32] = obs_raw[i, patch, g % 4, 0, (g // 4) * 8:(g // 4) * 8 + 8, :]
                    v = wf[0:8, 0:128]
                    v = v + pltpu.roll(v, 32, 1)
                    v = v + pltpu.roll(v, 64, 1)
                    for q in range(2):
                        obs_row[i, patch, g:g + 1, q * 128:q * 128 + 128] = jnp.sum(jnp.where(sub8 == lane8 + 4 * q, v, 0.0), axis=0, keepdims=True)
            return carry
        lax.fori_loop(0, patches, rows_of, 0)

    def prepare(unit):
        slot = unit % 2
        patch, dslot = unit // ens_size, unit % ens_size
        first = dest_of(dslot) * dev_rows + patch * 4

        def convert(r, carry):
            row = jnp.minimum(jnp.maximum(first + r - 1, 0), rows - 1)
            for m in range(members):
                for h in range(2):
                    xs[slot, h, r, 33 * m + 8:33 * m + 24, :] = xb[m, row, :, h * 128:h * 128 + 128].astype(jnp.float32)
            return carry
        lax.fori_loop(0, 6, convert, 0)

        def edges(r, carry):
            for h in range(2):
                gsend[unit, 0, r, :, h * 128:h * 128 + 128] = xs[slot, h, r + 1, pl.ds(23, members, stride=33), :].astype(jnp.bfloat16)
                gsend[unit, 1, r, :, h * 128:h * 128 + 128] = xs[slot, h, r + 1, pl.ds(8, members, stride=33), :].astype(jnp.bfloat16)
            return carry
        lax.fori_loop(0, 4, edges, 0)
        ghost_copy(unit).start()

    def forecast(unit):
        patch, dslot = unit // ens_size, unit % ens_size
        slot = unit % 2
        out_slot = jnp.where(dslot < 3, (patch % 3) * 3 + dslot, 9)

        @pl.when((dslot < 3) & (patch >= 3))
        def _():
            for copy in unit_copies(patch - 3, dslot):
                copy.wait_send()
        ghost_copy(unit).wait_recv()

        def block(r, carry):
            for h in range(2):
                xs[slot, h, r + 1, pl.ds(7, members, stride=33), :] = grecv[unit, 0, r, :, h * 128:h * 128 + 128].astype(jnp.float32)
                xs[slot, h, r + 1, pl.ds(24, members, stride=33), :] = grecv[unit, 1, r, :, h * 128:h * 128 + 128].astype(jnp.float32)
            for m in range(members):
                b = 33 * m
                for h in range(2):
                    cur = xs[slot, h, r + 1, b + 8:b + 24, :]
                    north = xs[slot, h, r, b + 8:b + 24, :]
                    south = xs[slot, h, r + 2, b + 8:b + 24, :]
                    west = xs[slot, h, r + 1, b + 7:b + 23, :]
                    east = xs[slot, h, r + 1, b + 9:b + 25, :]
                    lap = north + south + west + east - 4.0 * cur
                    xl[16 * m:16 * m + 16, h * 128:h * 128 + 128] = cur.astype(jnp.bfloat16)
                    xl[16 * m:16 * m + 16, CP + h * 128:CP + h * 128 + 128] = lap.astype(jnp.bfloat16)
            hidden = jnp.dot(xl[...], wi[...], preferred_element_type=jnp.float32)
            gel = gelu(hidden).astype(jnp.bfloat16)
            inc = jnp.dot(gel, wo[...], preferred_element_type=jnp.float32)
            for m in range(members):
                for h in range(2):
                    ts[h, 17 * m:17 * m + 16, :] = xs[slot, h, r + 1, 33 * m + 8:33 * m + 24, :] + inc[16 * m:16 * m + 16, h * 128:h * 128 + 128]
            for col in range(columns):
                sb1[out_slot, r, col] = ts[0, pl.ds(col, members, stride=17), :].astype(jnp.bfloat16)
                t2[r, col] = ts[1, pl.ds(col, members, stride=17), :]
            return carry
        lax.fori_loop(0, 4, block, 0)

        @pl.when(dslot < 3)
        def _():
            def pack(pair, carry):
                left = jnp.zeros((members, 128), jnp.float32)
                for k in range(8):
                    r, c0 = pair * 2 + k // 4, (k % 4) * 4
                    v = [t2[r, c0 + i] for i in range(4)]
                    for i in range(3):
                        sb2[out_slot, pair * 25 + k * 3 + i] = jnp.where(lane < 96, v[i], pltpu.roll(v[3], 96 - 32 * i, 1)).astype(jnp.bfloat16)
                    for i in range(4):
                        left = left + pltpu.roll(jnp.where(lane >= 96, v[i], 0.0), (32 + 3 * (4 * k + i)) % 128, 1)
                sb2[out_slot, pair * 25 + 24] = left.astype(jnp.bfloat16)
                return carry
            lax.fori_loop(0, 2, pack, 0)
            for copy in unit_copies(patch, dslot):
                copy.start()

        @pl.when(dslot == 3)
        def _():
            def own(r, carry):
                for col in range(columns):
                    gath[patch, r, col, mine, 0:128] = sb1[9, r, col]
                    gath[patch, r, col, mine, 128:256] = t2[r, col].astype(jnp.bfloat16)
                return carry
            lax.fori_loop(0, 4, own, 0)

    def unpack(patch, dslot):
        src = pl.ds(pl.multiple_of(dest_of(dslot) * members, members), members)
        box = patch * 3 + dslot

        def half(pair, carry):
            left = rb[box, pair * 25 + 24].astype(jnp.float32)
            for k in range(8):
                r, c0 = pair * 2 + k // 4, (k % 4) * 4
                p = [rb[box, pair * 25 + k * 3 + i].astype(jnp.float32) for i in range(3)]
                tail = [jnp.where(lane < 99, pltpu.roll(left, (96 - 3 * (4 * k + i)) % 128, 1), 0.0) for i in range(4)]
                for i in range(3):
                    gath[patch, r, c0 + i, src, 128:256] = jnp.where(lane < 96, p[i], tail[i]).astype(jnp.bfloat16)
                last = jnp.where(lane < 64, jnp.where(lane < 32, pltpu.roll(p[0], 32, 1), pltpu.roll(p[1], 64, 1)),
                                 jnp.where(lane < 96, pltpu.roll(p[2], 96, 1), tail[3]))
                gath[patch, r, c0 + 3, src, 128:256] = last.astype(jnp.bfloat16)
            return carry
        lax.fori_loop(0, 2, half, 0)

    def analysis(patch):
        def arrive(dslot, carry):
            for copy in unit_copies(patch, dslot):
                copy.wait_recv()
            unpack(patch, dslot)
            return carry
        lax.fori_loop(0, 3, lambda i, c: arrive(2 - i, c), 0)
        gath_copy(patch).start()
        eye = (lax.broadcasted_iota(jnp.int32, (total_m, total_m), 0) == lax.broadcasted_iota(jnp.int32, (total_m, total_m), 1)).astype(jnp.float32)
        csum = jnp.zeros((total_m, CP), jnp.float32)
        for half in range(2):
            lhs = jnp.concatenate([gath[patch, :, half * 8 + j].reshape(4 * total_m, CP) for j in range(8)], axis=1)
            yb = jnp.dot(lhs, wobs[...], preferred_element_type=jnp.float32)
            for r in range(4):
                g = half * 4 + r
                y = yb[r * total_m:(r + 1) * total_m]
                ybar = jnp.sum(y, axis=0, keepdims=True) * (1.0 / total_m)
                y = y - ybar
                c = y * obs_row[1, patch, g:g + 1, :]
                csum = csum + c * (obs_row[0, patch, g:g + 1, :] - ybar)
                yp[g] = y
                cm[g] = c
        a_mat = (total_m - 1.0) * eye
        for g in range(8):
            a_mat = a_mat + f32dot(cm[g], yp[g], NT)
        amat[patch % 2, :, 0:total_m] = a_mat
        amat[patch % 2, :, total_m:2 * total_m] = a_mat
        cvec[patch % 2] = jnp.broadcast_to(jnp.sum(csum, axis=1, keepdims=True), (total_m, 2 * total_m))

    def solve(patch):
        row = lax.broadcasted_iota(jnp.int32, (total_m, 2 * total_m), 0)
        col = lax.broadcasted_iota(jnp.int32, (total_m, 2 * total_m), 1)
        eye = ((row == col) | (row + total_m == col)).astype(jnp.float32)
        mats = [amat[i] for i in range(2)]
        traces = [0.5 * jnp.sum(jnp.sum(a * eye, axis=0, keepdims=True), axis=1, keepdims=True) for a in mats]

        def newton(step, carry):
            out = []
            for y, z in carry:
                mix = 1.5 * eye - 0.5 * twin_dot(pair_lhs(z), pair_rhs(y))
                out.append((twin_dot(pair_lhs(y), pair_rhs(mix)), twin_dot(pair_lhs(mix), pair_rhs(z))))
            return tuple(out)
        pairs = lax.fori_loop(0, NS_STEPS, newton, tuple((a / t, eye) for a, t in zip(mats, traces)))
        for i in range(2):
            root = pairs[i][1] / jnp.sqrt(traces[i])
            left = pair_lhs(root)
            wbar = twin_dot(left, pair_rhs(twin_dot(left, pair_rhs(cvec[i]))))
            trans = math.sqrt(total_m - 1.0) * root + wbar
            trans = trans + (1.0 - jnp.sum(trans, axis=0, keepdims=True)) * (1.0 / total_m)
            tt_ref[patch + i] = trans[:, 0:total_m].T

    def step(v, carry):
        @pl.when(v < units)
        def _():
            prepare(v)

        @pl.when((v >= 1) & (v <= units))
        def _():
            forecast(v - 1)

        @pl.when(v == 3)
        def _():
            setup()

        @pl.when((v >= 12) & (v % 4 == 0))
        def _():
            analysis(v // 4 - 3)

        @pl.when((v >= 12) & (v % 8 == 0))
        def _():
            solve(v // 4 - 4)
        return carry
    lax.fori_loop(0, units + 9, step, 0)

    def finish(patch, carry):
        @pl.when(patch >= patches - 3)
        def _():
            for dslot in range(3):
                for copy in unit_copies(patch, dslot):
                    copy.wait_send()
        for dslot in range(4):
            ghost_copy(patch * 4 + dslot).wait_send()
        gath_copy(patch).wait()
        return carry
    lax.fori_loop(0, patches, finish, 0)


def update_kernel(tt_ref, g_ref, out_ref):
    hi, mid, low = split3(tt_ref[0])
    n = tt_ref.shape[1]
    zero = jnp.zeros((n, n), jnp.float32)
    lhs = jnp.concatenate([
        jnp.concatenate([hi.astype(jnp.float32), mid.astype(jnp.float32)], axis=1),
        jnp.concatenate([low.astype(jnp.float32), zero], axis=1)], axis=0).astype(jnp.bfloat16)

    def row(r, carry):
        for col in range(g_ref.shape[2]):
            g = g_ref[0, r, col]
            res = jnp.dot(lhs, jnp.concatenate([g, g], axis=0), preferred_element_type=jnp.float32)
            val = res[n:] + res[:n]
            out_ref[r, col] = val[:, :out_ref.shape[3]].astype(jnp.bfloat16)
        return carry
    lax.fori_loop(0, g_ref.shape[1], row, 0)


def solution(mesh):
    ens_size = mesh.shape["ens"]
    obs_spec = P(None, None, "dom", None, None)

    def local_step(ens_state, w_in, w_out, obs_op, obs_val, obs_wt):
        members, rows, columns, channels = ens_state.shape
        total_m = members * ens_size
        dev_rows = rows // ens_size
        patches = dev_rows // 4
        units = patches * ens_size
        dims = (members, rows, columns, channels, patches, dev_rows, ens_size)
        vmem = pl.BlockSpec(memory_space=pltpu.VMEM)
        anym = pl.BlockSpec(memory_space=pl.ANY)
        bf, f32 = jnp.bfloat16, jnp.float32
        dma = pltpu.SemaphoreType.DMA
        gathered, trans = pl.pallas_call(
            functools.partial(exchange_kernel, dims),
            out_shape=(jax.ShapeDtypeStruct((patches, 4, columns, total_m, CP), bf),
                       jax.ShapeDtypeStruct((patches, total_m, total_m), f32)),
            in_specs=[anym, vmem, vmem, vmem, anym, anym],
            out_specs=(anym, vmem),
            scratch_shapes=[
                pltpu.VMEM((2, channels, columns, rows), bf),
                pltpu.VMEM((members, rows, columns, CP), bf),
                pltpu.VMEM((2, 2, 6, 544, 128), f32),
                pltpu.VMEM((members * columns, 2 * CP), bf),
                pltpu.VMEM((2, members * 17, 128), f32),
                pltpu.VMEM((4, columns, members, 128), f32),
                pltpu.VMEM((10, 4, columns, members, 128), bf),
                pltpu.VMEM((9, 50, members, 128), bf),
                pltpu.VMEM((patches * 3, 50, members, 128), bf),
                pltpu.VMEM((patches, 4, columns, total_m, CP), bf),
                pltpu.VMEM((units, 2, 4, members, CP), bf),
                pltpu.VMEM((units, 2, 4, members, CP), bf),
                pltpu.VMEM((2 * CP, 512), bf),
                pltpu.VMEM((512, CP), bf),
                pltpu.VMEM((488, 512), f32),
                pltpu.VMEM((8 * CP, CP), bf),
                pltpu.VMEM((2, patches, 4, 1, columns, 32), f32),
                pltpu.VMEM((2, patches, 8, CP), f32),
                pltpu.VMEM((8, total_m, CP), f32),
                pltpu.VMEM((8, total_m, CP), f32),
                pltpu.VMEM((2, total_m, 2 * total_m), f32),
                pltpu.VMEM((2, total_m, 2 * total_m), f32),
                dma((2,)), dma((units,)), dma((units,)), dma((patches, 3, 2)), dma((patches, 3, 2)), dma((patches,)), dma((2,)),
            ],
            compiler_params=pltpu.CompilerParams(collective_id=0, has_side_effects=True, vmem_limit_bytes=62 * 1024 * 1024),
        )(ens_state.transpose(0, 3, 2, 1), w_in, w_out.T, obs_op.T, obs_val, obs_wt)
        return pl.pallas_call(
            update_kernel,
            grid=(patches,),
            out_shape=jax.ShapeDtypeStruct((dev_rows, columns, total_m, channels), bf),
            in_specs=[pl.BlockSpec((1, total_m, total_m), lambda p: (p, 0, 0)),
                      pl.BlockSpec((1, 4, columns, total_m, CP), lambda p: (p, 0, 0, 0, 0))],
            out_specs=pl.BlockSpec((4, columns, total_m, channels), lambda p: (p, 0, 0, 0)),
            compiler_params=pltpu.CompilerParams(dimension_semantics=("arbitrary",)),
        )(trans, gathered)

    return jax.shard_map(local_step, mesh=mesh, in_specs=(P("ens", None, "dom", None), P(), P(), P(), obs_spec, obs_spec), out_specs=P("ens", "dom", None, None), check_vma=False)
```

```python
import functools
import math
import jax
import jax.numpy as jnp
from jax import lax
from jax.experimental import pallas as pl
from jax.experimental.pallas import tpu as pltpu
from jax.sharding import PartitionSpec as P

NS_STEPS = 18
MESH = pl.DeviceIdType.MESH
CP = 256
NT = (((1,), (1,)), ((), ()))


NN = (((1,), (0,)), ((), ()))


def gelu(x):
    scale = math.sqrt(2.0 / math.pi)
    return (0.5 * x) * (1.0 + jnp.tanh(x * (scale + (scale * 0.044715) * (x * x))))


def split3(a):
    hi = a.astype(jnp.bfloat16)
    rem = a - hi.astype(jnp.float32)
    mid = rem.astype(jnp.bfloat16)
    low = (rem - mid.astype(jnp.float32)).astype(jnp.bfloat16)
    return hi, mid, low


def f32dot(a, b, dims=NN):
    ah, am, al = split3(a)
    bh, bm, bl = split3(b)
    n = a.shape[0]

    def dot(u, v):
        return lax.dot_general(u, v, dims, preferred_element_type=jnp.float32)
    by_hi = dot(jnp.concatenate([ah, am, al], axis=0), bh)
    by_mid = dot(jnp.concatenate([ah, am], axis=0), bm)
    by_low = dot(ah, bl)
    small = (by_low + by_hi[2 * n:]) + by_mid[n:]
    return (small + (by_mid[:n] + by_hi[n:2 * n])) + by_hi[:n]


def pair_lhs(a):
    hi, mid, low = split3(a)
    first = lax.broadcasted_iota(jnp.int32, a.shape, 1) < a.shape[1] // 2
    hi, mid, low = (v.astype(jnp.float32) for v in (hi, mid, low))
    lead = jnp.where(first, hi, mid).astype(jnp.bfloat16)
    return jnp.concatenate([lead, lead, jnp.where(first, hi, low).astype(jnp.bfloat16)], axis=1)


def pair_rhs(b):
    hi, mid, low = split3(b)
    return jnp.concatenate([hi, hi, mid, mid, low, hi], axis=0)


def twin_dot(lhs, rhs):
    k = rhs.shape[1]
    acc = jnp.dot(lhs[:, 2*k:], rhs[2*k:], preferred_element_type=jnp.float32)
    acc = acc + jnp.dot(lhs[:, k:2*k], rhs[k:2*k], preferred_element_type=jnp.float32)
    return acc + jnp.dot(lhs[:, :k], rhs[:k], preferred_element_type=jnp.float32)


def exchange_kernel(dims, xt_hbm, wi_ref, wo_ref, op_ref, yo_hbm, wt_hbm, gath, tt_ref,
                    xn, xb, xs, xl, ts, t2, sb1, sb2, rb, gsend, grecv, wi, wo, wf, wobs, obs_raw, obs_row, yp, cm, amat, cvec,
                    xsem, gssem, grsem, ssem, rsem, osem):
    members, rows, columns, channels, patches, dev_rows, ens_size = dims
    units = patches * ens_size
    total_m = members * ens_size
    me = lax.axis_index("ens")
    mydom = lax.axis_index("dom")
    my_x, my_core = me // 2, me % 2
    mine = pl.ds(pl.multiple_of(me * members, members), members)

    def dest_of(dslot):
        dx = (my_x + 1 - dslot // 2) % 2
        dc = (my_core + (dslot + 1) // 2) % 2
        return dx * 2 + dc

    def x_copy(m):
        return pltpu.make_async_copy(xt_hbm.at[m], xn.at[m % 2], xsem.at[m % 2])

    def ghost_copy(unit):
        return pltpu.make_async_remote_copy(
            src_ref=gsend.at[unit], dst_ref=grecv.at[unit], send_sem=gssem.at[unit], recv_sem=grsem.at[unit],
            device_id={"dom": 1 - mydom}, device_id_type=MESH)

    def unit_copies(patch, dslot):
        dev = {"ens": dest_of(dslot)}
        first = pltpu.make_async_remote_copy(
            src_ref=sb1.at[(patch % 3) * 3 + dslot], dst_ref=gath.at[patch, :, :, mine, pl.ds(0, 128)],
            send_sem=ssem.at[patch, dslot, 0], recv_sem=rsem.at[patch, dslot, 0],
            device_id=dev, device_id_type=MESH)
        second = pltpu.make_async_remote_copy(
            src_ref=sb2.at[(patch % 3) * 3 + dslot], dst_ref=rb.at[patch * 3 + dslot],
            send_sem=ssem.at[patch, dslot, 1], recv_sem=rsem.at[patch, dslot, 1],
            device_id=dev, device_id_type=MESH)
        return first, second

    obs_copies = [pltpu.make_async_copy(ref.at[pl.ds(me * patches, patches)], obs_raw.at[i], osem.at[i]) for i, ref in enumerate((yo_hbm, wt_hbm))]

    x_copy(0).start()
    for copy in obs_copies:
        copy.start()
    barrier = pltpu.get_barrier_semaphore()
    for dslot in range(3):
        pl.semaphore_signal(barrier, inc=1, device_id={"ens": dest_of(dslot)}, device_id_type=MESH)
    pl.semaphore_signal(barrier, inc=1, device_id={"dom": 1 - mydom}, device_id_type=MESH)

    xs[0, 1, 3, 17 * (channels % 32):544, :] = jnp.zeros((544 - 17 * (channels % 32), 128), jnp.float32)
    wf[...] = jnp.zeros_like(wf)
    wf[0:channels, :] = wo_ref[...].astype(jnp.float32)
    wo[...] = wf[0:CP, :].T.astype(jnp.bfloat16)
    wf[0:2 * channels, :] = wi_ref[...].astype(jnp.float32)
    keep = lax.broadcasted_iota(jnp.int32, (CP, 512), 0) < channels
    wi[0:CP, :] = jnp.where(keep, wf[0:CP, :], 0.0).astype(jnp.bfloat16)
    wi[CP:2 * CP, :] = wf[channels:channels + CP, :].astype(jnp.bfloat16)
    turn = (lax.broadcasted_iota(jnp.int32, (128, 128), 0) == lax.broadcasted_iota(jnp.int32, (128, 128), 1)).astype(jnp.float32).astype(jnp.bfloat16)

    def relayout(m, carry):
        @pl.when(m + 1 < members)
        def _():
            x_copy(m + 1).start()
        x_copy(m).wait()

        def widen(b, c2):
            for cc in range(32):
                xs[0, b // 4, b % 4, 17 * cc:17 * cc + 16, :] = xn[m % 2, b * 32 + cc].astype(jnp.float32)
            return c2
        lax.fori_loop(0, channels // 32, widen, 0)
        for cc in range(channels % 32):
            xs[0, 1, 3, 17 * cc:17 * cc + 16, :] = xn[m % 2, channels - channels % 32 + cc].astype(jnp.float32)
        for col in range(columns):
            part = jnp.concatenate([xs[0, h, j, pl.ds(col, 32, stride=17), :] for h in range(2) for j in range(4)], axis=0)
            out = lax.dot_general(turn, part.astype(jnp.bfloat16), NT, preferred_element_type=jnp.float32)
            for h in range(2):
                for j in range(4):
                    xs[1, h, j, pl.ds(col, 32, stride=17), :] = out[32 * j:32 * j + 32, h * 128:h * 128 + 128]

        def narrow(j, c2):
            for rr in range(32):
                for h in range(2):
                    xb[m, 32 * j + rr, :, h * 128:h * 128 + 128] = xs[1, h, j, 17 * rr:17 * rr + 16, :].astype(jnp.bfloat16)
            return c2
        lax.fori_loop(0, 4, narrow, 0)
        return carry
    lax.fori_loop(0, members, relayout, 0)
    pl.semaphore_wait(barrier, 4)

    lane = lax.broadcasted_iota(jnp.int32, (members, 128), 1)

    def setup():
        wf[0:128, 0:CP] = jnp.zeros((128, CP), jnp.float32)
        wf[0:32, 0:channels] = op_ref[...].astype(jnp.float32)
        opt = wf[0:128, 0:CP].T.astype(jnp.bfloat16)
        for j in range(8):
            place = (lax.broadcasted_iota(jnp.int32, (128, CP), 1) == lax.broadcasted_iota(jnp.int32, (128, CP), 0) + 32 * j)
            wobs[j * CP:(j + 1) * CP, :] = jnp.dot(opt, place.astype(jnp.bfloat16), preferred_element_type=jnp.float32).astype(jnp.bfloat16)
        for copy in obs_copies:
            copy.wait()
        sub8 = lax.broadcasted_iota(jnp.int32, (8, 128), 0)
        lane8 = lax.broadcasted_iota(jnp.int32, (8, 128), 1) // 32
        wf[0:8, 0:128] = jnp.zeros((8, 128), jnp.float32)

        def rows_of(patch, carry):
            for i in range(2):
                for g in range(8):
                    wf[0:8, 0:32] = obs_raw[i, patch, g % 4, 0, (g // 4) * 8:(g // 4) * 8 + 8, :]
                    v = wf[0:8, 0:128]
                    v = v + pltpu.roll(v, 32, 1)
                    v = v + pltpu.roll(v, 64, 1)
                    for q in range(2):
                        obs_row[i, patch, g:g + 1, q * 128:q * 128 + 128] = jnp.sum(jnp.where(sub8 == lane8 + 4 * q, v, 0.0), axis=0, keepdims=True)
            return carry
        lax.fori_loop(0, patches, rows_of, 0)

    def prepare(unit):
        slot = unit % 2
        patch, dslot = unit // ens_size, unit % ens_size
        first = dest_of(dslot) * dev_rows + patch * 4

        def convert(r, carry):
            row = jnp.minimum(jnp.maximum(first + r - 1, 0), rows - 1)
            for m in range(members):
                for h in range(2):
                    xs[slot, h, r, 33 * m + 8:33 * m + 24, :] = xb[m, row, :, h * 128:h * 128 + 128].astype(jnp.float32)
            return carry
        lax.fori_loop(0, 6, convert, 0)

        def edges(r, carry):
            for h in range(2):
                gsend[unit, 0, r, :, h * 128:h * 128 + 128] = xs[slot, h, r + 1, pl.ds(23, members, stride=33), :].astype(jnp.bfloat16)
                gsend[unit, 1, r, :, h * 128:h * 128 + 128] = xs[slot, h, r + 1, pl.ds(8, members, stride=33), :].astype(jnp.bfloat16)
            return carry
        lax.fori_loop(0, 4, edges, 0)
        ghost_copy(unit).start()

    def forecast(unit):
        patch, dslot = unit // ens_size, unit % ens_size
        slot = unit % 2
        out_slot = jnp.where(dslot < 3, (patch % 3) * 3 + dslot, 9)

        @pl.when((dslot < 3) & (patch >= 3))
        def _():
            for copy in unit_copies(patch - 3, dslot):
                copy.wait_send()
        ghost_copy(unit).wait_recv()

        def block(r, carry):
            for h in range(2):
                xs[slot, h, r + 1, pl.ds(7, members, stride=33), :] = grecv[unit, 0, r, :, h * 128:h * 128 + 128].astype(jnp.float32)
                xs[slot, h, r + 1, pl.ds(24, members, stride=33), :] = grecv[unit, 1, r, :, h * 128:h * 128 + 128].astype(jnp.float32)
            for m in range(members):
                b = 33 * m
                for h in range(2):
                    cur = xs[slot, h, r + 1, b + 8:b + 24, :]
                    north = xs[slot, h, r, b + 8:b + 24, :]
                    south = xs[slot, h, r + 2, b + 8:b + 24, :]
                    west = xs[slot, h, r + 1, b + 7:b + 23, :]
                    east = xs[slot, h, r + 1, b + 9:b + 25, :]
                    lap = north + south + west + east - 4.0 * cur
                    xl[16 * m:16 * m + 16, h * 128:h * 128 + 128] = cur.astype(jnp.bfloat16)
                    xl[16 * m:16 * m + 16, CP + h * 128:CP + h * 128 + 128] = lap.astype(jnp.bfloat16)
            hidden = jnp.dot(xl[...], wi[...], preferred_element_type=jnp.float32)
            gel = gelu(hidden).astype(jnp.bfloat16)
            inc = jnp.dot(gel, wo[...], preferred_element_type=jnp.float32)
            for m in range(members):
                for h in range(2):
                    ts[h, 17 * m:17 * m + 16, :] = xs[slot, h, r + 1, 33 * m + 8:33 * m + 24, :] + inc[16 * m:16 * m + 16, h * 128:h * 128 + 128]
            for col in range(columns):
                sb1[out_slot, r, col] = ts[0, pl.ds(col, members, stride=17), :].astype(jnp.bfloat16)
                t2[r, col] = ts[1, pl.ds(col, members, stride=17), :]
            return carry
        lax.fori_loop(0, 4, block, 0)

        @pl.when(dslot < 3)
        def _():
            def pack(pair, carry):
                left = jnp.zeros((members, 128), jnp.float32)
                for k in range(8):
                    r, c0 = pair * 2 + k // 4, (k % 4) * 4
                    v = [t2[r, c0 + i] for i in range(4)]
                    for i in range(3):
                        sb2[out_slot, pair * 25 + k * 3 + i] = jnp.where(lane < 96, v[i], pltpu.roll(v[3], 96 - 32 * i, 1)).astype(jnp.bfloat16)
                    for i in range(4):
                        left = left + pltpu.roll(jnp.where(lane >= 96, v[i], 0.0), (32 + 3 * (4 * k + i)) % 128, 1)
                sb2[out_slot, pair * 25 + 24] = left.astype(jnp.bfloat16)
                return carry
            lax.fori_loop(0, 2, pack, 0)
            for copy in unit_copies(patch, dslot):
                copy.start()

        @pl.when(dslot == 3)
        def _():
            def own(r, carry):
                for col in range(columns):
                    gath[patch, r, col, mine, 0:128] = sb1[9, r, col]
                    gath[patch, r, col, mine, 128:256] = t2[r, col].astype(jnp.bfloat16)
                return carry
            lax.fori_loop(0, 4, own, 0)

    def unpack(patch, dslot):
        src = pl.ds(pl.multiple_of(dest_of(dslot) * members, members), members)
        box = patch * 3 + dslot

        def half(pair, carry):
            left = rb[box, pair * 25 + 24].astype(jnp.float32)
            for k in range(8):
                r, c0 = pair * 2 + k // 4, (k % 4) * 4
                p = [rb[box, pair * 25 + k * 3 + i].astype(jnp.float32) for i in range(3)]
                tail = [jnp.where(lane < 99, pltpu.roll(left, (96 - 3 * (4 * k + i)) % 128, 1), 0.0) for i in range(4)]
                for i in range(3):
                    gath[patch, r, c0 + i, src, 128:256] = jnp.where(lane < 96, p[i], tail[i]).astype(jnp.bfloat16)
                last = jnp.where(lane < 64, jnp.where(lane < 32, pltpu.roll(p[0], 32, 1), pltpu.roll(p[1], 64, 1)),
                                 jnp.where(lane < 96, pltpu.roll(p[2], 96, 1), tail[3]))
                gath[patch, r, c0 + 3, src, 128:256] = last.astype(jnp.bfloat16)
            return carry
        lax.fori_loop(0, 2, half, 0)

    def analysis(patch):
        def arrive(dslot, carry):
            for copy in unit_copies(patch, dslot):
                copy.wait_recv()
            unpack(patch, dslot)
            return carry
        lax.fori_loop(0, 3, lambda i, c: arrive(2 - i, c), 0)
        eye = (lax.broadcasted_iota(jnp.int32, (total_m, total_m), 0) == lax.broadcasted_iota(jnp.int32, (total_m, total_m), 1)).astype(jnp.float32)
        csum = jnp.zeros((total_m, CP), jnp.float32)
        for half in range(2):
            lhs = jnp.concatenate([gath[patch, :, half * 8 + j].reshape(4 * total_m, CP) for j in range(8)], axis=1)
            yb = jnp.dot(lhs, wobs[...], preferred_element_type=jnp.float32)
            for r in range(4):
                g = half * 4 + r
                y = yb[r * total_m:(r + 1) * total_m]
                ybar = jnp.sum(y, axis=0, keepdims=True) * (1.0 / total_m)
                y = y - ybar
                c = y * obs_row[1, patch, g:g + 1, :]
                csum = csum + c * (obs_row[0, patch, g:g + 1, :] - ybar)
                yp[g] = y
                cm[g] = c
        a_mat = (total_m - 1.0) * eye
        for g in range(8):
            a_mat = a_mat + f32dot(cm[g], yp[g], NT)
        amat[patch % 2, :, 0:total_m] = a_mat
        amat[patch % 2, :, total_m:2 * total_m] = a_mat
        cvec[patch % 2] = jnp.broadcast_to(jnp.sum(csum, axis=1, keepdims=True), (total_m, 2 * total_m))

    def solve(patch):
        row = lax.broadcasted_iota(jnp.int32, (total_m, 2 * total_m), 0)
        col = lax.broadcasted_iota(jnp.int32, (total_m, 2 * total_m), 1)
        eye = ((row == col) | (row + total_m == col)).astype(jnp.float32)
        mats = [amat[i] for i in range(2)]
        traces = [0.5 * jnp.sum(jnp.sum(a * eye, axis=0, keepdims=True), axis=1, keepdims=True) for a in mats]

        def newton(step, carry):
            out = []
            for y, z in carry:
                mix = 1.5 * eye - 0.5 * twin_dot(pair_lhs(z), pair_rhs(y))
                out.append((twin_dot(pair_lhs(y), pair_rhs(mix)), twin_dot(pair_lhs(mix), pair_rhs(z))))
            return tuple(out)
        pairs = lax.fori_loop(0, NS_STEPS, newton, tuple((a / t, eye) for a, t in zip(mats, traces)))
        for i in range(2):
            root = pairs[i][1] / jnp.sqrt(traces[i])
            left = pair_lhs(root)
            wbar = twin_dot(left, pair_rhs(twin_dot(left, pair_rhs(cvec[i]))))
            trans = math.sqrt(total_m - 1.0) * root + wbar
            trans = trans + (1.0 - jnp.sum(trans, axis=0, keepdims=True)) * (1.0 / total_m)
            tt_ref[patch + i] = trans[:, 0:total_m].T

    def step(v, carry):
        @pl.when(v < units)
        def _():
            prepare(v)

        @pl.when((v >= 1) & (v <= units))
        def _():
            forecast(v - 1)

        @pl.when(v == 3)
        def _():
            setup()

        @pl.when((v >= 12) & (v % 4 == 0))
        def _():
            analysis(v // 4 - 3)

        @pl.when((v >= 12) & (v % 8 == 0))
        def _():
            solve(v // 4 - 4)
        return carry
    lax.fori_loop(0, units + 9, step, 0)

    def finish(patch, carry):
        @pl.when(patch >= patches - 3)
        def _():
            for dslot in range(3):
                for copy in unit_copies(patch, dslot):
                    copy.wait_send()
        for dslot in range(4):
            ghost_copy(patch * 4 + dslot).wait_send()
        return carry
    lax.fori_loop(0, patches, finish, 0)


def update_kernel(tt_ref, g_ref, out_ref):
    hi, mid, low = split3(tt_ref[pl.program_id(0)])
    n = tt_ref.shape[1]
    zero = jnp.zeros((n, n), jnp.float32)
    lhs = jnp.concatenate([
        jnp.concatenate([hi.astype(jnp.float32), mid.astype(jnp.float32)], axis=1),
        jnp.concatenate([low.astype(jnp.float32), zero], axis=1)], axis=0).astype(jnp.bfloat16)

    def row(r, carry):
        for col in range(out_ref.shape[1]):
            g = g_ref[pl.program_id(0), r, col]
            res = jnp.dot(lhs, jnp.concatenate([g, g], axis=0), preferred_element_type=jnp.float32)
            val = res[n:] + res[:n]
            out_ref[r, col] = val[:, :out_ref.shape[3]].astype(jnp.bfloat16)
        return carry
    lax.fori_loop(0, out_ref.shape[0], row, 0)


def solution(mesh):
    ens_size = mesh.shape["ens"]
    obs_spec = P(None, None, "dom", None, None)

    def local_step(ens_state, w_in, w_out, obs_op, obs_val, obs_wt):
        members, rows, columns, channels = ens_state.shape
        total_m = members * ens_size
        dev_rows = rows // ens_size
        patches = dev_rows // 4
        units = patches * ens_size
        dims = (members, rows, columns, channels, patches, dev_rows, ens_size)
        vmem = pl.BlockSpec(memory_space=pltpu.VMEM)
        anym = pl.BlockSpec(memory_space=pl.ANY)
        bf, f32 = jnp.bfloat16, jnp.float32
        dma = pltpu.SemaphoreType.DMA
        gathered, trans = pl.pallas_call(
            functools.partial(exchange_kernel, dims),
            out_shape=(pltpu.VMEM((patches, 4, columns, total_m, CP), bf),
                       pltpu.VMEM((patches, total_m, total_m), f32)),
            in_specs=[anym, vmem, vmem, vmem, anym, anym],
            out_specs=(vmem, vmem),
            scratch_shapes=[
                pltpu.VMEM((2, channels, columns, rows), bf),
                pltpu.VMEM((members, rows, columns, CP), bf),
                pltpu.VMEM((2, 2, 6, 544, 128), f32),
                pltpu.VMEM((members * columns, 2 * CP), bf),
                pltpu.VMEM((2, members * 17, 128), f32),
                pltpu.VMEM((4, columns, members, 128), f32),
                pltpu.VMEM((10, 4, columns, members, 128), bf),
                pltpu.VMEM((9, 50, members, 128), bf),
                pltpu.VMEM((patches * 3, 50, members, 128), bf),
                pltpu.VMEM((units, 2, 4, members, CP), bf),
                pltpu.VMEM((units, 2, 4, members, CP), bf),
                pltpu.VMEM((2 * CP, 512), bf),
                pltpu.VMEM((512, CP), bf),
                pltpu.VMEM((488, 512), f32),
                pltpu.VMEM((8 * CP, CP), bf),
                pltpu.VMEM((2, patches, 4, 1, columns, 32), f32),
                pltpu.VMEM((2, patches, 8, CP), f32),
                pltpu.VMEM((8, total_m, CP), f32),
                pltpu.VMEM((8, total_m, CP), f32),
                pltpu.VMEM((2, total_m, 2 * total_m), f32),
                pltpu.VMEM((2, total_m, 2 * total_m), f32),
                dma((2,)), dma((units,)), dma((units,)), dma((patches, 3, 2)), dma((patches, 3, 2)), dma((2,)),
            ],
            compiler_params=pltpu.CompilerParams(collective_id=0, has_side_effects=True, vmem_limit_bytes=44 * 1024 * 1024),
        )(ens_state.transpose(0, 3, 2, 1), w_in, w_out.T, obs_op.T, obs_val, obs_wt)
        return pl.pallas_call(
            update_kernel,
            grid=(patches,),
            out_shape=jax.ShapeDtypeStruct((dev_rows, columns, total_m, channels), bf),
            in_specs=[vmem, vmem],
            out_specs=pl.BlockSpec((4, columns, total_m, channels), lambda p: (p, 0, 0, 0)),
            compiler_params=pltpu.CompilerParams(dimension_semantics=("arbitrary",), vmem_limit_bytes=24 * 1024 * 1024),
        )(pltpu.with_memory_space_constraint(trans, pltpu.VMEM), pltpu.with_memory_space_constraint(gathered, pltpu.VMEM))

    return jax.shard_map(local_step, mesh=mesh, in_specs=(P("ens", None, "dom", None), P(), P(), P(), obs_spec, obs_spec), out_specs=P("ens", "dom", None, None), check_vma=False)
```

```python
import functools
import math
import jax
import jax.numpy as jnp
from jax import lax
from jax.experimental import pallas as pl
from jax.experimental.pallas import tpu as pltpu
from jax.sharding import PartitionSpec as P

NS_STEPS = 18
MESH = pl.DeviceIdType.MESH
CP = 256
NT = (((1,), (1,)), ((), ()))


NN = (((1,), (0,)), ((), ()))


def gelu(x):
    scale = math.sqrt(2.0 / math.pi)
    return (0.5 * x) * (1.0 + jnp.tanh(x * (scale + (scale * 0.044715) * (x * x))))


def split3(a):
    hi = a.astype(jnp.bfloat16)
    rem = a - hi.astype(jnp.float32)
    mid = rem.astype(jnp.bfloat16)
    low = (rem - mid.astype(jnp.float32)).astype(jnp.bfloat16)
    return hi, mid, low


def f32dot(a, b, dims=NN):
    ah, am, al = split3(a)
    bh, bm, bl = split3(b)
    n = a.shape[0]

    def dot(u, v):
        return lax.dot_general(u, v, dims, preferred_element_type=jnp.float32)
    by_hi = dot(jnp.concatenate([ah, am, al], axis=0), bh)
    by_mid = dot(jnp.concatenate([ah, am], axis=0), bm)
    by_low = dot(ah, bl)
    small = (by_low + by_hi[2 * n:]) + by_mid[n:]
    return (small + (by_mid[:n] + by_hi[n:2 * n])) + by_hi[:n]


def pair_lhs(a):
    hi, mid, low = split3(a)
    first = lax.broadcasted_iota(jnp.int32, a.shape, 1) < a.shape[1] // 2
    hi, mid, low = (v.astype(jnp.float32) for v in (hi, mid, low))
    lead = jnp.where(first, hi, mid).astype(jnp.bfloat16)
    return jnp.concatenate([lead, lead, jnp.where(first, hi, low).astype(jnp.bfloat16)], axis=1)


def pair_rhs(b):
    hi, mid, low = split3(b)
    return jnp.concatenate([hi, hi, mid, mid, low, hi], axis=0)


def twin_dot(lhs, rhs):
    k = rhs.shape[1]
    acc = jnp.dot(lhs[:, 2*k:], rhs[2*k:], preferred_element_type=jnp.float32)
    acc = acc + jnp.dot(lhs[:, k:2*k], rhs[k:2*k], preferred_element_type=jnp.float32)
    return acc + jnp.dot(lhs[:, :k], rhs[:k], preferred_element_type=jnp.float32)


def stacked(t):
    hi, mid, low = (v.astype(jnp.float32) for v in split3(t))
    return jnp.concatenate([
        jnp.concatenate([hi, mid], axis=1),
        jnp.concatenate([low, jnp.zeros_like(low)], axis=1)], axis=0).astype(jnp.bfloat16)


def transform(lhs, g):
    n = lhs.shape[0] // 2
    res = jnp.dot(lhs, jnp.concatenate([g, g], axis=0), preferred_element_type=jnp.float32)
    return (res[n:] + res[:n]).astype(jnp.bfloat16)


def exchange_kernel(dims, xt_hbm, wi_ref, wo_ref, op_ref, yo_hbm, wt_hbm, gath, tt_ref,
                    xn, xb, xs, xl, ts, t2, sb1, sb2, rb, gsend, grecv, wi, wo, wf, wobs, obs_raw, obs_row, yp, cm, amat, cvec,
                    xsem, gssem, grsem, ssem, rsem, osem):
    members, rows, columns, channels, patches, dev_rows, ens_size, done = dims
    units = patches * ens_size
    total_m = members * ens_size
    me = lax.axis_index("ens")
    mydom = lax.axis_index("dom")
    my_x, my_core = me // 2, me % 2
    mine = pl.ds(pl.multiple_of(me * members, members), members)

    def dest_of(dslot):
        dx = (my_x + 1 - dslot // 2) % 2
        dc = (my_core + (dslot + 1) // 2) % 2
        return dx * 2 + dc

    def x_copy(m):
        return pltpu.make_async_copy(xt_hbm.at[m], xn.at[m % 2], xsem.at[m % 2])

    def ghost_copy(unit):
        return pltpu.make_async_remote_copy(
            src_ref=gsend.at[unit], dst_ref=grecv.at[unit], send_sem=gssem.at[unit], recv_sem=grsem.at[unit],
            device_id={"dom": 1 - mydom}, device_id_type=MESH)

    def unit_copies(patch, dslot):
        dev = {"ens": dest_of(dslot)}
        first = pltpu.make_async_remote_copy(
            src_ref=sb1.at[(patch % 3) * 3 + dslot], dst_ref=gath.at[patch, :, :, mine, pl.ds(0, 128)],
            send_sem=ssem.at[patch, dslot, 0], recv_sem=rsem.at[patch, dslot, 0],
            device_id=dev, device_id_type=MESH)
        second = pltpu.make_async_remote_copy(
            src_ref=sb2.at[(patch % 3) * 3 + dslot], dst_ref=rb.at[patch * 3 + dslot],
            send_sem=ssem.at[patch, dslot, 1], recv_sem=rsem.at[patch, dslot, 1],
            device_id=dev, device_id_type=MESH)
        return first, second

    obs_copies = [pltpu.make_async_copy(ref.at[pl.ds(me * patches, patches)], obs_raw.at[i], osem.at[i]) for i, ref in enumerate((yo_hbm, wt_hbm))]

    x_copy(0).start()
    for copy in obs_copies:
        copy.start()
    barrier = pltpu.get_barrier_semaphore()
    for dslot in range(3):
        pl.semaphore_signal(barrier, inc=1, device_id={"ens": dest_of(dslot)}, device_id_type=MESH)
    pl.semaphore_signal(barrier, inc=1, device_id={"dom": 1 - mydom}, device_id_type=MESH)

    xs[0, 1, 3, 17 * (channels % 32):544, :] = jnp.zeros((544 - 17 * (channels % 32), 128), jnp.float32)
    wf[...] = jnp.zeros_like(wf)
    wf[0:channels, :] = wo_ref[...].astype(jnp.float32)
    wo[...] = wf[0:CP, :].T.astype(jnp.bfloat16)
    wf[0:2 * channels, :] = wi_ref[...].astype(jnp.float32)
    keep = lax.broadcasted_iota(jnp.int32, (CP, 512), 0) < channels
    wi[0:CP, :] = jnp.where(keep, wf[0:CP, :], 0.0).astype(jnp.bfloat16)
    wi[CP:2 * CP, :] = wf[channels:channels + CP, :].astype(jnp.bfloat16)
    turn = (lax.broadcasted_iota(jnp.int32, (128, 128), 0) == lax.broadcasted_iota(jnp.int32, (128, 128), 1)).astype(jnp.float32).astype(jnp.bfloat16)

    def relayout(m, carry):
        @pl.when(m + 1 < members)
        def _():
            x_copy(m + 1).start()
        x_copy(m).wait()

        def widen(b, c2):
            for cc in range(32):
                xs[0, b // 4, b % 4, 17 * cc:17 * cc + 16, :] = xn[m % 2, b * 32 + cc].astype(jnp.float32)
            return c2
        lax.fori_loop(0, channels // 32, widen, 0)
        for cc in range(channels % 32):
            xs[0, 1, 3, 17 * cc:17 * cc + 16, :] = xn[m % 2, channels - channels % 32 + cc].astype(jnp.float32)
        for col in range(columns):
            part = jnp.concatenate([xs[0, h, j, pl.ds(col, 32, stride=17), :] for h in range(2) for j in range(4)], axis=0)
            out = lax.dot_general(turn, part.astype(jnp.bfloat16), NT, preferred_element_type=jnp.float32)
            for h in range(2):
                for j in range(4):
                    xs[1, h, j, pl.ds(col, 32, stride=17), :] = out[32 * j:32 * j + 32, h * 128:h * 128 + 128]

        def narrow(j, c2):
            for rr in range(32):
                for h in range(2):
                    xb[m, 32 * j + rr, :, h * 128:h * 128 + 128] = xs[1, h, j, 17 * rr:17 * rr + 16, :].astype(jnp.bfloat16)
            return c2
        lax.fori_loop(0, 4, narrow, 0)
        return carry
    lax.fori_loop(0, members, relayout, 0)
    pl.semaphore_wait(barrier, 4)

    lane = lax.broadcasted_iota(jnp.int32, (members, 128), 1)

    def setup():
        wf[0:128, 0:CP] = jnp.zeros((128, CP), jnp.float32)
        wf[0:32, 0:channels] = op_ref[...].astype(jnp.float32)
        opt = wf[0:128, 0:CP].T.astype(jnp.bfloat16)
        for j in range(8):
            place = (lax.broadcasted_iota(jnp.int32, (128, CP), 1) == lax.broadcasted_iota(jnp.int32, (128, CP), 0) + 32 * j)
            wobs[j * CP:(j + 1) * CP, :] = jnp.dot(opt, place.astype(jnp.bfloat16), preferred_element_type=jnp.float32).astype(jnp.bfloat16)
        for copy in obs_copies:
            copy.wait()
        sub8 = lax.broadcasted_iota(jnp.int32, (8, 128), 0)
        lane8 = lax.broadcasted_iota(jnp.int32, (8, 128), 1) // 32
        wf[0:8, 0:128] = jnp.zeros((8, 128), jnp.float32)

        def rows_of(patch, carry):
            for i in range(2):
                for g in range(8):
                    wf[0:8, 0:32] = obs_raw[i, patch, g % 4, 0, (g // 4) * 8:(g // 4) * 8 + 8, :]
                    v = wf[0:8, 0:128]
                    v = v + pltpu.roll(v, 32, 1)
                    v = v + pltpu.roll(v, 64, 1)
                    for q in range(2):
                        obs_row[i, patch, g:g + 1, q * 128:q * 128 + 128] = jnp.sum(jnp.where(sub8 == lane8 + 4 * q, v, 0.0), axis=0, keepdims=True)
            return carry
        lax.fori_loop(0, patches, rows_of, 0)

    def prepare(unit):
        slot = unit % 2
        patch, dslot = unit // ens_size, unit % ens_size
        first = dest_of(dslot) * dev_rows + patch * 4

        def convert(r, carry):
            row = jnp.minimum(jnp.maximum(first + r - 1, 0), rows - 1)
            for m in range(members):
                for h in range(2):
                    xs[slot, h, r, 33 * m + 8:33 * m + 24, :] = xb[m, row, :, h * 128:h * 128 + 128].astype(jnp.float32)
            return carry
        lax.fori_loop(0, 6, convert, 0)

        def edges(r, carry):
            for h in range(2):
                gsend[unit, 0, r, :, h * 128:h * 128 + 128] = xs[slot, h, r + 1, pl.ds(23, members, stride=33), :].astype(jnp.bfloat16)
                gsend[unit, 1, r, :, h * 128:h * 128 + 128] = xs[slot, h, r + 1, pl.ds(8, members, stride=33), :].astype(jnp.bfloat16)
            return carry
        lax.fori_loop(0, 4, edges, 0)
        ghost_copy(unit).start()

    def forecast(unit):
        patch, dslot = unit // ens_size, unit % ens_size
        slot = unit % 2
        out_slot = jnp.where(dslot < 3, (patch % 3) * 3 + dslot, 9)

        @pl.when((dslot < 3) & (patch >= 3))
        def _():
            for copy in unit_copies(patch - 3, dslot):
                copy.wait_send()
        ghost_copy(unit).wait_recv()

        def block(r, carry):
            for h in range(2):
                xs[slot, h, r + 1, pl.ds(7, members, stride=33), :] = grecv[unit, 0, r, :, h * 128:h * 128 + 128].astype(jnp.float32)
                xs[slot, h, r + 1, pl.ds(24, members, stride=33), :] = grecv[unit, 1, r, :, h * 128:h * 128 + 128].astype(jnp.float32)
            for m in range(members):
                b = 33 * m
                for h in range(2):
                    cur = xs[slot, h, r + 1, b + 8:b + 24, :]
                    north = xs[slot, h, r, b + 8:b + 24, :]
                    south = xs[slot, h, r + 2, b + 8:b + 24, :]
                    west = xs[slot, h, r + 1, b + 7:b + 23, :]
                    east = xs[slot, h, r + 1, b + 9:b + 25, :]
                    lap = north + south + west + east - 4.0 * cur
                    xl[16 * m:16 * m + 16, h * 128:h * 128 + 128] = cur.astype(jnp.bfloat16)
                    xl[16 * m:16 * m + 16, CP + h * 128:CP + h * 128 + 128] = lap.astype(jnp.bfloat16)
            hidden = jnp.dot(xl[...], wi[...], preferred_element_type=jnp.float32)
            gel = gelu(hidden).astype(jnp.bfloat16)
            inc = jnp.dot(gel, wo[...], preferred_element_type=jnp.float32)
            for m in range(members):
                for h in range(2):
                    ts[h, 17 * m:17 * m + 16, :] = xs[slot, h, r + 1, 33 * m + 8:33 * m + 24, :] + inc[16 * m:16 * m + 16, h * 128:h * 128 + 128]
            for col in range(columns):
                sb1[out_slot, r, col] = ts[0, pl.ds(col, members, stride=17), :].astype(jnp.bfloat16)
                t2[r, col] = ts[1, pl.ds(col, members, stride=17), :]
            return carry
        lax.fori_loop(0, 4, block, 0)

        @pl.when(dslot < 3)
        def _():
            def pack(pair, carry):
                left = jnp.zeros((members, 128), jnp.float32)
                for k in range(8):
                    r, c0 = pair * 2 + k // 4, (k % 4) * 4
                    v = [t2[r, c0 + i] for i in range(4)]
                    for i in range(3):
                        sb2[out_slot, pair * 25 + k * 3 + i] = jnp.where(lane < 96, v[i], pltpu.roll(v[3], 96 - 32 * i, 1)).astype(jnp.bfloat16)
                    for i in range(4):
                        left = left + pltpu.roll(jnp.where(lane >= 96, v[i], 0.0), (32 + 3 * (4 * k + i)) % 128, 1)
                sb2[out_slot, pair * 25 + 24] = left.astype(jnp.bfloat16)
                return carry
            lax.fori_loop(0, 2, pack, 0)
            for copy in unit_copies(patch, dslot):
                copy.start()

        @pl.when(dslot == 3)
        def _():
            def own(r, carry):
                for col in range(columns):
                    gath[patch, r, col, mine, 0:128] = sb1[9, r, col]
                    gath[patch, r, col, mine, 128:256] = t2[r, col].astype(jnp.bfloat16)
                return carry
            lax.fori_loop(0, 4, own, 0)

    def unpack(patch, dslot):
        src = pl.ds(pl.multiple_of(dest_of(dslot) * members, members), members)
        box = patch * 3 + dslot

        def half(pair, carry):
            left = rb[box, pair * 25 + 24].astype(jnp.float32)
            for k in range(8):
                r, c0 = pair * 2 + k // 4, (k % 4) * 4
                p = [rb[box, pair * 25 + k * 3 + i].astype(jnp.float32) for i in range(3)]
                tail = [jnp.where(lane < 99, pltpu.roll(left, (96 - 3 * (4 * k + i)) % 128, 1), 0.0) for i in range(4)]
                for i in range(3):
                    gath[patch, r, c0 + i, src, 128:256] = jnp.where(lane < 96, p[i], tail[i]).astype(jnp.bfloat16)
                last = jnp.where(lane < 64, jnp.where(lane < 32, pltpu.roll(p[0], 32, 1), pltpu.roll(p[1], 64, 1)),
                                 jnp.where(lane < 96, pltpu.roll(p[2], 96, 1), tail[3]))
                gath[patch, r, c0 + 3, src, 128:256] = last.astype(jnp.bfloat16)
            return carry
        lax.fori_loop(0, 2, half, 0)

    def analysis(patch):
        def arrive(dslot, carry):
            for copy in unit_copies(patch, dslot):
                copy.wait_recv()
            unpack(patch, dslot)
            return carry
        lax.fori_loop(0, 3, lambda i, c: arrive(2 - i, c), 0)
        eye = (lax.broadcasted_iota(jnp.int32, (total_m, total_m), 0) == lax.broadcasted_iota(jnp.int32, (total_m, total_m), 1)).astype(jnp.float32)
        csum = jnp.zeros((total_m, CP), jnp.float32)
        for half in range(2):
            lhs = jnp.concatenate([gath[patch, :, half * 8 + j].reshape(4 * total_m, CP) for j in range(8)], axis=1)
            yb = jnp.dot(lhs, wobs[...], preferred_element_type=jnp.float32)
            for r in range(4):
                g = half * 4 + r
                y = yb[r * total_m:(r + 1) * total_m]
                ybar = jnp.sum(y, axis=0, keepdims=True) * (1.0 / total_m)
                y = y - ybar
                c = y * obs_row[1, patch, g:g + 1, :]
                csum = csum + c * (obs_row[0, patch, g:g + 1, :] - ybar)
                yp[g] = y
                cm[g] = c
        a_mat = (total_m - 1.0) * eye
        for g in range(8):
            a_mat = a_mat + f32dot(cm[g], yp[g], NT)
        amat[patch % 2, :, 0:total_m] = a_mat
        amat[patch % 2, :, total_m:2 * total_m] = a_mat
        cvec[patch % 2] = jnp.broadcast_to(jnp.sum(csum, axis=1, keepdims=True), (total_m, 2 * total_m))

    def solve(patch):
        row = lax.broadcasted_iota(jnp.int32, (total_m, 2 * total_m), 0)
        col = lax.broadcasted_iota(jnp.int32, (total_m, 2 * total_m), 1)
        eye = ((row == col) | (row + total_m == col)).astype(jnp.float32)
        mats = [amat[i] for i in range(2)]
        traces = [0.5 * jnp.sum(jnp.sum(a * eye, axis=0, keepdims=True), axis=1, keepdims=True) for a in mats]

        def newton(step, carry):
            out = []
            for y, z in carry:
                mix = 1.5 * eye - 0.5 * twin_dot(pair_lhs(z), pair_rhs(y))
                out.append((twin_dot(pair_lhs(y), pair_rhs(mix)), twin_dot(pair_lhs(mix), pair_rhs(z))))
            return tuple(out)
        pairs = lax.fori_loop(0, NS_STEPS, newton, tuple((a / t, eye) for a, t in zip(mats, traces)))
        for i in range(2):
            root = pairs[i][1] / jnp.sqrt(traces[i])
            left = pair_lhs(root)
            wbar = twin_dot(left, pair_rhs(twin_dot(left, pair_rhs(cvec[i]))))
            trans = math.sqrt(total_m - 1.0) * root + wbar
            trans = trans + (1.0 - jnp.sum(trans, axis=0, keepdims=True)) * (1.0 / total_m)
            tt_ref[patch + i] = trans[:, 0:total_m].T

        @pl.when(patch < done)
        def _():
            def apply(i, carry):
                lhs = stacked(tt_ref[patch + i // 4])
                for c in range(columns):
                    gath[patch + i // 4, i % 4, c] = transform(lhs, gath[patch + i // 4, i % 4, c])
                return carry
            lax.fori_loop(0, 8, apply, 0)

    def step(v, carry):
        @pl.when(v < units)
        def _():
            prepare(v)

        @pl.when((v >= 1) & (v <= units))
        def _():
            forecast(v - 1)

        @pl.when(v == 3)
        def _():
            setup()

        @pl.when((v >= 12) & (v % 4 == 0))
        def _():
            analysis(v // 4 - 3)

        @pl.when((v >= 12) & (v % 8 == 0))
        def _():
            solve(v // 4 - 4)
        return carry
    lax.fori_loop(0, units + 9, step, 0)

    def finish(patch, carry):
        @pl.when(patch >= patches - 3)
        def _():
            for dslot in range(3):
                for copy in unit_copies(patch, dslot):
                    copy.wait_send()
        for dslot in range(4):
            ghost_copy(patch * 4 + dslot).wait_send()
        return carry
    lax.fori_loop(0, patches, finish, 0)


def update_kernel(done, tt_ref, g_ref, out_ref):
    patch = pl.program_id(0)
    channels = out_ref.shape[3]

    @pl.when(patch < done)
    def _():
        def row(r, carry):
            for col in range(out_ref.shape[1]):
                out_ref[r, col] = g_ref[patch, r, col, :, 0:channels]
            return carry
        lax.fori_loop(0, out_ref.shape[0], row, 0)

    @pl.when(patch >= done)
    def _():
        lhs = stacked(tt_ref[patch])

        def row(r, carry):
            for col in range(out_ref.shape[1]):
                out_ref[r, col] = transform(lhs, g_ref[patch, r, col])[:, 0:channels]
            return carry
        lax.fori_loop(0, out_ref.shape[0], row, 0)


def solution(mesh):
    ens_size = mesh.shape["ens"]
    obs_spec = P(None, None, "dom", None, None)

    def local_step(ens_state, w_in, w_out, obs_op, obs_val, obs_wt):
        members, rows, columns, channels = ens_state.shape
        total_m = members * ens_size
        dev_rows = rows // ens_size
        patches = dev_rows // 4
        units = patches * ens_size
        done = patches - 2
        dims = (members, rows, columns, channels, patches, dev_rows, ens_size, done)
        vmem = pl.BlockSpec(memory_space=pltpu.VMEM)
        anym = pl.BlockSpec(memory_space=pl.ANY)
        bf, f32 = jnp.bfloat16, jnp.float32
        dma = pltpu.SemaphoreType.DMA
        gathered, trans = pl.pallas_call(
            functools.partial(exchange_kernel, dims),
            out_shape=(pltpu.VMEM((patches, 4, columns, total_m, CP), bf),
                       pltpu.VMEM((patches, total_m, total_m), f32)),
            in_specs=[anym, vmem, vmem, vmem, anym, anym],
            out_specs=(vmem, vmem),
            scratch_shapes=[
                pltpu.VMEM((2, channels, columns, rows), bf),
                pltpu.VMEM((members, rows, columns, CP), bf),
                pltpu.VMEM((2, 2, 6, 544, 128), f32),
                pltpu.VMEM((members * columns, 2 * CP), bf),
                pltpu.VMEM((2, members * 17, 128), f32),
                pltpu.VMEM((4, columns, members, 128), f32),
                pltpu.VMEM((10, 4, columns, members, 128), bf),
                pltpu.VMEM((9, 50, members, 128), bf),
                pltpu.VMEM((patches * 3, 50, members, 128), bf),
                pltpu.VMEM((units, 2, 4, members, CP), bf),
                pltpu.VMEM((units, 2, 4, members, CP), bf),
                pltpu.VMEM((2 * CP, 512), bf),
                pltpu.VMEM((512, CP), bf),
                pltpu.VMEM((488, 512), f32),
                pltpu.VMEM((8 * CP, CP), bf),
                pltpu.VMEM((2, patches, 4, 1, columns, 32), f32),
                pltpu.VMEM((2, patches, 8, CP), f32),
                pltpu.VMEM((8, total_m, CP), f32),
                pltpu.VMEM((8, total_m, CP), f32),
                pltpu.VMEM((2, total_m, 2 * total_m), f32),
                pltpu.VMEM((2, total_m, 2 * total_m), f32),
                dma((2,)), dma((units,)), dma((units,)), dma((patches, 3, 2)), dma((patches, 3, 2)), dma((2,)),
            ],
            compiler_params=pltpu.CompilerParams(collective_id=0, has_side_effects=True, vmem_limit_bytes=44 * 1024 * 1024),
        )(ens_state.transpose(0, 3, 2, 1), w_in, w_out.T, obs_op.T, obs_val, obs_wt)
        return pl.pallas_call(
            functools.partial(update_kernel, done),
            grid=(patches,),
            out_shape=jax.ShapeDtypeStruct((dev_rows, columns, total_m, channels), bf),
            in_specs=[vmem, vmem],
            out_specs=pl.BlockSpec((4, columns, total_m, channels), lambda p: (p, 0, 0, 0)),
            compiler_params=pltpu.CompilerParams(dimension_semantics=("arbitrary",), vmem_limit_bytes=24 * 1024 * 1024),
        )(pltpu.with_memory_space_constraint(trans, pltpu.VMEM), pltpu.with_memory_space_constraint(gathered, pltpu.VMEM))

    return jax.shard_map(local_step, mesh=mesh, in_specs=(P("ens", None, "dom", None), P(), P(), P(), obs_spec, obs_spec), out_specs=P("ens", "dom", None, None), check_vma=False)
```

```python
import functools
import math
import jax
import jax.numpy as jnp
from jax import lax
from jax.experimental import pallas as pl
from jax.experimental.pallas import tpu as pltpu
from jax.sharding import PartitionSpec as P

NS_STEPS = 18
MESH = pl.DeviceIdType.MESH
CP = 256
NT = (((1,), (1,)), ((), ()))


NN = (((1,), (0,)), ((), ()))


def gelu(x):
    scale = math.sqrt(2.0 / math.pi)
    return (0.5 * x) * (1.0 + jnp.tanh(x * (scale + (scale * 0.044715) * (x * x))))


def split3(a):
    hi = a.astype(jnp.bfloat16)
    rem = a - hi.astype(jnp.float32)
    mid = rem.astype(jnp.bfloat16)
    low = (rem - mid.astype(jnp.float32)).astype(jnp.bfloat16)
    return hi, mid, low


def f32dot(a, b, dims=NN):
    ah, am, al = split3(a)
    bh, bm, bl = split3(b)
    n = a.shape[0]

    def dot(u, v):
        return lax.dot_general(u, v, dims, preferred_element_type=jnp.float32)
    by_hi = dot(jnp.concatenate([ah, am, al], axis=0), bh)
    by_mid = dot(jnp.concatenate([ah, am], axis=0), bm)
    by_low = dot(ah, bl)
    small = (by_low + by_hi[2 * n:]) + by_mid[n:]
    return (small + (by_mid[:n] + by_hi[n:2 * n])) + by_hi[:n]


def pair_lhs(a):
    hi, mid, low = split3(a)
    first = lax.broadcasted_iota(jnp.int32, a.shape, 1) < a.shape[1] // 2
    hi, mid, low = (v.astype(jnp.float32) for v in (hi, mid, low))
    lead = jnp.where(first, hi, mid).astype(jnp.bfloat16)
    return jnp.concatenate([lead, lead, jnp.where(first, hi, low).astype(jnp.bfloat16)], axis=1)


def pair_rhs(b):
    hi, mid, low = split3(b)
    return jnp.concatenate([hi, hi, mid, mid, low, hi], axis=0)


def twin_dot(lhs, rhs):
    k = rhs.shape[1]
    acc = jnp.dot(lhs[:, 2*k:], rhs[2*k:], preferred_element_type=jnp.float32)
    acc = acc + jnp.dot(lhs[:, k:2*k], rhs[k:2*k], preferred_element_type=jnp.float32)
    return acc + jnp.dot(lhs[:, :k], rhs[:k], preferred_element_type=jnp.float32)


def stacked(t):
    hi, mid, low = (v.astype(jnp.float32) for v in split3(t))
    return jnp.concatenate([
        jnp.concatenate([hi, mid], axis=1),
        jnp.concatenate([low, jnp.zeros_like(low)], axis=1)], axis=0).astype(jnp.bfloat16)


def transform(lhs, g):
    n = lhs.shape[0] // 2
    res = jnp.dot(lhs, jnp.concatenate([g, g], axis=0), preferred_element_type=jnp.float32)
    return (res[n:] + res[:n]).astype(jnp.bfloat16)


def exchange_kernel(dims, xt_hbm, wi_ref, wo_ref, op_ref, yo_hbm, wt_hbm, gath, tt_ref,
                    xn, xb, xs, xl, ts, t2, sb1, sb2, rb, gsend, grecv, wi, wo, wf, wobs, obs_raw, obs_row, yp, cm, amat, cvec,
                    xsem, gssem, grsem, ssem, rsem, osem):
    members, rows, columns, channels, patches, dev_rows, ens_size, done = dims
    units = patches * ens_size
    total_m = members * ens_size
    me = lax.axis_index("ens")
    mydom = lax.axis_index("dom")
    my_x, my_core = me // 2, me % 2
    mine = pl.ds(pl.multiple_of(me * members, members), members)

    def dest_of(dslot):
        dx = (my_x + 1 - dslot // 2) % 2
        dc = (my_core + (dslot + 1) // 2) % 2
        return dx * 2 + dc

    def x_copy(m):
        return pltpu.make_async_copy(xt_hbm.at[m], xn.at[m % 2], xsem.at[m % 2])

    def ghost_copy(unit):
        return pltpu.make_async_remote_copy(
            src_ref=gsend.at[unit], dst_ref=grecv.at[unit], send_sem=gssem.at[unit], recv_sem=grsem.at[unit],
            device_id={"dom": 1 - mydom}, device_id_type=MESH)

    def unit_copies(patch, dslot):
        dev = {"ens": dest_of(dslot)}
        first = pltpu.make_async_remote_copy(
            src_ref=sb1.at[(patch % 3) * 3 + dslot], dst_ref=gath.at[patch, :, :, mine, pl.ds(0, 128)],
            send_sem=ssem.at[patch, dslot, 0], recv_sem=rsem.at[patch, dslot, 0],
            device_id=dev, device_id_type=MESH)
        second = pltpu.make_async_remote_copy(
            src_ref=sb2.at[(patch % 3) * 3 + dslot], dst_ref=rb.at[patch * 3 + dslot],
            send_sem=ssem.at[patch, dslot, 1], recv_sem=rsem.at[patch, dslot, 1],
            device_id=dev, device_id_type=MESH)
        return first, second

    obs_copies = [pltpu.make_async_copy(ref.at[pl.ds(me * patches, patches)], obs_raw.at[i], osem.at[i]) for i, ref in enumerate((yo_hbm, wt_hbm))]

    x_copy(0).start()
    for copy in obs_copies:
        copy.start()
    barrier = pltpu.get_barrier_semaphore()
    for dslot in range(3):
        pl.semaphore_signal(barrier, inc=1, device_id={"ens": dest_of(dslot)}, device_id_type=MESH)
    pl.semaphore_signal(barrier, inc=1, device_id={"dom": 1 - mydom}, device_id_type=MESH)

    xs[0, 1, 3, 17 * (channels % 32):544, :] = jnp.zeros((544 - 17 * (channels % 32), 128), jnp.float32)
    wf[...] = jnp.zeros_like(wf)
    wf[0:channels, :] = wo_ref[...].astype(jnp.float32)
    wo[...] = wf[0:CP, :].T.astype(jnp.bfloat16)
    wf[0:2 * channels, :] = wi_ref[...].astype(jnp.float32)
    keep = lax.broadcasted_iota(jnp.int32, (CP, 512), 0) < channels
    wi[0:CP, :] = jnp.where(keep, wf[0:CP, :], 0.0).astype(jnp.bfloat16)
    wi[CP:2 * CP, :] = wf[channels:channels + CP, :].astype(jnp.bfloat16)
    turn = (lax.broadcasted_iota(jnp.int32, (128, 128), 0) == lax.broadcasted_iota(jnp.int32, (128, 128), 1)).astype(jnp.float32).astype(jnp.bfloat16)

    def relayout(m, carry):
        @pl.when(m + 1 < members)
        def _():
            x_copy(m + 1).start()
        x_copy(m).wait()

        def widen(b, c2):
            for cc in range(32):
                xs[0, b // 4, b % 4, 17 * cc:17 * cc + 16, :] = xn[m % 2, b * 32 + cc].astype(jnp.float32)
            return c2
        lax.fori_loop(0, channels // 32, widen, 0)
        for cc in range(channels % 32):
            xs[0, 1, 3, 17 * cc:17 * cc + 16, :] = xn[m % 2, channels - channels % 32 + cc].astype(jnp.float32)
        for col in range(columns):
            part = jnp.concatenate([xs[0, h, j, pl.ds(col, 32, stride=17), :] for h in range(2) for j in range(4)], axis=0)
            out = lax.dot_general(turn, part.astype(jnp.bfloat16), NT, preferred_element_type=jnp.float32)
            for h in range(2):
                for j in range(4):
                    xs[1, h, j, pl.ds(col, 32, stride=17), :] = out[32 * j:32 * j + 32, h * 128:h * 128 + 128]

        def narrow(j, c2):
            for rr in range(32):
                for h in range(2):
                    xb[m, 32 * j + rr, :, h * 128:h * 128 + 128] = xs[1, h, j, 17 * rr:17 * rr + 16, :].astype(jnp.bfloat16)
            return c2
        lax.fori_loop(0, 4, narrow, 0)
        return carry
    lax.fori_loop(0, members, relayout, 0)
    pl.semaphore_wait(barrier, 4)

    lane = lax.broadcasted_iota(jnp.int32, (members, 128), 1)

    def setup():
        wf[0:128, 0:CP] = jnp.zeros((128, CP), jnp.float32)
        wf[0:32, 0:channels] = op_ref[...].astype(jnp.float32)
        opt = wf[0:128, 0:CP].T.astype(jnp.bfloat16)
        for j in range(8):
            place = (lax.broadcasted_iota(jnp.int32, (128, CP), 1) == lax.broadcasted_iota(jnp.int32, (128, CP), 0) + 32 * j)
            wobs[j * CP:(j + 1) * CP, :] = jnp.dot(opt, place.astype(jnp.bfloat16), preferred_element_type=jnp.float32).astype(jnp.bfloat16)
        for copy in obs_copies:
            copy.wait()
        sub8 = lax.broadcasted_iota(jnp.int32, (8, 128), 0)
        lane8 = lax.broadcasted_iota(jnp.int32, (8, 128), 1) // 32
        wf[0:8, 0:128] = jnp.zeros((8, 128), jnp.float32)

        def rows_of(patch, carry):
            for i in range(2):
                for g in range(8):
                    wf[0:8, 0:32] = obs_raw[i, patch, g % 4, 0, (g // 4) * 8:(g // 4) * 8 + 8, :]
                    v = wf[0:8, 0:128]
                    v = v + pltpu.roll(v, 32, 1)
                    v = v + pltpu.roll(v, 64, 1)
                    for q in range(2):
                        obs_row[i, patch, g:g + 1, q * 128:q * 128 + 128] = jnp.sum(jnp.where(sub8 == lane8 + 4 * q, v, 0.0), axis=0, keepdims=True)
            return carry
        lax.fori_loop(0, patches, rows_of, 0)

    def prepare(unit):
        slot = unit % 2
        patch, dslot = unit // ens_size, unit % ens_size
        first = dest_of(dslot) * dev_rows + patch * 4

        def convert(r, carry):
            row = jnp.minimum(jnp.maximum(first + r - 1, 0), rows - 1)
            for m in range(members):
                for h in range(2):
                    xs[slot, h, r, 33 * m + 8:33 * m + 24, :] = xb[m, row, :, h * 128:h * 128 + 128].astype(jnp.float32)
            return carry
        lax.fori_loop(0, 6, convert, 0)

        def edges(r, carry):
            for h in range(2):
                gsend[unit, 0, r, :, h * 128:h * 128 + 128] = xs[slot, h, r + 1, pl.ds(23, members, stride=33), :].astype(jnp.bfloat16)
                gsend[unit, 1, r, :, h * 128:h * 128 + 128] = xs[slot, h, r + 1, pl.ds(8, members, stride=33), :].astype(jnp.bfloat16)
            return carry
        lax.fori_loop(0, 4, edges, 0)
        ghost_copy(unit).start()

    def forecast(unit):
        patch, dslot = unit // ens_size, unit % ens_size
        slot = unit % 2
        out_slot = jnp.where(dslot < 3, (patch % 3) * 3 + dslot, 9)

        @pl.when((dslot < 3) & (patch >= 3))
        def _():
            for copy in unit_copies(patch - 3, dslot):
                copy.wait_send()
        ghost_copy(unit).wait_recv()

        def block(r, carry):
            for h in range(2):
                xs[slot, h, r + 1, pl.ds(7, members, stride=33), :] = grecv[unit, 0, r, :, h * 128:h * 128 + 128].astype(jnp.float32)
                xs[slot, h, r + 1, pl.ds(24, members, stride=33), :] = grecv[unit, 1, r, :, h * 128:h * 128 + 128].astype(jnp.float32)
            for m in range(members):
                b = 33 * m
                for h in range(2):
                    cur = xs[slot, h, r + 1, b + 8:b + 24, :]
                    north = xs[slot, h, r, b + 8:b + 24, :]
                    south = xs[slot, h, r + 2, b + 8:b + 24, :]
                    west = xs[slot, h, r + 1, b + 7:b + 23, :]
                    east = xs[slot, h, r + 1, b + 9:b + 25, :]
                    lap = north + south + west + east - 4.0 * cur
                    xl[16 * m:16 * m + 16, h * 128:h * 128 + 128] = cur.astype(jnp.bfloat16)
                    xl[16 * m:16 * m + 16, CP + h * 128:CP + h * 128 + 128] = lap.astype(jnp.bfloat16)
            hidden = jnp.dot(xl[...], wi[...], preferred_element_type=jnp.float32)
            gel = gelu(hidden).astype(jnp.bfloat16)
            inc = jnp.dot(gel, wo[...], preferred_element_type=jnp.float32)
            for m in range(members):
                for h in range(2):
                    ts[h, 17 * m:17 * m + 16, :] = xs[slot, h, r + 1, 33 * m + 8:33 * m + 24, :] + inc[16 * m:16 * m + 16, h * 128:h * 128 + 128]
            for col in range(columns):
                sb1[out_slot, r, col] = ts[0, pl.ds(col, members, stride=17), :].astype(jnp.bfloat16)
                t2[r, col] = ts[1, pl.ds(col, members, stride=17), :]
            return carry
        lax.fori_loop(0, 4, block, 0)

        @pl.when(dslot < 3)
        def _():
            def pack(pair, carry):
                left = jnp.zeros((members, 128), jnp.float32)
                for k in range(8):
                    r, c0 = pair * 2 + k // 4, (k % 4) * 4
                    v = [t2[r, c0 + i] for i in range(4)]
                    for i in range(3):
                        sb2[out_slot, pair * 25 + k * 3 + i] = jnp.where(lane < 96, v[i], pltpu.roll(v[3], 96 - 32 * i, 1)).astype(jnp.bfloat16)
                    for i in range(4):
                        left = left + pltpu.roll(jnp.where(lane >= 96, v[i], 0.0), (32 + 3 * (4 * k + i)) % 128, 1)
                sb2[out_slot, pair * 25 + 24] = left.astype(jnp.bfloat16)
                return carry
            lax.fori_loop(0, 2, pack, 0)
            for copy in unit_copies(patch, dslot):
                copy.start()

        @pl.when(dslot == 3)
        def _():
            def own(r, carry):
                for col in range(columns):
                    gath[patch, r, col, mine, 0:128] = sb1[9, r, col]
                    gath[patch, r, col, mine, 128:256] = t2[r, col].astype(jnp.bfloat16)
                return carry
            lax.fori_loop(0, 4, own, 0)

    def unpack(patch, dslot):
        src = pl.ds(pl.multiple_of(dest_of(dslot) * members, members), members)
        box = patch * 3 + dslot

        def half(pair, carry):
            left = rb[box, pair * 25 + 24].astype(jnp.float32)
            for k in range(8):
                r, c0 = pair * 2 + k // 4, (k % 4) * 4
                p = [rb[box, pair * 25 + k * 3 + i].astype(jnp.float32) for i in range(3)]
                tail = [jnp.where(lane < 99, pltpu.roll(left, (96 - 3 * (4 * k + i)) % 128, 1), 0.0) for i in range(4)]
                for i in range(3):
                    gath[patch, r, c0 + i, src, 128:256] = jnp.where(lane < 96, p[i], tail[i]).astype(jnp.bfloat16)
                last = jnp.where(lane < 64, jnp.where(lane < 32, pltpu.roll(p[0], 32, 1), pltpu.roll(p[1], 64, 1)),
                                 jnp.where(lane < 96, pltpu.roll(p[2], 96, 1), tail[3]))
                gath[patch, r, c0 + 3, src, 128:256] = last.astype(jnp.bfloat16)
            return carry
        lax.fori_loop(0, 2, half, 0)

    def analysis(patch):
        def arrive(dslot, carry):
            for copy in unit_copies(patch, dslot):
                copy.wait_recv()
            unpack(patch, dslot)
            return carry
        lax.fori_loop(0, 3, lambda i, c: arrive(2 - i, c), 0)
        eye = (lax.broadcasted_iota(jnp.int32, (total_m, total_m), 0) == lax.broadcasted_iota(jnp.int32, (total_m, total_m), 1)).astype(jnp.float32)
        csum = jnp.zeros((total_m, CP), jnp.float32)
        for half in range(2):
            lhs = jnp.concatenate([gath[patch, :, half * 8 + j].reshape(4 * total_m, CP) for j in range(8)], axis=1)
            yb = jnp.dot(lhs, wobs[...], preferred_element_type=jnp.float32)
            for r in range(4):
                g = half * 4 + r
                y = yb[r * total_m:(r + 1) * total_m]
                ybar = jnp.sum(y, axis=0, keepdims=True) * (1.0 / total_m)
                y = y - ybar
                c = y * obs_row[1, patch, g:g + 1, :]
                csum = csum + c * (obs_row[0, patch, g:g + 1, :] - ybar)
                yp[g] = y
                cm[g] = c
        a_mat = (total_m - 1.0) * eye
        for g in range(8):
            a_mat = a_mat + f32dot(cm[g], yp[g], NT)
        amat[patch % 2, :, 0:total_m] = a_mat
        amat[patch % 2, :, total_m:2 * total_m] = a_mat
        cvec[patch % 2] = jnp.broadcast_to(jnp.sum(csum, axis=1, keepdims=True), (total_m, 2 * total_m))

    def solve(patch, slots):
        row = lax.broadcasted_iota(jnp.int32, (total_m, 2 * total_m), 0)
        col = lax.broadcasted_iota(jnp.int32, (total_m, 2 * total_m), 1)
        eye = ((row == col) | (row + total_m == col)).astype(jnp.float32)
        mats = [amat[i] for i in slots]
        traces = [0.5 * jnp.sum(jnp.sum(a * eye, axis=0, keepdims=True), axis=1, keepdims=True) for a in mats]

        def newton(step, carry):
            out = []
            for y, z in carry:
                mix = 1.5 * eye - 0.5 * twin_dot(pair_lhs(z), pair_rhs(y))
                out.append((twin_dot(pair_lhs(y), pair_rhs(mix)), twin_dot(pair_lhs(mix), pair_rhs(z))))
            return tuple(out)
        pairs = lax.fori_loop(0, NS_STEPS, newton, tuple((a / t, eye) for a, t in zip(mats, traces)))
        for i, slot in enumerate(slots):
            root = pairs[i][1] / jnp.sqrt(traces[i])
            left = pair_lhs(root)
            wbar = twin_dot(left, pair_rhs(twin_dot(left, pair_rhs(cvec[slot]))))
            trans = math.sqrt(total_m - 1.0) * root + wbar
            trans = trans + (1.0 - jnp.sum(trans, axis=0, keepdims=True)) * (1.0 / total_m)
            tt_ref[patch + i] = trans[:, 0:total_m].T

        @pl.when(patch < done)
        def _():
            def apply(i, carry):
                lhs = stacked(tt_ref[patch + i // 4])
                for c in range(columns):
                    gath[patch + i // 4, i % 4, c] = transform(lhs, gath[patch + i // 4, i % 4, c])
                return carry
            lax.fori_loop(0, 4 * len(slots), apply, 0)

    def step(v, carry):
        @pl.when(v < units)
        def _():
            prepare(v)

        @pl.when((v >= 1) & (v <= units))
        def _():
            forecast(v - 1)

        @pl.when(v == 3)
        def _():
            setup()

        @pl.when((v >= 12) & (v % 4 == 0))
        def _():
            analysis(v // 4 - 3)

        @pl.when((v >= 12) & (v <= units) & (v % 8 == 0))
        def _():
            solve(v // 4 - 4, (0, 1))

        @pl.when((v > units) & (v % 4 == 0))
        def _():
            solve(v // 4 - 3, ((v // 4 - 3) % 2,))
        return carry
    lax.fori_loop(0, units + 9, step, 0)

    def finish(patch, carry):
        @pl.when(patch >= patches - 3)
        def _():
            for dslot in range(3):
                for copy in unit_copies(patch, dslot):
                    copy.wait_send()
        for dslot in range(4):
            ghost_copy(patch * 4 + dslot).wait_send()
        return carry
    lax.fori_loop(0, patches, finish, 0)


def update_kernel(done, tt_ref, g_ref, out_hbm, stage, sem):
    channels = out_hbm.shape[3]

    def copy(r):
        return pltpu.make_async_copy(stage.at[r], out_hbm.at[r], sem.at[r])

    def write(r, carry):
        for col in range(stage.shape[1]):
            stage[r, col] = g_ref[r // 4, r % 4, col, :, 0:channels]
        copy(r).start()
        return carry
    lax.fori_loop(0, 4 * done, write, 0)

    def last(r, carry):
        lhs = stacked(tt_ref[r // 4])
        for col in range(stage.shape[1]):
            stage[r, col] = transform(lhs, g_ref[r // 4, r % 4, col])[:, 0:channels]
        copy(r).start()
        return carry
    lax.fori_loop(4 * done, stage.shape[0], last, 0)

    def drain(r, carry):
        copy(r).wait()
        return carry
    lax.fori_loop(0, stage.shape[0], drain, 0)


def solution(mesh):
    ens_size = mesh.shape["ens"]
    obs_spec = P(None, None, "dom", None, None)

    def local_step(ens_state, w_in, w_out, obs_op, obs_val, obs_wt):
        members, rows, columns, channels = ens_state.shape
        total_m = members * ens_size
        dev_rows = rows // ens_size
        patches = dev_rows // 4
        units = patches * ens_size
        done = patches - 1
        dims = (members, rows, columns, channels, patches, dev_rows, ens_size, done)
        vmem = pl.BlockSpec(memory_space=pltpu.VMEM)
        anym = pl.BlockSpec(memory_space=pl.ANY)
        bf, f32 = jnp.bfloat16, jnp.float32
        dma = pltpu.SemaphoreType.DMA
        gathered, trans = pl.pallas_call(
            functools.partial(exchange_kernel, dims),
            out_shape=(pltpu.VMEM((patches, 4, columns, total_m, CP), bf),
                       pltpu.VMEM((patches, total_m, total_m), f32)),
            in_specs=[anym, vmem, vmem, vmem, anym, anym],
            out_specs=(vmem, vmem),
            scratch_shapes=[
                pltpu.VMEM((2, channels, columns, rows), bf),
                pltpu.VMEM((members, rows, columns, CP), bf),
                pltpu.VMEM((2, 2, 6, 544, 128), f32),
                pltpu.VMEM((members * columns, 2 * CP), bf),
                pltpu.VMEM((2, members * 17, 128), f32),
                pltpu.VMEM((4, columns, members, 128), f32),
                pltpu.VMEM((10, 4, columns, members, 128), bf),
                pltpu.VMEM((9, 50, members, 128), bf),
                pltpu.VMEM((patches * 3, 50, members, 128), bf),
                pltpu.VMEM((units, 2, 4, members, CP), bf),
                pltpu.VMEM((units, 2, 4, members, CP), bf),
                pltpu.VMEM((2 * CP, 512), bf),
                pltpu.VMEM((512, CP), bf),
                pltpu.VMEM((488, 512), f32),
                pltpu.VMEM((8 * CP, CP), bf),
                pltpu.VMEM((2, patches, 4, 1, columns, 32), f32),
                pltpu.VMEM((2, patches, 8, CP), f32),
                pltpu.VMEM((8, total_m, CP), f32),
                pltpu.VMEM((8, total_m, CP), f32),
                pltpu.VMEM((2, total_m, 2 * total_m), f32),
                pltpu.VMEM((2, total_m, 2 * total_m), f32),
                dma((2,)), dma((units,)), dma((units,)), dma((patches, 3, 2)), dma((patches, 3, 2)), dma((2,)),
            ],
            compiler_params=pltpu.CompilerParams(collective_id=0, has_side_effects=True, vmem_limit_bytes=44 * 1024 * 1024),
        )(ens_state.transpose(0, 3, 2, 1), w_in, w_out.T, obs_op.T, obs_val, obs_wt)
        return pl.pallas_call(
            functools.partial(update_kernel, done),
            out_shape=jax.ShapeDtypeStruct((dev_rows, columns, total_m, channels), bf),
            in_specs=[vmem, vmem],
            out_specs=anym,
            scratch_shapes=[pltpu.VMEM((dev_rows, columns, total_m, channels), bf), dma((dev_rows,))],
            compiler_params=pltpu.CompilerParams(vmem_limit_bytes=24 * 1024 * 1024),
        )(pltpu.with_memory_space_constraint(trans, pltpu.VMEM), pltpu.with_memory_space_constraint(gathered, pltpu.VMEM))

    return jax.shard_map(local_step, mesh=mesh, in_specs=(P("ens", None, "dom", None), P(), P(), P(), obs_spec, obs_spec), out_specs=P("ens", "dom", None, None), check_vma=False)
```

```python
import functools
import math
import jax
import jax.numpy as jnp
from jax import lax
from jax.experimental import pallas as pl
from jax.experimental.pallas import tpu as pltpu
from jax.sharding import PartitionSpec as P

NS_STEPS = 18
MESH = pl.DeviceIdType.MESH
CP = 256
NT = (((1,), (1,)), ((), ()))


NN = (((1,), (0,)), ((), ()))


def gelu(x):
    scale = math.sqrt(2.0 / math.pi)
    return (0.5 * x) * (1.0 + jnp.tanh(x * (scale + (scale * 0.044715) * (x * x))))


def split3(a):
    hi = a.astype(jnp.bfloat16)
    rem = a - hi.astype(jnp.float32)
    mid = rem.astype(jnp.bfloat16)
    low = (rem - mid.astype(jnp.float32)).astype(jnp.bfloat16)
    return hi, mid, low


def f32dot(a, b, dims=NN):
    ah, am, al = split3(a)
    bh, bm, bl = split3(b)
    n = a.shape[0]

    def dot(u, v):
        return lax.dot_general(u, v, dims, preferred_element_type=jnp.float32)
    by_hi = dot(jnp.concatenate([ah, am, al], axis=0), bh)
    by_mid = dot(jnp.concatenate([ah, am], axis=0), bm)
    by_low = dot(ah, bl)
    small = (by_low + by_hi[2 * n:]) + by_mid[n:]
    return (small + (by_mid[:n] + by_hi[n:2 * n])) + by_hi[:n]


def pair_lhs(a):
    hi, mid, low = split3(a)
    first = lax.broadcasted_iota(jnp.int32, a.shape, 1) < a.shape[1] // 2
    hi, mid, low = (v.astype(jnp.float32) for v in (hi, mid, low))
    lead = jnp.where(first, hi, mid).astype(jnp.bfloat16)
    return jnp.concatenate([lead, lead, jnp.where(first, hi, low).astype(jnp.bfloat16)], axis=1)


def pair_rhs(b):
    hi, mid, low = split3(b)
    return jnp.concatenate([hi, hi, mid, mid, low, hi], axis=0)


def twin_dot(lhs, rhs):
    k = rhs.shape[1]
    acc = jnp.dot(lhs[:, 2*k:], rhs[2*k:], preferred_element_type=jnp.float32)
    acc = acc + jnp.dot(lhs[:, k:2*k], rhs[k:2*k], preferred_element_type=jnp.float32)
    return acc + jnp.dot(lhs[:, :k], rhs[:k], preferred_element_type=jnp.float32)


def stacked(t):
    hi, mid, low = (v.astype(jnp.float32) for v in split3(t))
    return jnp.concatenate([
        jnp.concatenate([hi, mid], axis=1),
        jnp.concatenate([low, jnp.zeros_like(low)], axis=1)], axis=0).astype(jnp.bfloat16)


def transform(lhs, g):
    n = lhs.shape[0] // 2
    res = jnp.dot(lhs, jnp.concatenate([g, g], axis=0), preferred_element_type=jnp.float32)
    return (res[n:] + res[:n]).astype(jnp.bfloat16)


def exchange_kernel(dims, xt_hbm, wi_ref, wo_ref, op_ref, yo_hbm, wt_hbm, gath, tt_ref,
                    xn, xb, xs, xa, xl, ts, t2, sb1, sb2, rb, gsend, grecv, wi, wo, wf, wobs, obs_raw, obs_row, yp, cm, amat, cvec,
                    xsem, gssem, grsem, ssem, rsem, osem):
    members, rows, columns, channels, patches, dev_rows, ens_size, done = dims
    units = patches * ens_size
    total_m = members * ens_size
    me = lax.axis_index("ens")
    mydom = lax.axis_index("dom")
    my_x, my_core = me // 2, me % 2
    mine = pl.ds(pl.multiple_of(me * members, members), members)

    def dest_of(dslot):
        dx = (my_x + 1 - dslot // 2) % 2
        dc = (my_core + (dslot + 1) // 2) % 2
        return dx * 2 + dc

    def x_copy(m):
        return pltpu.make_async_copy(xt_hbm.at[m], xn.at[m % 2], xsem.at[m % 2])

    def ghost_copy(unit):
        return pltpu.make_async_remote_copy(
            src_ref=gsend.at[unit], dst_ref=grecv.at[unit], send_sem=gssem.at[unit], recv_sem=grsem.at[unit],
            device_id={"dom": 1 - mydom}, device_id_type=MESH)

    def unit_copies(patch, dslot):
        dev = {"ens": dest_of(dslot)}
        first = pltpu.make_async_remote_copy(
            src_ref=sb1.at[(patch % 2) * 3 + dslot], dst_ref=gath.at[patch, :, :, mine, pl.ds(0, 128)],
            send_sem=ssem.at[patch, dslot, 0], recv_sem=rsem.at[patch, dslot, 0],
            device_id=dev, device_id_type=MESH)
        second = pltpu.make_async_remote_copy(
            src_ref=sb2.at[(patch % 2) * 3 + dslot], dst_ref=rb.at[patch * 3 + dslot],
            send_sem=ssem.at[patch, dslot, 1], recv_sem=rsem.at[patch, dslot, 1],
            device_id=dev, device_id_type=MESH)
        return first, second

    obs_copies = [pltpu.make_async_copy(ref.at[pl.ds(me * patches, patches)], obs_raw.at[i], osem.at[i]) for i, ref in enumerate((yo_hbm, wt_hbm))]

    x_copy(0).start()
    x_copy(1).start()
    for copy in obs_copies:
        copy.start()
    barrier = pltpu.get_barrier_semaphore()
    for dslot in range(3):
        pl.semaphore_signal(barrier, inc=1, device_id={"ens": dest_of(dslot)}, device_id_type=MESH)
    pl.semaphore_signal(barrier, inc=1, device_id={"dom": 1 - mydom}, device_id_type=MESH)

    wf[...] = jnp.zeros_like(wf)
    wf[0:channels, :] = wo_ref[...].astype(jnp.float32)
    wo[...] = wf[0:CP, :].T.astype(jnp.bfloat16)
    wf[0:2 * channels, :] = wi_ref[...].astype(jnp.float32)
    keep = lax.broadcasted_iota(jnp.int32, (CP, 512), 0) < channels
    wi[0:CP, :] = jnp.where(keep, wf[0:CP, :], 0.0).astype(jnp.bfloat16)
    wi[CP:2 * CP, :] = wf[channels:channels + CP, :].astype(jnp.bfloat16)
    turn = (lax.broadcasted_iota(jnp.int32, (128, 128), 0) == lax.broadcasted_iota(jnp.int32, (128, 128), 1)).astype(jnp.float32).astype(jnp.bfloat16)

    wide = ([[xs.at[0, h, j] for j in range(4)] for h in range(2)],
            [[xs.at[j // 2, h, 4 + j % 2] for j in range(4)] for h in range(2)])
    turned = ([[xs.at[1, h, j] for j in range(4)] for h in range(2)],
              [[xa.at[h, j] for j in range(4)] for h in range(2)])

    def widen(odd, c):
        wide[odd][c // 128][c // 32 % 4][17 * (c % 32):17 * (c % 32) + 16, :] = xn[odd, c].astype(jnp.float32)

    def turn_column(odd, col):
        part = jnp.concatenate([wide[odd][h][j][pl.ds(col, 32, stride=17), :] for h in range(2) for j in range(4)], axis=0)
        out = lax.dot_general(turn, part.astype(jnp.bfloat16), NT, preferred_element_type=jnp.float32)
        for h in range(2):
            for j in range(4):
                turned[odd][h][j][pl.ds(col, 32, stride=17), :] = out[32 * j:32 * j + 32, h * 128:h * 128 + 128]

    def narrow(odd, m, row):
        for h in range(2):
            xb[m, row, :, h * 128:h * 128 + 128] = turned[odd][h][row // 32][17 * (row % 32):17 * (row % 32) + 16, :].astype(jnp.bfloat16)

    def relayout(t, carry):
        for odd in range(2):
            m = 2 * t + odd

            @pl.when(m + 2 < members)
            def _():
                x_copy(m + 2).start()

            @pl.when(m + 1 < members)
            def _():
                x_copy(m + 1).wait()
            for col in range(columns):
                turn_column(odd, col)
                for c in range(channels * col // columns, channels * (col + 1) // columns):
                    widen(1 - odd, c)
                for row in range(rows * col // columns, rows * (col + 1) // columns):
                    narrow(1 - odd, jnp.maximum(m - 1, 0), row)
        return carry
    for ref in (wide[0][1][3], wide[1][1][3]):
        ref[17 * (channels % 32):544, :] = jnp.zeros((544 - 17 * (channels % 32), 128), jnp.float32)
    x_copy(0).wait()
    for c in range(channels):
        widen(0, c)
    lax.fori_loop(0, members // 2, relayout, 0)

    for row in range(rows):
        narrow(1, members - 1, row)
    pl.semaphore_wait(barrier, 4)

    lane = lax.broadcasted_iota(jnp.int32, (members, 128), 1)

    def setup():
        wf[0:128, 0:CP] = jnp.zeros((128, CP), jnp.float32)
        wf[0:32, 0:channels] = op_ref[...].astype(jnp.float32)
        opt = wf[0:128, 0:CP].T.astype(jnp.bfloat16)
        for j in range(8):
            place = (lax.broadcasted_iota(jnp.int32, (128, CP), 1) == lax.broadcasted_iota(jnp.int32, (128, CP), 0) + 32 * j)
            wobs[j * CP:(j + 1) * CP, :] = jnp.dot(opt, place.astype(jnp.bfloat16), preferred_element_type=jnp.float32).astype(jnp.bfloat16)
        for copy in obs_copies:
            copy.wait()
        sub8 = lax.broadcasted_iota(jnp.int32, (8, 128), 0)
        lane8 = lax.broadcasted_iota(jnp.int32, (8, 128), 1) // 32
        wf[0:8, 0:128] = jnp.zeros((8, 128), jnp.float32)

        def rows_of(patch, carry):
            for i in range(2):
                for g in range(8):
                    wf[0:8, 0:32] = obs_raw[i, patch, g % 4, 0, (g // 4) * 8:(g // 4) * 8 + 8, :]
                    v = wf[0:8, 0:128]
                    v = v + pltpu.roll(v, 32, 1)
                    v = v + pltpu.roll(v, 64, 1)
                    for q in range(2):
                        obs_row[i, patch, g:g + 1, q * 128:q * 128 + 128] = jnp.sum(jnp.where(sub8 == lane8 + 4 * q, v, 0.0), axis=0, keepdims=True)
            return carry
        lax.fori_loop(0, patches, rows_of, 0)

    def prepare(unit):
        slot = unit % 2
        patch, dslot = unit // ens_size, unit % ens_size
        first = dest_of(dslot) * dev_rows + patch * 4

        def convert(r, carry):
            row = jnp.minimum(jnp.maximum(first + r - 1, 0), rows - 1)
            for m in range(members):
                for h in range(2):
                    xs[slot, h, r, 33 * m + 8:33 * m + 24, :] = xb[m, row, :, h * 128:h * 128 + 128].astype(jnp.float32)
            return carry
        lax.fori_loop(0, 6, convert, 0)

        def edges(r, carry):
            for h in range(2):
                gsend[unit, 0, r, :, h * 128:h * 128 + 128] = xs[slot, h, r + 1, pl.ds(23, members, stride=33), :].astype(jnp.bfloat16)
                gsend[unit, 1, r, :, h * 128:h * 128 + 128] = xs[slot, h, r + 1, pl.ds(8, members, stride=33), :].astype(jnp.bfloat16)
            return carry
        lax.fori_loop(0, 4, edges, 0)
        ghost_copy(unit).start()

    def forecast(unit):
        patch, dslot = unit // ens_size, unit % ens_size
        slot = unit % 2
        out_slot = jnp.where(dslot < 3, (patch % 2) * 3 + dslot, 6)

        @pl.when((dslot < 3) & (patch >= 2))
        def _():
            for copy in unit_copies(patch - 2, dslot):
                copy.wait_send()
        ghost_copy(unit).wait_recv()

        def block(r, carry):
            for h in range(2):
                xs[slot, h, r + 1, pl.ds(7, members, stride=33), :] = grecv[unit, 0, r, :, h * 128:h * 128 + 128].astype(jnp.float32)
                xs[slot, h, r + 1, pl.ds(24, members, stride=33), :] = grecv[unit, 1, r, :, h * 128:h * 128 + 128].astype(jnp.float32)
            for m in range(members):
                b = 33 * m
                for h in range(2):
                    cur = xs[slot, h, r + 1, b + 8:b + 24, :]
                    north = xs[slot, h, r, b + 8:b + 24, :]
                    south = xs[slot, h, r + 2, b + 8:b + 24, :]
                    west = xs[slot, h, r + 1, b + 7:b + 23, :]
                    east = xs[slot, h, r + 1, b + 9:b + 25, :]
                    lap = north + south + west + east - 4.0 * cur
                    xl[16 * m:16 * m + 16, h * 128:h * 128 + 128] = cur.astype(jnp.bfloat16)
                    xl[16 * m:16 * m + 16, CP + h * 128:CP + h * 128 + 128] = lap.astype(jnp.bfloat16)
            hidden = jnp.dot(xl[...], wi[...], preferred_element_type=jnp.float32)
            gel = gelu(hidden).astype(jnp.bfloat16)
            inc = jnp.dot(gel, wo[...], preferred_element_type=jnp.float32)
            for m in range(members):
                for h in range(2):
                    ts[h, 17 * m:17 * m + 16, :] = xs[slot, h, r + 1, 33 * m + 8:33 * m + 24, :] + inc[16 * m:16 * m + 16, h * 128:h * 128 + 128]
            for col in range(columns):
                sb1[out_slot, r, col] = ts[0, pl.ds(col, members, stride=17), :].astype(jnp.bfloat16)
                t2[r, col] = ts[1, pl.ds(col, members, stride=17), :]
            return carry
        lax.fori_loop(0, 4, block, 0)

        @pl.when(dslot < 3)
        def _():
            def pack(pair, carry):
                left = jnp.zeros((members, 128), jnp.float32)
                for k in range(8):
                    r, c0 = pair * 2 + k // 4, (k % 4) * 4
                    v = [t2[r, c0 + i] for i in range(4)]
                    for i in range(3):
                        sb2[out_slot, pair * 25 + k * 3 + i] = jnp.where(lane < 96, v[i], pltpu.roll(v[3], 96 - 32 * i, 1)).astype(jnp.bfloat16)
                    for i in range(4):
                        left = left + pltpu.roll(jnp.where(lane >= 96, v[i], 0.0), (32 + 3 * (4 * k + i)) % 128, 1)
                sb2[out_slot, pair * 25 + 24] = left.astype(jnp.bfloat16)
                return carry
            lax.fori_loop(0, 2, pack, 0)
            for copy in unit_copies(patch, dslot):
                copy.start()

        @pl.when(dslot == 3)
        def _():
            def own(r, carry):
                for col in range(columns):
                    gath[patch, r, col, mine, 0:128] = sb1[6, r, col]
                    gath[patch, r, col, mine, 128:256] = t2[r, col].astype(jnp.bfloat16)
                return carry
            lax.fori_loop(0, 4, own, 0)

    def unpack(patch, dslot):
        src = pl.ds(pl.multiple_of(dest_of(dslot) * members, members), members)
        box = patch * 3 + dslot

        def half(pair, carry):
            left = rb[box, pair * 25 + 24].astype(jnp.float32)
            for k in range(8):
                r, c0 = pair * 2 + k // 4, (k % 4) * 4
                p = [rb[box, pair * 25 + k * 3 + i].astype(jnp.float32) for i in range(3)]
                tail = [jnp.where(lane < 99, pltpu.roll(left, (96 - 3 * (4 * k + i)) % 128, 1), 0.0) for i in range(4)]
                for i in range(3):
                    gath[patch, r, c0 + i, src, 128:256] = jnp.where(lane < 96, p[i], tail[i]).astype(jnp.bfloat16)
                last = jnp.where(lane < 64, jnp.where(lane < 32, pltpu.roll(p[0], 32, 1), pltpu.roll(p[1], 64, 1)),
                                 jnp.where(lane < 96, pltpu.roll(p[2], 96, 1), tail[3]))
                gath[patch, r, c0 + 3, src, 128:256] = last.astype(jnp.bfloat16)
            return carry
        lax.fori_loop(0, 2, half, 0)

    def analysis(patch):
        def arrive(dslot, carry):
            for copy in unit_copies(patch, dslot):
                copy.wait_recv()
            unpack(patch, dslot)
            return carry
        lax.fori_loop(0, 3, lambda i, c: arrive(2 - i, c), 0)
        eye = (lax.broadcasted_iota(jnp.int32, (total_m, total_m), 0) == lax.broadcasted_iota(jnp.int32, (total_m, total_m), 1)).astype(jnp.float32)
        csum = jnp.zeros((total_m, CP), jnp.float32)
        for half in range(2):
            lhs = jnp.concatenate([gath[patch, :, half * 8 + j].reshape(4 * total_m, CP) for j in range(8)], axis=1)
            yb = jnp.dot(lhs, wobs[...], preferred_element_type=jnp.float32)
            for r in range(4):
                g = half * 4 + r
                y = yb[r * total_m:(r + 1) * total_m]
                ybar = jnp.sum(y, axis=0, keepdims=True) * (1.0 / total_m)
                y = y - ybar
                c = y * obs_row[1, patch, g:g + 1, :]
                csum = csum + c * (obs_row[0, patch, g:g + 1, :] - ybar)
                yp[g] = y
                cm[g] = c
        a_mat = (total_m - 1.0) * eye
        for g in range(8):
            a_mat = a_mat + f32dot(cm[g], yp[g], NT)
        amat[patch % 2, :, 0:total_m] = a_mat
        amat[patch % 2, :, total_m:2 * total_m] = a_mat
        cvec[patch % 2] = jnp.broadcast_to(jnp.sum(csum, axis=1, keepdims=True), (total_m, 2 * total_m))

    def solve(patch, slots):
        row = lax.broadcasted_iota(jnp.int32, (total_m, 2 * total_m), 0)
        col = lax.broadcasted_iota(jnp.int32, (total_m, 2 * total_m), 1)
        eye = ((row == col) | (row + total_m == col)).astype(jnp.float32)
        mats = [amat[i] for i in slots]
        traces = [0.5 * jnp.sum(jnp.sum(a * eye, axis=0, keepdims=True), axis=1, keepdims=True) for a in mats]

        def newton(step, carry):
            out = []
            for y, z in carry:
                mix = 1.5 * eye - 0.5 * twin_dot(pair_lhs(z), pair_rhs(y))
                out.append((twin_dot(pair_lhs(y), pair_rhs(mix)), twin_dot(pair_lhs(mix), pair_rhs(z))))
            return tuple(out)
        pairs = lax.fori_loop(0, NS_STEPS, newton, tuple((a / t, eye) for a, t in zip(mats, traces)))
        for i, slot in enumerate(slots):
            root = pairs[i][1] / jnp.sqrt(traces[i])
            left = pair_lhs(root)
            wbar = twin_dot(left, pair_rhs(twin_dot(left, pair_rhs(cvec[slot]))))
            trans = math.sqrt(total_m - 1.0) * root + wbar
            trans = trans + (1.0 - jnp.sum(trans, axis=0, keepdims=True)) * (1.0 / total_m)
            tt_ref[patch + i] = trans[:, 0:total_m].T

        @pl.when(patch < done)
        def _():
            def apply(i, carry):
                lhs = stacked(tt_ref[patch + i // 4])
                for c in range(columns):
                    gath[patch + i // 4, i % 4, c] = transform(lhs, gath[patch + i // 4, i % 4, c])
                return carry
            lax.fori_loop(0, 4 * len(slots), apply, 0)

    def step(v, carry):
        @pl.when(v < units)
        def _():
            prepare(v)

        @pl.when((v >= 1) & (v <= units))
        def _():
            forecast(v - 1)

        @pl.when(v == 3)
        def _():
            setup()

        @pl.when((v >= 12) & (v % 4 == 0))
        def _():
            analysis(v // 4 - 3)

        @pl.when((v >= 12) & (v <= units) & (v % 8 == 0))
        def _():
            solve(v // 4 - 4, (0, 1))

        @pl.when((v > units) & (v % 4 == 0))
        def _():
            solve(v // 4 - 3, ((v // 4 - 3) % 2,))
        return carry
    lax.fori_loop(0, units + 9, step, 0)

    def finish(patch, carry):
        @pl.when(patch >= patches - 2)
        def _():
            for dslot in range(3):
                for copy in unit_copies(patch, dslot):
                    copy.wait_send()
        for dslot in range(4):
            ghost_copy(patch * 4 + dslot).wait_send()
        return carry
    lax.fori_loop(0, patches, finish, 0)


def update_kernel(done, tt_ref, g_ref, out_hbm, stage, sem):
    channels = out_hbm.shape[3]

    def copy(r):
        return pltpu.make_async_copy(stage.at[r], out_hbm.at[r], sem.at[r])

    def write(r, carry):
        for col in range(stage.shape[1]):
            stage[r, col] = g_ref[r // 4, r % 4, col, :, 0:channels]
        copy(r).start()
        return carry
    lax.fori_loop(0, 4 * done, write, 0)

    def last(r, carry):
        lhs = stacked(tt_ref[r // 4])
        for col in range(stage.shape[1]):
            stage[r, col] = transform(lhs, g_ref[r // 4, r % 4, col])[:, 0:channels]
        copy(r).start()
        return carry
    lax.fori_loop(4 * done, stage.shape[0], last, 0)

    def drain(r, carry):
        copy(r).wait()
        return carry
    lax.fori_loop(0, stage.shape[0], drain, 0)


def solution(mesh):
    ens_size = mesh.shape["ens"]
    obs_spec = P(None, None, "dom", None, None)

    def local_step(ens_state, w_in, w_out, obs_op, obs_val, obs_wt):
        members, rows, columns, channels = ens_state.shape
        total_m = members * ens_size
        dev_rows = rows // ens_size
        patches = dev_rows // 4
        units = patches * ens_size
        done = patches - 1
        dims = (members, rows, columns, channels, patches, dev_rows, ens_size, done)
        vmem = pl.BlockSpec(memory_space=pltpu.VMEM)
        anym = pl.BlockSpec(memory_space=pl.ANY)
        bf, f32 = jnp.bfloat16, jnp.float32
        dma = pltpu.SemaphoreType.DMA
        gathered, trans = pl.pallas_call(
            functools.partial(exchange_kernel, dims),
            out_shape=(pltpu.VMEM((patches, 4, columns, total_m, CP), bf),
                       pltpu.VMEM((patches, total_m, total_m), f32)),
            in_specs=[anym, vmem, vmem, vmem, anym, anym],
            out_specs=(vmem, vmem),
            scratch_shapes=[
                pltpu.VMEM((2, channels, columns, rows), bf),
                pltpu.VMEM((members, rows, columns, CP), bf),
                pltpu.VMEM((2, 2, 6, 544, 128), f32),
                pltpu.VMEM((2, 4, 544, 128), f32),
                pltpu.VMEM((members * columns, 2 * CP), bf),
                pltpu.VMEM((2, members * 17, 128), f32),
                pltpu.VMEM((4, columns, members, 128), f32),
                pltpu.VMEM((7, 4, columns, members, 128), bf),
                pltpu.VMEM((6, 50, members, 128), bf),
                pltpu.VMEM((patches * 3, 50, members, 128), bf),
                pltpu.VMEM((units, 2, 4, members, CP), bf),
                pltpu.VMEM((units, 2, 4, members, CP), bf),
                pltpu.VMEM((2 * CP, 512), bf),
                pltpu.VMEM((512, CP), bf),
                pltpu.VMEM((488, 512), f32),
                pltpu.VMEM((8 * CP, CP), bf),
                pltpu.VMEM((2, patches, 4, 1, columns, 32), f32),
                pltpu.VMEM((2, patches, 8, CP), f32),
                pltpu.VMEM((8, total_m, CP), f32),
                pltpu.VMEM((8, total_m, CP), f32),
                pltpu.VMEM((2, total_m, 2 * total_m), f32),
                pltpu.VMEM((2, total_m, 2 * total_m), f32),
                dma((2,)), dma((units,)), dma((units,)), dma((patches, 3, 2)), dma((patches, 3, 2)), dma((2,)),
            ],
            compiler_params=pltpu.CompilerParams(collective_id=0, has_side_effects=True, vmem_limit_bytes=46 * 1024 * 1024),
        )(ens_state.transpose(0, 3, 2, 1), w_in, w_out.T, obs_op.T, obs_val, obs_wt)
        return pl.pallas_call(
            functools.partial(update_kernel, done),
            out_shape=jax.ShapeDtypeStruct((dev_rows, columns, total_m, channels), bf),
            in_specs=[vmem, vmem],
            out_specs=anym,
            scratch_shapes=[pltpu.VMEM((dev_rows, columns, total_m, channels), bf), dma((dev_rows,))],
            compiler_params=pltpu.CompilerParams(vmem_limit_bytes=24 * 1024 * 1024),
        )(pltpu.with_memory_space_constraint(trans, pltpu.VMEM), pltpu.with_memory_space_constraint(gathered, pltpu.VMEM))

    return jax.shard_map(local_step, mesh=mesh, in_specs=(P("ens", None, "dom", None), P(), P(), P(), obs_spec, obs_spec), out_specs=P("ens", "dom", None, None), check_vma=False)
```

```python
import functools
import math
import jax
import jax.numpy as jnp
from jax import lax
from jax.experimental import pallas as pl
from jax.experimental.pallas import tpu as pltpu
from jax.sharding import PartitionSpec as P

NS_STEPS = 18
MESH = pl.DeviceIdType.MESH
CP = 256
NT = (((1,), (1,)), ((), ()))


NN = (((1,), (0,)), ((), ()))


def gelu(x):
    scale = math.sqrt(2.0 / math.pi)
    return (0.5 * x) * (1.0 + jnp.tanh(x * (scale + (scale * 0.044715) * (x * x))))


def split3(a):
    hi = a.astype(jnp.bfloat16)
    rem = a - hi.astype(jnp.float32)
    mid = rem.astype(jnp.bfloat16)
    low = (rem - mid.astype(jnp.float32)).astype(jnp.bfloat16)
    return hi, mid, low


def f32dot(a, b, dims=NN):
    ah, am, al = split3(a)
    bh, bm, bl = split3(b)
    n = a.shape[0]

    def dot(u, v):
        return lax.dot_general(u, v, dims, preferred_element_type=jnp.float32)
    by_hi = dot(jnp.concatenate([ah, am, al], axis=0), bh)
    by_mid = dot(jnp.concatenate([ah, am], axis=0), bm)
    by_low = dot(ah, bl)
    small = (by_low + by_hi[2 * n:]) + by_mid[n:]
    return (small + (by_mid[:n] + by_hi[n:2 * n])) + by_hi[:n]


def pair_lhs(a):
    hi, mid, low = split3(a)
    first = lax.broadcasted_iota(jnp.int32, a.shape, 1) < a.shape[1] // 2
    hi, mid, low = (v.astype(jnp.float32) for v in (hi, mid, low))
    lead = jnp.where(first, hi, mid).astype(jnp.bfloat16)
    return jnp.concatenate([lead, lead, jnp.where(first, hi, low).astype(jnp.bfloat16)], axis=1)


def pair_rhs(b):
    hi, mid, low = split3(b)
    return jnp.concatenate([hi, hi, mid, mid, low, hi], axis=0)


def twin_dot(lhs, rhs):
    k = rhs.shape[1]
    acc = jnp.dot(lhs[:, 2*k:], rhs[2*k:], preferred_element_type=jnp.float32)
    acc = acc + jnp.dot(lhs[:, k:2*k], rhs[k:2*k], preferred_element_type=jnp.float32)
    return acc + jnp.dot(lhs[:, :k], rhs[:k], preferred_element_type=jnp.float32)


def stacked(t):
    hi, mid, low = (v.astype(jnp.float32) for v in split3(t))
    return jnp.concatenate([
        jnp.concatenate([hi, mid], axis=1),
        jnp.concatenate([low, jnp.zeros_like(low)], axis=1)], axis=0).astype(jnp.bfloat16)


def transform(lhs, g):
    n = lhs.shape[0] // 2
    res = jnp.dot(lhs, jnp.concatenate([g, g], axis=0), preferred_element_type=jnp.float32)
    return (res[n:] + res[:n]).astype(jnp.bfloat16)


def exchange_kernel(dims, xt_hbm, wi_ref, wo_ref, op_ref, yo_hbm, wt_hbm, gath, tt_ref,
                    xn, xb, xs, xa, xl, ts, t2, sb1, sb2, rb, gsend, grecv, wi, wo, wf, wobs, obs_raw, obs_row, yp, cm, amat, cvec,
                    xsem, gssem, grsem, ssem, rsem, osem):
    members, rows, columns, channels, patches, dev_rows, ens_size, done = dims
    units = patches * ens_size
    total_m = members * ens_size
    me = lax.axis_index("ens")
    mydom = lax.axis_index("dom")
    my_x, my_core = me // 2, me % 2
    mine = pl.ds(pl.multiple_of(me * members, members), members)

    def dest_of(dslot):
        dx = (my_x + 1 - dslot // 2) % 2
        dc = (my_core + (dslot + 1) // 2) % 2
        return dx * 2 + dc

    def x_copy(m):
        return pltpu.make_async_copy(xt_hbm.at[m], xn.at[m % 2], xsem.at[m % 2])

    def ghost_copy(unit):
        return pltpu.make_async_remote_copy(
            src_ref=gsend.at[unit], dst_ref=grecv.at[unit], send_sem=gssem.at[unit], recv_sem=grsem.at[unit],
            device_id={"dom": 1 - mydom}, device_id_type=MESH)

    def unit_copies(patch, dslot):
        dev = {"ens": dest_of(dslot)}
        first = pltpu.make_async_remote_copy(
            src_ref=sb1.at[(patch % 2) * 3 + dslot], dst_ref=gath.at[patch, :, :, mine, pl.ds(0, 128)],
            send_sem=ssem.at[patch, dslot, 0], recv_sem=rsem.at[patch, dslot, 0],
            device_id=dev, device_id_type=MESH)
        second = pltpu.make_async_remote_copy(
            src_ref=sb2.at[(patch % 2) * 3 + dslot], dst_ref=rb.at[patch * 3 + dslot],
            send_sem=ssem.at[patch, dslot, 1], recv_sem=rsem.at[patch, dslot, 1],
            device_id=dev, device_id_type=MESH)
        return first, second

    obs_copies = [pltpu.make_async_copy(ref.at[pl.ds(me * patches, patches)], obs_raw.at[i], osem.at[i]) for i, ref in enumerate((yo_hbm, wt_hbm))]

    x_copy(0).start()
    x_copy(1).start()
    for copy in obs_copies:
        copy.start()
    barrier = pltpu.get_barrier_semaphore()
    for dslot in range(3):
        pl.semaphore_signal(barrier, inc=1, device_id={"ens": dest_of(dslot)}, device_id_type=MESH)
    pl.semaphore_signal(barrier, inc=1, device_id={"dom": 1 - mydom}, device_id_type=MESH)

    wf[...] = jnp.zeros_like(wf)
    wf[0:channels, :] = wo_ref[...].astype(jnp.float32)
    wo[...] = wf[0:CP, :].T.astype(jnp.bfloat16)
    wf[0:2 * channels, :] = wi_ref[...].astype(jnp.float32)
    keep = lax.broadcasted_iota(jnp.int32, (CP, 512), 0) < channels
    wi[0:CP, :] = jnp.where(keep, wf[0:CP, :], 0.0).astype(jnp.bfloat16)
    wi[CP:2 * CP, :] = wf[channels:channels + CP, :].astype(jnp.bfloat16)
    turn = (lax.broadcasted_iota(jnp.int32, (128, 128), 0) == lax.broadcasted_iota(jnp.int32, (128, 128), 1)).astype(jnp.float32).astype(jnp.bfloat16)

    wide = ([[xs.at[0, h, j] for j in range(4)] for h in range(2)],
            [[xs.at[j // 2, h, 4 + j % 2] for j in range(4)] for h in range(2)])
    turned = ([[xs.at[1, h, j] for j in range(4)] for h in range(2)],
              [[xa.at[h, j] for j in range(4)] for h in range(2)])

    def widen(odd, c):
        wide[odd][c // 128][c // 32 % 4][17 * (c % 32):17 * (c % 32) + 16, :] = xn[odd, c].astype(jnp.float32)

    def turn_column(odd, col):
        part = jnp.concatenate([wide[odd][h][j][pl.ds(col, 32, stride=17), :] for h in range(2) for j in range(4)], axis=0)
        out = lax.dot_general(turn, part.astype(jnp.bfloat16), NT, preferred_element_type=jnp.float32)
        for h in range(2):
            for j in range(4):
                turned[odd][h][j][pl.ds(col, 32, stride=17), :] = out[32 * j:32 * j + 32, h * 128:h * 128 + 128]

    def narrow(odd, m, row):
        for h in range(2):
            xb[m, row, :, h * 128:h * 128 + 128] = turned[odd][h][row // 32][17 * (row % 32):17 * (row % 32) + 16, :].astype(jnp.bfloat16)

    def relayout(t, carry):
        for odd in range(2):
            m = 2 * t + odd

            @pl.when(m + 2 < members)
            def _():
                x_copy(m + 2).start()

            @pl.when(m + 1 < members)
            def _():
                x_copy(m + 1).wait()
            for col in range(columns):
                turn_column(odd, col)
                for c in range(channels * col // columns, channels * (col + 1) // columns):
                    widen(1 - odd, c)
                for row in range(rows * col // columns, rows * (col + 1) // columns):
                    narrow(1 - odd, jnp.maximum(m - 1, 0), row)
        return carry
    for ref in (wide[0][1][3], wide[1][1][3]):
        ref[17 * (channels % 32):544, :] = jnp.zeros((544 - 17 * (channels % 32), 128), jnp.float32)
    x_copy(0).wait()
    for c in range(channels):
        widen(0, c)
    lax.fori_loop(0, members // 2, relayout, 0)

    for row in range(rows):
        narrow(1, members - 1, row)
    pl.semaphore_wait(barrier, 4)

    lane = lax.broadcasted_iota(jnp.int32, (members, 128), 1)

    def setup():
        wf[0:128, 0:CP] = jnp.zeros((128, CP), jnp.float32)
        wf[0:32, 0:channels] = op_ref[...].astype(jnp.float32)
        opt = wf[0:128, 0:CP].T.astype(jnp.bfloat16)
        for j in range(8):
            place = (lax.broadcasted_iota(jnp.int32, (128, CP), 1) == lax.broadcasted_iota(jnp.int32, (128, CP), 0) + 32 * j)
            wobs[j * CP:(j + 1) * CP, :] = jnp.dot(opt, place.astype(jnp.bfloat16), preferred_element_type=jnp.float32).astype(jnp.bfloat16)
        for copy in obs_copies:
            copy.wait()
        sub8 = lax.broadcasted_iota(jnp.int32, (8, 128), 0)
        lane8 = lax.broadcasted_iota(jnp.int32, (8, 128), 1) // 32
        wf[0:8, 0:128] = jnp.zeros((8, 128), jnp.float32)

        def rows_of(patch, carry):
            for i in range(2):
                for g in range(8):
                    wf[0:8, 0:32] = obs_raw[i, patch, g % 4, 0, (g // 4) * 8:(g // 4) * 8 + 8, :]
                    v = wf[0:8, 0:128]
                    v = v + pltpu.roll(v, 32, 1)
                    v = v + pltpu.roll(v, 64, 1)
                    for q in range(2):
                        obs_row[i, patch, g:g + 1, q * 128:q * 128 + 128] = jnp.sum(jnp.where(sub8 == lane8 + 4 * q, v, 0.0), axis=0, keepdims=True)
            return carry
        lax.fori_loop(0, patches, rows_of, 0)

    def prepare(unit):
        slot = unit % 2
        patch, dslot = unit // ens_size, unit % ens_size
        first = dest_of(dslot) * dev_rows + patch * 4

        def convert(r, carry):
            row = jnp.minimum(jnp.maximum(first + r - 1, 0), rows - 1)
            for m in range(members):
                for h in range(2):
                    xs[slot, h, r, 33 * m + 8:33 * m + 24, :] = xb[m, row, :, h * 128:h * 128 + 128].astype(jnp.float32)
            return carry
        lax.fori_loop(0, 6, convert, 0)

        def edges(r, carry):
            for h in range(2):
                gsend[unit, 0, r, :, h * 128:h * 128 + 128] = xs[slot, h, r + 1, pl.ds(23, members, stride=33), :].astype(jnp.bfloat16)
                gsend[unit, 1, r, :, h * 128:h * 128 + 128] = xs[slot, h, r + 1, pl.ds(8, members, stride=33), :].astype(jnp.bfloat16)
            return carry
        lax.fori_loop(0, 4, edges, 0)
        ghost_copy(unit).start()

    def forecast(unit):
        patch, dslot = unit // ens_size, unit % ens_size
        slot = unit % 2
        out_slot = jnp.where(dslot < 3, (patch % 2) * 3 + dslot, 6)

        @pl.when((dslot < 3) & (patch >= 2))
        def _():
            for copy in unit_copies(patch - 2, dslot):
                copy.wait_send()
        ghost_copy(unit).wait_recv()

        def block(r, carry):
            for h in range(2):
                xs[slot, h, r + 1, pl.ds(7, members, stride=33), :] = grecv[unit, 0, r, :, h * 128:h * 128 + 128].astype(jnp.float32)
                xs[slot, h, r + 1, pl.ds(24, members, stride=33), :] = grecv[unit, 1, r, :, h * 128:h * 128 + 128].astype(jnp.float32)
            for m in range(members):
                b = 33 * m
                for h in range(2):
                    cur = xs[slot, h, r + 1, b + 8:b + 24, :]
                    north = xs[slot, h, r, b + 8:b + 24, :]
                    south = xs[slot, h, r + 2, b + 8:b + 24, :]
                    west = xs[slot, h, r + 1, b + 7:b + 23, :]
                    east = xs[slot, h, r + 1, b + 9:b + 25, :]
                    lap = north + south + west + east - 4.0 * cur
                    xl[16 * m:16 * m + 16, h * 128:h * 128 + 128] = cur.astype(jnp.bfloat16)
                    xl[16 * m:16 * m + 16, CP + h * 128:CP + h * 128 + 128] = lap.astype(jnp.bfloat16)
            hidden = jnp.dot(xl[...], wi[...], preferred_element_type=jnp.float32)
            gel = gelu(hidden).astype(jnp.bfloat16)
            inc = jnp.dot(gel, wo[...], preferred_element_type=jnp.float32)
            for m in range(members):
                for h in range(2):
                    ts[h, 17 * m:17 * m + 16, :] = xs[slot, h, r + 1, 33 * m + 8:33 * m + 24, :] + inc[16 * m:16 * m + 16, h * 128:h * 128 + 128]
            for col in range(columns):
                sb1[out_slot, r, col] = ts[0, pl.ds(col, members, stride=17), :].astype(jnp.bfloat16)
                t2[r, col] = ts[1, pl.ds(col, members, stride=17), :]
            return carry
        lax.fori_loop(0, 4, block, 0)

        @pl.when(dslot < 3)
        def _():
            def pack(pair, carry):
                left = jnp.zeros((members, 128), jnp.float32)
                for k in range(8):
                    r, c0 = pair * 2 + k // 4, (k % 4) * 4
                    v = [t2[r, c0 + i] for i in range(4)]
                    for i in range(3):
                        sb2[out_slot, pair * 25 + k * 3 + i] = jnp.where(lane < 96, v[i], pltpu.roll(v[3], 96 - 32 * i, 1)).astype(jnp.bfloat16)
                    for i in range(4):
                        left = left + pltpu.roll(jnp.where(lane >= 96, v[i], 0.0), (32 + 3 * (4 * k + i)) % 128, 1)
                sb2[out_slot, pair * 25 + 24] = left.astype(jnp.bfloat16)
                return carry
            lax.fori_loop(0, 2, pack, 0)
            for copy in unit_copies(patch, dslot):
                copy.start()

        @pl.when(dslot == 3)
        def _():
            def own(r, carry):
                for col in range(columns):
                    gath[patch, r, col, mine, 0:128] = sb1[6, r, col]
                    gath[patch, r, col, mine, 128:256] = t2[r, col].astype(jnp.bfloat16)
                return carry
            lax.fori_loop(0, 4, own, 0)

    def unpack(patch, dslot):
        src = pl.ds(pl.multiple_of(dest_of(dslot) * members, members), members)
        box = patch * 3 + dslot

        def half(pair, carry):
            left = rb[box, pair * 25 + 24].astype(jnp.float32)
            for k in range(8):
                r, c0 = pair * 2 + k // 4, (k % 4) * 4
                p = [rb[box, pair * 25 + k * 3 + i].astype(jnp.float32) for i in range(3)]
                tail = [jnp.where(lane < 99, pltpu.roll(left, (96 - 3 * (4 * k + i)) % 128, 1), 0.0) for i in range(4)]
                for i in range(3):
                    gath[patch, r, c0 + i, src, 128:256] = jnp.where(lane < 96, p[i], tail[i]).astype(jnp.bfloat16)
                last = jnp.where(lane < 64, jnp.where(lane < 32, pltpu.roll(p[0], 32, 1), pltpu.roll(p[1], 64, 1)),
                                 jnp.where(lane < 96, pltpu.roll(p[2], 96, 1), tail[3]))
                gath[patch, r, c0 + 3, src, 128:256] = last.astype(jnp.bfloat16)
            return carry
        lax.fori_loop(0, 2, half, 0)

    def analysis(patch):
        def arrive(dslot, carry):
            for copy in unit_copies(patch, dslot):
                copy.wait_recv()
            unpack(patch, dslot)
            return carry
        lax.fori_loop(0, 3, lambda i, c: arrive(2 - i, c), 0)
        eye = (lax.broadcasted_iota(jnp.int32, (total_m, total_m), 0) == lax.broadcasted_iota(jnp.int32, (total_m, total_m), 1)).astype(jnp.float32)
        csum = jnp.zeros((total_m, CP), jnp.float32)
        for half in range(2):
            lhs = jnp.concatenate([gath[patch, :, half * 8 + j].reshape(4 * total_m, CP) for j in range(8)], axis=1)
            yb = jnp.dot(lhs, wobs[...], preferred_element_type=jnp.float32)
            for r in range(4):
                g = half * 4 + r
                y = yb[r * total_m:(r + 1) * total_m]
                ybar = jnp.sum(y, axis=0, keepdims=True) * (1.0 / total_m)
                y = y - ybar
                c = y * obs_row[1, patch, g:g + 1, :]
                csum = csum + c * (obs_row[0, patch, g:g + 1, :] - ybar)
                yp[g] = y
                cm[g] = c
        a_mat = (total_m - 1.0) * eye
        for g in range(8):
            a_mat = a_mat + f32dot(cm[g], yp[g], NT)
        amat[patch % 2, :, 0:total_m] = a_mat
        amat[patch % 2, :, total_m:2 * total_m] = a_mat
        cvec[patch % 2] = jnp.broadcast_to(jnp.sum(csum, axis=1, keepdims=True), (total_m, 2 * total_m))

    def solve(patch, slots):
        row = lax.broadcasted_iota(jnp.int32, (total_m, 2 * total_m), 0)
        col = lax.broadcasted_iota(jnp.int32, (total_m, 2 * total_m), 1)
        eye = ((row == col) | (row + total_m == col)).astype(jnp.float32)
        mats = [amat[i] for i in slots]
        traces = [0.5 * jnp.sum(jnp.sum(a * eye, axis=0, keepdims=True), axis=1, keepdims=True) for a in mats]

        def newton(step, carry):
            out = []
            for y, z in carry:
                mix = 1.5 * eye - 0.5 * twin_dot(pair_lhs(z), pair_rhs(y))
                out.append((twin_dot(pair_lhs(y), pair_rhs(mix)), twin_dot(pair_lhs(mix), pair_rhs(z))))
            return tuple(out)
        pairs = lax.fori_loop(0, NS_STEPS, newton, tuple((a / t, eye) for a, t in zip(mats, traces)))
        for i, slot in enumerate(slots):
            root = pairs[i][1] / jnp.sqrt(traces[i])
            left = pair_lhs(root)
            wbar = twin_dot(left, pair_rhs(twin_dot(left, pair_rhs(cvec[slot]))))
            trans = math.sqrt(total_m - 1.0) * root + wbar
            trans = trans + (1.0 - jnp.sum(trans, axis=0, keepdims=True)) * (1.0 / total_m)
            tt_ref[patch + i] = trans[:, 0:total_m].T

        @pl.when(patch < done)
        def _():
            def apply(i, carry):
                lhs = stacked(tt_ref[patch + i // 4])
                for c in range(columns):
                    gath[patch + i // 4, i % 4, c] = transform(lhs, gath[patch + i // 4, i % 4, c])
                return carry
            lax.fori_loop(0, 4 * len(slots), apply, 0)

    def step(v, carry):
        @pl.when(v < units)
        def _():
            prepare(v)

        @pl.when((v >= 1) & (v <= units))
        def _():
            forecast(v - 1)

        @pl.when(v == 3)
        def _():
            setup()

        @pl.when((v >= 12) & (v % 4 == 0))
        def _():
            analysis(v // 4 - 3)

        @pl.when((v >= 12) & (v % 8 == 0))
        def _():
            solve(v // 4 - 4, (0, 1))
        return carry
    lax.fori_loop(0, units + 9, step, 0)

    def finish(patch, carry):
        @pl.when(patch >= patches - 2)
        def _():
            for dslot in range(3):
                for copy in unit_copies(patch, dslot):
                    copy.wait_send()
        for dslot in range(4):
            ghost_copy(patch * 4 + dslot).wait_send()
        return carry
    lax.fori_loop(0, patches, finish, 0)


def update_kernel(done, tt_ref, g_ref, out_hbm, stage, sem):
    channels = out_hbm.shape[3]

    def copy(r):
        return pltpu.make_async_copy(stage.at[r], out_hbm.at[r], sem.at[r])

    def write(r, carry):
        for col in range(stage.shape[1]):
            stage[r, col] = g_ref[r // 4, r % 4, col, :, 0:channels]
        copy(r).start()
        return carry
    lax.fori_loop(0, 4 * done, write, 0)

    def last(r, carry):
        lhs = stacked(tt_ref[r // 4])
        for col in range(stage.shape[1]):
            stage[r, col] = transform(lhs, g_ref[r // 4, r % 4, col])[:, 0:channels]
        copy(r).start()
        return carry
    lax.fori_loop(4 * done, stage.shape[0], last, 0)

    def drain(r, carry):
        copy(r).wait()
        return carry
    lax.fori_loop(0, stage.shape[0], drain, 0)


def solution(mesh):
    ens_size = mesh.shape["ens"]
    obs_spec = P(None, None, "dom", None, None)

    def local_step(ens_state, w_in, w_out, obs_op, obs_val, obs_wt):
        members, rows, columns, channels = ens_state.shape
        total_m = members * ens_size
        dev_rows = rows // ens_size
        patches = dev_rows // 4
        units = patches * ens_size
        done = patches - 2
        dims = (members, rows, columns, channels, patches, dev_rows, ens_size, done)
        vmem = pl.BlockSpec(memory_space=pltpu.VMEM)
        anym = pl.BlockSpec(memory_space=pl.ANY)
        bf, f32 = jnp.bfloat16, jnp.float32
        dma = pltpu.SemaphoreType.DMA
        gathered, trans = pl.pallas_call(
            functools.partial(exchange_kernel, dims),
            out_shape=(pltpu.VMEM((patches, 4, columns, total_m, CP), bf),
                       pltpu.VMEM((patches, total_m, total_m), f32)),
            in_specs=[anym, vmem, vmem, vmem, anym, anym],
            out_specs=(vmem, vmem),
            scratch_shapes=[
                pltpu.VMEM((2, channels, columns, rows), bf),
                pltpu.VMEM((members, rows, columns, CP), bf),
                pltpu.VMEM((2, 2, 6, 544, 128), f32),
                pltpu.VMEM((2, 4, 544, 128), f32),
                pltpu.VMEM((members * columns, 2 * CP), bf),
                pltpu.VMEM((2, members * 17, 128), f32),
                pltpu.VMEM((4, columns, members, 128), f32),
                pltpu.VMEM((7, 4, columns, members, 128), bf),
                pltpu.VMEM((6, 50, members, 128), bf),
                pltpu.VMEM((patches * 3, 50, members, 128), bf),
                pltpu.VMEM((units, 2, 4, members, CP), bf),
                pltpu.VMEM((units, 2, 4, members, CP), bf),
                pltpu.VMEM((2 * CP, 512), bf),
                pltpu.VMEM((512, CP), bf),
                pltpu.VMEM((488, 512), f32),
                pltpu.VMEM((8 * CP, CP), bf),
                pltpu.VMEM((2, patches, 4, 1, columns, 32), f32),
                pltpu.VMEM((2, patches, 8, CP), f32),
                pltpu.VMEM((8, total_m, CP), f32),
                pltpu.VMEM((8, total_m, CP), f32),
                pltpu.VMEM((2, total_m, 2 * total_m), f32),
                pltpu.VMEM((2, total_m, 2 * total_m), f32),
                dma((2,)), dma((units,)), dma((units,)), dma((patches, 3, 2)), dma((patches, 3, 2)), dma((2,)),
            ],
            compiler_params=pltpu.CompilerParams(collective_id=0, has_side_effects=True, vmem_limit_bytes=46 * 1024 * 1024),
        )(ens_state.transpose(0, 3, 2, 1), w_in, w_out.T, obs_op.T, obs_val, obs_wt)
        return pl.pallas_call(
            functools.partial(update_kernel, done),
            out_shape=jax.ShapeDtypeStruct((dev_rows, columns, total_m, channels), bf),
            in_specs=[vmem, vmem],
            out_specs=anym,
            scratch_shapes=[pltpu.VMEM((dev_rows, columns, total_m, channels), bf), dma((dev_rows,))],
            compiler_params=pltpu.CompilerParams(vmem_limit_bytes=24 * 1024 * 1024),
        )(pltpu.with_memory_space_constraint(trans, pltpu.VMEM), pltpu.with_memory_space_constraint(gathered, pltpu.VMEM))

    return jax.shard_map(local_step, mesh=mesh, in_specs=(P("ens", None, "dom", None), P(), P(), P(), obs_spec, obs_spec), out_specs=P("ens", "dom", None, None), check_vma=False)
```

```python
import functools
import math
import jax
import jax.numpy as jnp
from jax import lax
from jax.experimental import pallas as pl
from jax.experimental.pallas import tpu as pltpu
from jax.sharding import PartitionSpec as P

NS_STEPS = 18
MESH = pl.DeviceIdType.MESH
CP = 256
NT = (((1,), (1,)), ((), ()))


NN = (((1,), (0,)), ((), ()))


def gelu(x):
    scale = math.sqrt(2.0 / math.pi)
    return (0.5 * x) * (1.0 + jnp.tanh(x * (scale + (scale * 0.044715) * (x * x))))


def split3(a):
    hi = a.astype(jnp.bfloat16)
    rem = a - hi.astype(jnp.float32)
    mid = rem.astype(jnp.bfloat16)
    low = (rem - mid.astype(jnp.float32)).astype(jnp.bfloat16)
    return hi, mid, low


def f32dot(a, b, dims=NN):
    ah, am, al = split3(a)
    bh, bm, bl = split3(b)
    n = a.shape[0]

    def dot(u, v):
        return lax.dot_general(u, v, dims, preferred_element_type=jnp.float32)
    by_hi = dot(jnp.concatenate([ah, am, al], axis=0), bh)
    by_mid = dot(jnp.concatenate([ah, am], axis=0), bm)
    by_low = dot(ah, bl)
    small = (by_low + by_hi[2 * n:]) + by_mid[n:]
    return (small + (by_mid[:n] + by_hi[n:2 * n])) + by_hi[:n]


def packed_dot(a, b, left, right):
    ah, am, al = split3(a)
    bh, bm, bl = split3(b)
    n = a.shape[0]

    def dot(u, v):
        blocks = jnp.concatenate([v * left, v * right], axis=0)
        return jnp.dot(u, blocks, preferred_element_type=jnp.float32)
    by_hi = dot(jnp.concatenate([ah, am, al], axis=0), bh)
    by_mid = dot(jnp.concatenate([ah, am], axis=0), bm)
    by_low = dot(ah, bl)
    small = (by_low + by_hi[2 * n:]) + by_mid[n:]
    return (small + (by_mid[:n] + by_hi[n:2 * n])) + by_hi[:n]


def stacked(t):
    hi, mid, low = (v.astype(jnp.float32) for v in split3(t))
    return jnp.concatenate([
        jnp.concatenate([hi, mid], axis=1),
        jnp.concatenate([low, jnp.zeros_like(low)], axis=1)], axis=0).astype(jnp.bfloat16)


def transform(lhs, g):
    n = lhs.shape[0] // 2
    res = jnp.dot(lhs, jnp.concatenate([g, g], axis=0), preferred_element_type=jnp.float32)
    return (res[n:] + res[:n]).astype(jnp.bfloat16)


def exchange_kernel(dims, xt_hbm, wi_ref, wo_ref, op_ref, yo_hbm, wt_hbm, gath, tt_ref,
                    xn, xb, xs, xa, xl, ts, t2, sb1, sb2, rb, gsend, grecv, wi, wo, wf, wobs, obs_raw, obs_row, yp, cm, amat, cvec,
                    xsem, gssem, grsem, ssem, rsem, osem):
    members, rows, columns, channels, patches, dev_rows, ens_size, done = dims
    units = patches * ens_size
    total_m = members * ens_size
    me = lax.axis_index("ens")
    mydom = lax.axis_index("dom")
    my_x, my_core = me // 2, me % 2
    mine = pl.ds(pl.multiple_of(me * members, members), members)

    def dest_of(dslot):
        dx = (my_x + 1 - dslot // 2) % 2
        dc = (my_core + (dslot + 1) // 2) % 2
        return dx * 2 + dc

    def x_copy(m):
        return pltpu.make_async_copy(xt_hbm.at[m], xn.at[m % 2], xsem.at[m % 2])

    def ghost_copy(unit):
        return pltpu.make_async_remote_copy(
            src_ref=gsend.at[unit], dst_ref=grecv.at[unit], send_sem=gssem.at[unit], recv_sem=grsem.at[unit],
            device_id={"dom": 1 - mydom}, device_id_type=MESH)

    def unit_copies(patch, dslot):
        dev = {"ens": dest_of(dslot)}
        first = pltpu.make_async_remote_copy(
            src_ref=sb1.at[(patch % 2) * 3 + dslot], dst_ref=gath.at[patch, :, :, mine, pl.ds(0, 128)],
            send_sem=ssem.at[patch, dslot, 0], recv_sem=rsem.at[patch, dslot, 0],
            device_id=dev, device_id_type=MESH)
        second = pltpu.make_async_remote_copy(
            src_ref=sb2.at[(patch % 2) * 3 + dslot], dst_ref=rb.at[patch * 3 + dslot],
            send_sem=ssem.at[patch, dslot, 1], recv_sem=rsem.at[patch, dslot, 1],
            device_id=dev, device_id_type=MESH)
        return first, second

    obs_copies = [pltpu.make_async_copy(ref.at[pl.ds(me * patches, patches)], obs_raw.at[i], osem.at[i]) for i, ref in enumerate((yo_hbm, wt_hbm))]

    x_copy(0).start()
    x_copy(1).start()
    for copy in obs_copies:
        copy.start()
    barrier = pltpu.get_barrier_semaphore()
    for dslot in range(3):
        pl.semaphore_signal(barrier, inc=1, device_id={"ens": dest_of(dslot)}, device_id_type=MESH)
    pl.semaphore_signal(barrier, inc=1, device_id={"dom": 1 - mydom}, device_id_type=MESH)

    wf[...] = jnp.zeros_like(wf)
    wf[0:channels, :] = wo_ref[...].astype(jnp.float32)
    wo[...] = wf[0:CP, :].T.astype(jnp.bfloat16)
    wf[0:2 * channels, :] = wi_ref[...].astype(jnp.float32)
    keep = lax.broadcasted_iota(jnp.int32, (CP, 512), 0) < channels
    wi[0:CP, :] = jnp.where(keep, wf[0:CP, :], 0.0).astype(jnp.bfloat16)
    wi[CP:2 * CP, :] = wf[channels:channels + CP, :].astype(jnp.bfloat16)
    turn = (lax.broadcasted_iota(jnp.int32, (128, 128), 0) == lax.broadcasted_iota(jnp.int32, (128, 128), 1)).astype(jnp.float32).astype(jnp.bfloat16)

    wide = ([[xs.at[0, h, j] for j in range(4)] for h in range(2)],
            [[xs.at[j // 2, h, 4 + j % 2] for j in range(4)] for h in range(2)])
    turned = ([[xs.at[1, h, j] for j in range(4)] for h in range(2)],
              [[xa.at[h, j] for j in range(4)] for h in range(2)])

    def widen(odd, c):
        wide[odd][c // 128][c // 32 % 4][17 * (c % 32):17 * (c % 32) + 16, :] = xn[odd, c].astype(jnp.float32)

    def turn_column(odd, col):
        part = jnp.concatenate([wide[odd][h][j][pl.ds(col, 32, stride=17), :] for h in range(2) for j in range(4)], axis=0)
        out = lax.dot_general(turn, part.astype(jnp.bfloat16), NT, preferred_element_type=jnp.float32)
        for h in range(2):
            for j in range(4):
                turned[odd][h][j][pl.ds(col, 32, stride=17), :] = out[32 * j:32 * j + 32, h * 128:h * 128 + 128]

    def narrow(odd, m, row):
        for h in range(2):
            xb[m, row, :, h * 128:h * 128 + 128] = turned[odd][h][row // 32][17 * (row % 32):17 * (row % 32) + 16, :].astype(jnp.bfloat16)

    def relayout(t, carry):
        for odd in range(2):
            m = 2 * t + odd

            @pl.when(m + 2 < members)
            def _():
                x_copy(m + 2).start()

            @pl.when(m + 1 < members)
            def _():
                x_copy(m + 1).wait()
            for col in range(columns):
                turn_column(odd, col)
                for c in range(channels * col // columns, channels * (col + 1) // columns):
                    widen(1 - odd, c)
                for row in range(rows * col // columns, rows * (col + 1) // columns):
                    narrow(1 - odd, jnp.maximum(m - 1, 0), row)
        return carry
    for ref in (wide[0][1][3], wide[1][1][3]):
        ref[17 * (channels % 32):544, :] = jnp.zeros((544 - 17 * (channels % 32), 128), jnp.float32)
    x_copy(0).wait()
    for c in range(channels):
        widen(0, c)
    lax.fori_loop(0, members // 2, relayout, 0)

    for row in range(rows):
        narrow(1, members - 1, row)
    pl.semaphore_wait(barrier, 4)

    lane = lax.broadcasted_iota(jnp.int32, (members, 128), 1)

    def setup():
        wf[0:128, 0:CP] = jnp.zeros((128, CP), jnp.float32)
        wf[0:32, 0:channels] = op_ref[...].astype(jnp.float32)
        opt = wf[0:128, 0:CP].T.astype(jnp.bfloat16)
        for j in range(8):
            place = (lax.broadcasted_iota(jnp.int32, (128, CP), 1) == lax.broadcasted_iota(jnp.int32, (128, CP), 0) + 32 * j)
            wobs[j * CP:(j + 1) * CP, :] = jnp.dot(opt, place.astype(jnp.bfloat16), preferred_element_type=jnp.float32).astype(jnp.bfloat16)
        for copy in obs_copies:
            copy.wait()
        sub8 = lax.broadcasted_iota(jnp.int32, (8, 128), 0)
        lane8 = lax.broadcasted_iota(jnp.int32, (8, 128), 1) // 32
        wf[0:8, 0:128] = jnp.zeros((8, 128), jnp.float32)

        def rows_of(patch, carry):
            for i in range(2):
                for g in range(8):
                    wf[0:8, 0:32] = obs_raw[i, patch, g % 4, 0, (g // 4) * 8:(g // 4) * 8 + 8, :]
                    v = wf[0:8, 0:128]
                    v = v + pltpu.roll(v, 32, 1)
                    v = v + pltpu.roll(v, 64, 1)
                    for q in range(2):
                        obs_row[i, patch, g:g + 1, q * 128:q * 128 + 128] = jnp.sum(jnp.where(sub8 == lane8 + 4 * q, v, 0.0), axis=0, keepdims=True)
            return carry
        lax.fori_loop(0, patches, rows_of, 0)

    def prepare(unit):
        slot = unit % 2
        patch, dslot = unit // ens_size, unit % ens_size
        first = dest_of(dslot) * dev_rows + patch * 4

        def convert(r, carry):
            row = jnp.minimum(jnp.maximum(first + r - 1, 0), rows - 1)
            for m in range(members):
                for h in range(2):
                    xs[slot, h, r, 33 * m + 8:33 * m + 24, :] = xb[m, row, :, h * 128:h * 128 + 128].astype(jnp.float32)
            return carry
        lax.fori_loop(0, 6, convert, 0)

        def edges(r, carry):
            for h in range(2):
                gsend[unit, 0, r, :, h * 128:h * 128 + 128] = xs[slot, h, r + 1, pl.ds(23, members, stride=33), :].astype(jnp.bfloat16)
                gsend[unit, 1, r, :, h * 128:h * 128 + 128] = xs[slot, h, r + 1, pl.ds(8, members, stride=33), :].astype(jnp.bfloat16)
            return carry
        lax.fori_loop(0, 4, edges, 0)
        ghost_copy(unit).start()

    def forecast(unit):
        patch, dslot = unit // ens_size, unit % ens_size
        slot = unit % 2
        out_slot = jnp.where(dslot < 3, (patch % 2) * 3 + dslot, 6)

        @pl.when((dslot < 3) & (patch >= 2))
        def _():
            for copy in unit_copies(patch - 2, dslot):
                copy.wait_send()
        ghost_copy(unit).wait_recv()

        def block(r, carry):
            for h in range(2):
                xs[slot, h, r + 1, pl.ds(7, members, stride=33), :] = grecv[unit, 0, r, :, h * 128:h * 128 + 128].astype(jnp.float32)
                xs[slot, h, r + 1, pl.ds(24, members, stride=33), :] = grecv[unit, 1, r, :, h * 128:h * 128 + 128].astype(jnp.float32)
            for m in range(members):
                b = 33 * m
                for h in range(2):
                    cur = xs[slot, h, r + 1, b + 8:b + 24, :]
                    north = xs[slot, h, r, b + 8:b + 24, :]
                    south = xs[slot, h, r + 2, b + 8:b + 24, :]
                    west = xs[slot, h, r + 1, b + 7:b + 23, :]
                    east = xs[slot, h, r + 1, b + 9:b + 25, :]
                    lap = north + south + west + east - 4.0 * cur
                    xl[16 * m:16 * m + 16, h * 128:h * 128 + 128] = cur.astype(jnp.bfloat16)
                    xl[16 * m:16 * m + 16, CP + h * 128:CP + h * 128 + 128] = lap.astype(jnp.bfloat16)
            hidden = jnp.dot(xl[...], wi[...], preferred_element_type=jnp.float32)
            gel = gelu(hidden).astype(jnp.bfloat16)
            inc = jnp.dot(gel, wo[...], preferred_element_type=jnp.float32)
            for m in range(members):
                for h in range(2):
                    ts[h, 17 * m:17 * m + 16, :] = xs[slot, h, r + 1, 33 * m + 8:33 * m + 24, :] + inc[16 * m:16 * m + 16, h * 128:h * 128 + 128]
            for col in range(columns):
                sb1[out_slot, r, col] = ts[0, pl.ds(col, members, stride=17), :].astype(jnp.bfloat16)
                t2[r, col] = ts[1, pl.ds(col, members, stride=17), :]
            return carry
        lax.fori_loop(0, 4, block, 0)

        @pl.when(dslot < 3)
        def _():
            def pack(pair, carry):
                left = jnp.zeros((members, 128), jnp.float32)
                for k in range(8):
                    r, c0 = pair * 2 + k // 4, (k % 4) * 4
                    v = [t2[r, c0 + i] for i in range(4)]
                    for i in range(3):
                        sb2[out_slot, pair * 25 + k * 3 + i] = jnp.where(lane < 96, v[i], pltpu.roll(v[3], 96 - 32 * i, 1)).astype(jnp.bfloat16)
                    for i in range(4):
                        left = left + pltpu.roll(jnp.where(lane >= 96, v[i], 0.0), (32 + 3 * (4 * k + i)) % 128, 1)
                sb2[out_slot, pair * 25 + 24] = left.astype(jnp.bfloat16)
                return carry
            lax.fori_loop(0, 2, pack, 0)
            for copy in unit_copies(patch, dslot):
                copy.start()

        @pl.when(dslot == 3)
        def _():
            def own(r, carry):
                for col in range(columns):
                    gath[patch, r, col, mine, 0:128] = sb1[6, r, col]
                    gath[patch, r, col, mine, 128:256] = t2[r, col].astype(jnp.bfloat16)
                return carry
            lax.fori_loop(0, 4, own, 0)

    def unpack(patch, dslot):
        src = pl.ds(pl.multiple_of(dest_of(dslot) * members, members), members)
        box = patch * 3 + dslot

        def half(pair, carry):
            left = rb[box, pair * 25 + 24].astype(jnp.float32)
            for k in range(8):
                r, c0 = pair * 2 + k // 4, (k % 4) * 4
                p = [rb[box, pair * 25 + k * 3 + i].astype(jnp.float32) for i in range(3)]
                tail = [jnp.where(lane < 99, pltpu.roll(left, (96 - 3 * (4 * k + i)) % 128, 1), 0.0) for i in range(4)]
                for i in range(3):
                    gath[patch, r, c0 + i, src, 128:256] = jnp.where(lane < 96, p[i], tail[i]).astype(jnp.bfloat16)
                last = jnp.where(lane < 64, jnp.where(lane < 32, pltpu.roll(p[0], 32, 1), pltpu.roll(p[1], 64, 1)),
                                 jnp.where(lane < 96, pltpu.roll(p[2], 96, 1), tail[3]))
                gath[patch, r, c0 + 3, src, 128:256] = last.astype(jnp.bfloat16)
            return carry
        lax.fori_loop(0, 2, half, 0)

    def analysis(patch):
        def arrive(dslot, carry):
            for copy in unit_copies(patch, dslot):
                copy.wait_recv()
            unpack(patch, dslot)
            return carry
        lax.fori_loop(0, 3, lambda i, c: arrive(2 - i, c), 0)
        eye = (lax.broadcasted_iota(jnp.int32, (total_m, total_m), 0) == lax.broadcasted_iota(jnp.int32, (total_m, total_m), 1)).astype(jnp.float32)
        csum = jnp.zeros((total_m, CP), jnp.float32)
        for half in range(2):
            lhs = jnp.concatenate([gath[patch, :, half * 8 + j].reshape(4 * total_m, CP) for j in range(8)], axis=1)
            yb = jnp.dot(lhs, wobs[...], preferred_element_type=jnp.float32)
            for r in range(4):
                g = half * 4 + r
                y = yb[r * total_m:(r + 1) * total_m]
                ybar = jnp.sum(y, axis=0, keepdims=True) * (1.0 / total_m)
                y = y - ybar
                c = y * obs_row[1, patch, g:g + 1, :]
                csum = csum + c * (obs_row[0, patch, g:g + 1, :] - ybar)
                yp[g] = y
                cm[g] = c
        a_mat = (total_m - 1.0) * eye
        for g in range(8):
            a_mat = a_mat + f32dot(cm[g], yp[g], NT)
        amat[patch % 2, :, 0:total_m] = a_mat
        amat[patch % 2, :, total_m:2 * total_m] = a_mat
        cvec[patch % 2] = jnp.broadcast_to(jnp.sum(csum, axis=1, keepdims=True), (total_m, 2 * total_m))

    def solve(patch):
        row = lax.broadcasted_iota(jnp.int32, (total_m, 2 * total_m), 0)
        col = lax.broadcasted_iota(jnp.int32, (total_m, 2 * total_m), 1)
        eye = ((row == col) | (row + total_m == col)).astype(jnp.float32)
        first = col < total_m
        left = first.astype(jnp.float32).astype(jnp.bfloat16)
        right = (col >= total_m).astype(jnp.float32).astype(jnp.bfloat16)
        mats = jnp.where(first, amat[0], amat[1])
        diag = jnp.sum(mats * eye, axis=0, keepdims=True)
        trace = jnp.where(first[0:1], jnp.sum(jnp.where(first[0:1], diag, 0.0), axis=1, keepdims=True),
                          jnp.sum(jnp.where(first[0:1], 0.0, diag), axis=1, keepdims=True))

        def newton(step, carry):
            y, z = carry
            mix = 1.5 * eye - 0.5 * packed_dot(z, y, left, right)
            return packed_dot(y, mix, left, right), packed_dot(mix, z, left, right)
        _, inv = lax.fori_loop(0, NS_STEPS, newton, (mats / trace, eye))
        root = inv / jnp.sqrt(trace)
        wbar = packed_dot(root, packed_dot(root, jnp.where(first, cvec[0], cvec[1]), left, right), left, right)
        trans = math.sqrt(total_m - 1.0) * root + wbar
        trans = trans + (1.0 - jnp.sum(trans, axis=0, keepdims=True)) * (1.0 / total_m)
        both = trans.T
        tt_ref[patch] = both[0:total_m]
        tt_ref[patch + 1] = both[total_m:2 * total_m]

        @pl.when(patch < done)
        def _():
            def apply(i, carry):
                lhs = stacked(tt_ref[patch + i // 4])
                for c in range(columns):
                    gath[patch + i // 4, i % 4, c] = transform(lhs, gath[patch + i // 4, i % 4, c])
                return carry
            lax.fori_loop(0, 8, apply, 0)

    def step(v, carry):
        @pl.when(v < units)
        def _():
            prepare(v)

        @pl.when((v >= 1) & (v <= units))
        def _():
            forecast(v - 1)

        @pl.when(v == 3)
        def _():
            setup()

        @pl.when((v >= 12) & (v % 4 == 0))
        def _():
            analysis(v // 4 - 3)

        @pl.when((v >= 12) & (v % 8 == 0))
        def _():
            solve(v // 4 - 4)
        return carry
    lax.fori_loop(0, units + 9, step, 0)

    def finish(patch, carry):
        @pl.when(patch >= patches - 2)
        def _():
            for dslot in range(3):
                for copy in unit_copies(patch, dslot):
                    copy.wait_send()
        for dslot in range(4):
            ghost_copy(patch * 4 + dslot).wait_send()
        return carry
    lax.fori_loop(0, patches, finish, 0)


def update_kernel(done, tt_ref, g_ref, out_hbm, stage, sem):
    channels = out_hbm.shape[3]

    def copy(r):
        return pltpu.make_async_copy(stage.at[r], out_hbm.at[r], sem.at[r])

    def write(r, carry):
        for col in range(stage.shape[1]):
            stage[r, col] = g_ref[r // 4, r % 4, col, :, 0:channels]
        copy(r).start()
        return carry
    lax.fori_loop(0, 4 * done, write, 0)

    def last(r, carry):
        lhs = stacked(tt_ref[r // 4])
        for col in range(stage.shape[1]):
            stage[r, col] = transform(lhs, g_ref[r // 4, r % 4, col])[:, 0:channels]
        copy(r).start()
        return carry
    lax.fori_loop(4 * done, stage.shape[0], last, 0)

    def drain(r, carry):
        copy(r).wait()
        return carry
    lax.fori_loop(0, stage.shape[0], drain, 0)


def solution(mesh):
    ens_size = mesh.shape["ens"]
    obs_spec = P(None, None, "dom", None, None)

    def local_step(ens_state, w_in, w_out, obs_op, obs_val, obs_wt):
        members, rows, columns, channels = ens_state.shape
        total_m = members * ens_size
        dev_rows = rows // ens_size
        patches = dev_rows // 4
        units = patches * ens_size
        done = patches - 2
        dims = (members, rows, columns, channels, patches, dev_rows, ens_size, done)
        vmem = pl.BlockSpec(memory_space=pltpu.VMEM)
        anym = pl.BlockSpec(memory_space=pl.ANY)
        bf, f32 = jnp.bfloat16, jnp.float32
        dma = pltpu.SemaphoreType.DMA
        gathered, trans = pl.pallas_call(
            functools.partial(exchange_kernel, dims),
            out_shape=(pltpu.VMEM((patches, 4, columns, total_m, CP), bf),
                       pltpu.VMEM((patches, total_m, total_m), f32)),
            in_specs=[anym, vmem, vmem, vmem, anym, anym],
            out_specs=(vmem, vmem),
            scratch_shapes=[
                pltpu.VMEM((2, channels, columns, rows), bf),
                pltpu.VMEM((members, rows, columns, CP), bf),
                pltpu.VMEM((2, 2, 6, 544, 128), f32),
                pltpu.VMEM((2, 4, 544, 128), f32),
                pltpu.VMEM((members * columns, 2 * CP), bf),
                pltpu.VMEM((2, members * 17, 128), f32),
                pltpu.VMEM((4, columns, members, 128), f32),
                pltpu.VMEM((7, 4, columns, members, 128), bf),
                pltpu.VMEM((6, 50, members, 128), bf),
                pltpu.VMEM((patches * 3, 50, members, 128), bf),
                pltpu.VMEM((units, 2, 4, members, CP), bf),
                pltpu.VMEM((units, 2, 4, members, CP), bf),
                pltpu.VMEM((2 * CP, 512), bf),
                pltpu.VMEM((512, CP), bf),
                pltpu.VMEM((488, 512), f32),
                pltpu.VMEM((8 * CP, CP), bf),
                pltpu.VMEM((2, patches, 4, 1, columns, 32), f32),
                pltpu.VMEM((2, patches, 8, CP), f32),
                pltpu.VMEM((8, total_m, CP), f32),
                pltpu.VMEM((8, total_m, CP), f32),
                pltpu.VMEM((2, total_m, 2 * total_m), f32),
                pltpu.VMEM((2, total_m, 2 * total_m), f32),
                dma((2,)), dma((units,)), dma((units,)), dma((patches, 3, 2)), dma((patches, 3, 2)), dma((2,)),
            ],
            compiler_params=pltpu.CompilerParams(collective_id=0, has_side_effects=True, vmem_limit_bytes=46 * 1024 * 1024),
        )(ens_state.transpose(0, 3, 2, 1), w_in, w_out.T, obs_op.T, obs_val, obs_wt)
        return pl.pallas_call(
            functools.partial(update_kernel, done),
            out_shape=jax.ShapeDtypeStruct((dev_rows, columns, total_m, channels), bf),
            in_specs=[vmem, vmem],
            out_specs=anym,
            scratch_shapes=[pltpu.VMEM((dev_rows, columns, total_m, channels), bf), dma((dev_rows,))],
            compiler_params=pltpu.CompilerParams(vmem_limit_bytes=24 * 1024 * 1024),
        )(pltpu.with_memory_space_constraint(trans, pltpu.VMEM), pltpu.with_memory_space_constraint(gathered, pltpu.VMEM))

    return jax.shard_map(local_step, mesh=mesh, in_specs=(P("ens", None, "dom", None), P(), P(), P(), obs_spec, obs_spec), out_specs=P("ens", "dom", None, None), check_vma=False)
```

```python
import functools
import math
import jax
import jax.numpy as jnp
from jax import lax
from jax.experimental import pallas as pl
from jax.experimental.pallas import tpu as pltpu
from jax.sharding import PartitionSpec as P

NS_STEPS = 18
MESH = pl.DeviceIdType.MESH
CP = 256
NT = (((1,), (1,)), ((), ()))


NN = (((1,), (0,)), ((), ()))


def gelu(x):
    scale = math.sqrt(2.0 / math.pi)
    return (0.5 * x) * (1.0 + jnp.tanh(x * (scale + (scale * 0.044715) * (x * x))))


def split3(a):
    hi = a.astype(jnp.bfloat16)
    rem = a - hi.astype(jnp.float32)
    mid = rem.astype(jnp.bfloat16)
    low = (rem - mid.astype(jnp.float32)).astype(jnp.bfloat16)
    return hi, mid, low


def f32dot(a, b, dims=NN):
    ah, am, al = split3(a)
    bh, bm, bl = split3(b)
    n = a.shape[0]

    def dot(u, v):
        return lax.dot_general(u, v, dims, preferred_element_type=jnp.float32)
    by_hi = dot(jnp.concatenate([ah, am, al], axis=0), bh)
    by_mid = dot(jnp.concatenate([ah, am], axis=0), bm)
    by_low = dot(ah, bl)
    small = (by_low + by_hi[2 * n:]) + by_mid[n:]
    return (small + (by_mid[:n] + by_hi[n:2 * n])) + by_hi[:n]


def packed_dot(a, b, left, right):
    ah, am, al = split3(a)
    bh, bm, bl = split3(b)
    n = a.shape[0]

    def dot(u, v):
        blocks = jnp.concatenate([v * left, v * right], axis=0)
        return jnp.dot(u, blocks, preferred_element_type=jnp.float32)
    by_hi = dot(jnp.concatenate([ah, am, al], axis=0), bh)
    by_mid = dot(jnp.concatenate([ah, am], axis=0), bm)
    by_low = dot(ah, bl)
    small = (by_low + by_hi[2 * n:]) + by_mid[n:]
    return (small + (by_mid[:n] + by_hi[n:2 * n])) + by_hi[:n]


def stacked(t):
    hi, mid, low = (v.astype(jnp.float32) for v in split3(t))
    return jnp.concatenate([
        jnp.concatenate([hi, mid], axis=1),
        jnp.concatenate([low, jnp.zeros_like(low)], axis=1)], axis=0).astype(jnp.bfloat16)


def transform(lhs, g):
    n = lhs.shape[0] // 2
    res = jnp.dot(lhs, jnp.concatenate([g, g], axis=0), preferred_element_type=jnp.float32)
    return (res[n:] + res[:n]).astype(jnp.bfloat16)


def exchange_kernel(dims, xt_hbm, wi_ref, wo_ref, op_ref, yo_hbm, wt_hbm, gath, tt_ref,
                    xn, xb, xs, xa, xl, ts, t2, sb1, sb2, rb, gsend, grecv, wi, wo, wf, wobs, obs_raw, obs_row, yp, cm, amat, cvec,
                    xsem, gssem, grsem, ssem, rsem, osem):
    members, rows, columns, channels, patches, dev_rows, ens_size, done = dims
    units = patches * ens_size
    total_m = members * ens_size
    me = lax.axis_index("ens")
    mydom = lax.axis_index("dom")
    my_x, my_core = me // 2, me % 2
    mine = pl.ds(pl.multiple_of(me * members, members), members)

    def dest_of(dslot):
        dx = (my_x + 1 - dslot // 2) % 2
        dc = (my_core + (dslot + 1) // 2) % 2
        return dx * 2 + dc

    def x_copy(m):
        return pltpu.make_async_copy(xt_hbm.at[m], xn.at[m % 2], xsem.at[m % 2])

    def ghost_copy(unit):
        return pltpu.make_async_remote_copy(
            src_ref=gsend.at[unit], dst_ref=grecv.at[unit], send_sem=gssem.at[unit], recv_sem=grsem.at[unit],
            device_id={"dom": 1 - mydom}, device_id_type=MESH)

    def pair_copies(patch, dslot, pair):
        dev = {"ens": dest_of(dslot)}
        slot, box = (patch % 2) * 3 + dslot, patch * 3 + dslot
        two, tiles = pl.ds(pair * 2, 2), pl.ds(pair * 25, 25)
        first = pltpu.make_async_remote_copy(
            src_ref=sb1.at[slot, two], dst_ref=gath.at[patch, two, :, mine, pl.ds(0, 128)],
            send_sem=ssem.at[patch, dslot, pair * 2], recv_sem=rsem.at[patch, dslot, pair * 2],
            device_id=dev, device_id_type=MESH)
        second = pltpu.make_async_remote_copy(
            src_ref=sb2.at[slot, tiles], dst_ref=rb.at[box, tiles],
            send_sem=ssem.at[patch, dslot, pair * 2 + 1], recv_sem=rsem.at[patch, dslot, pair * 2 + 1],
            device_id=dev, device_id_type=MESH)
        return first, second

    def wait_sent(patch, dslot):
        for pair in range(2):
            for copy in pair_copies(patch, dslot, pair):
                copy.wait_send()

    obs_copies = [pltpu.make_async_copy(ref.at[pl.ds(me * patches, patches)], obs_raw.at[i], osem.at[i]) for i, ref in enumerate((yo_hbm, wt_hbm))]

    x_copy(0).start()
    x_copy(1).start()
    for copy in obs_copies:
        copy.start()
    barrier = pltpu.get_barrier_semaphore()
    for dslot in range(3):
        pl.semaphore_signal(barrier, inc=1, device_id={"ens": dest_of(dslot)}, device_id_type=MESH)
    pl.semaphore_signal(barrier, inc=1, device_id={"dom": 1 - mydom}, device_id_type=MESH)

    wf[...] = jnp.zeros_like(wf)
    wf[0:channels, :] = wo_ref[...].astype(jnp.float32)
    wo[...] = wf[0:CP, :].T.astype(jnp.bfloat16)
    wf[0:2 * channels, :] = wi_ref[...].astype(jnp.float32)
    keep = lax.broadcasted_iota(jnp.int32, (CP, 512), 0) < channels
    wi[0:CP, :] = jnp.where(keep, wf[0:CP, :], 0.0).astype(jnp.bfloat16)
    wi[CP:2 * CP, :] = wf[channels:channels + CP, :].astype(jnp.bfloat16)
    turn = (lax.broadcasted_iota(jnp.int32, (128, 128), 0) == lax.broadcasted_iota(jnp.int32, (128, 128), 1)).astype(jnp.float32).astype(jnp.bfloat16)

    wide = ([[xs.at[0, h, j] for j in range(4)] for h in range(2)],
            [[xs.at[j // 2, h, 4 + j % 2] for j in range(4)] for h in range(2)])
    turned = ([[xs.at[1, h, j] for j in range(4)] for h in range(2)],
              [[xa.at[h, j] for j in range(4)] for h in range(2)])

    def widen(odd, c):
        wide[odd][c // 128][c // 32 % 4][17 * (c % 32):17 * (c % 32) + 16, :] = xn[odd, c].astype(jnp.float32)

    def turn_column(odd, col):
        part = jnp.concatenate([wide[odd][h][j][pl.ds(col, 32, stride=17), :] for h in range(2) for j in range(4)], axis=0)
        out = lax.dot_general(turn, part.astype(jnp.bfloat16), NT, preferred_element_type=jnp.float32)
        for h in range(2):
            for j in range(4):
                turned[odd][h][j][pl.ds(col, 32, stride=17), :] = out[32 * j:32 * j + 32, h * 128:h * 128 + 128]

    def narrow(odd, m, row):
        for h in range(2):
            xb[m, row, :, h * 128:h * 128 + 128] = turned[odd][h][row // 32][17 * (row % 32):17 * (row % 32) + 16, :].astype(jnp.bfloat16)

    def relayout(t, carry):
        for odd in range(2):
            m = 2 * t + odd

            @pl.when(m + 2 < members)
            def _():
                x_copy(m + 2).start()

            @pl.when(m + 1 < members)
            def _():
                x_copy(m + 1).wait()
            for col in range(columns):
                turn_column(odd, col)
                for c in range(channels * col // columns, channels * (col + 1) // columns):
                    widen(1 - odd, c)
                for row in range(rows * col // columns, rows * (col + 1) // columns):
                    narrow(1 - odd, jnp.maximum(m - 1, 0), row)
        return carry
    for ref in (wide[0][1][3], wide[1][1][3]):
        ref[17 * (channels % 32):544, :] = jnp.zeros((544 - 17 * (channels % 32), 128), jnp.float32)
    x_copy(0).wait()
    for c in range(channels):
        widen(0, c)
    lax.fori_loop(0, members // 2, relayout, 0)

    for row in range(rows):
        narrow(1, members - 1, row)
    pl.semaphore_wait(barrier, 4)

    lane = lax.broadcasted_iota(jnp.int32, (members, 128), 1)

    def setup():
        wf[0:128, 0:CP] = jnp.zeros((128, CP), jnp.float32)
        wf[0:32, 0:channels] = op_ref[...].astype(jnp.float32)
        opt = wf[0:128, 0:CP].T.astype(jnp.bfloat16)
        for j in range(8):
            place = (lax.broadcasted_iota(jnp.int32, (128, CP), 1) == lax.broadcasted_iota(jnp.int32, (128, CP), 0) + 32 * j)
            wobs[j * CP:(j + 1) * CP, :] = jnp.dot(opt, place.astype(jnp.bfloat16), preferred_element_type=jnp.float32).astype(jnp.bfloat16)
        for copy in obs_copies:
            copy.wait()
        sub8 = lax.broadcasted_iota(jnp.int32, (8, 128), 0)
        lane8 = lax.broadcasted_iota(jnp.int32, (8, 128), 1) // 32
        wf[0:8, 0:128] = jnp.zeros((8, 128), jnp.float32)

        def rows_of(patch, carry):
            for i in range(2):
                for g in range(8):
                    wf[0:8, 0:32] = obs_raw[i, patch, g % 4, 0, (g // 4) * 8:(g // 4) * 8 + 8, :]
                    v = wf[0:8, 0:128]
                    v = v + pltpu.roll(v, 32, 1)
                    v = v + pltpu.roll(v, 64, 1)
                    for q in range(2):
                        obs_row[i, patch, g:g + 1, q * 128:q * 128 + 128] = jnp.sum(jnp.where(sub8 == lane8 + 4 * q, v, 0.0), axis=0, keepdims=True)
            return carry
        lax.fori_loop(0, patches, rows_of, 0)

    def prepare(unit):
        slot = unit % 2
        patch, dslot = unit // ens_size, unit % ens_size
        first = dest_of(dslot) * dev_rows + patch * 4

        def convert(r, carry):
            row = jnp.minimum(jnp.maximum(first + r - 1, 0), rows - 1)
            for m in range(members):
                for h in range(2):
                    xs[slot, h, r, 33 * m + 8:33 * m + 24, :] = xb[m, row, :, h * 128:h * 128 + 128].astype(jnp.float32)
            return carry
        lax.fori_loop(0, 6, convert, 0)

        def edges(r, carry):
            for h in range(2):
                gsend[unit, 0, r, :, h * 128:h * 128 + 128] = xs[slot, h, r + 1, pl.ds(23, members, stride=33), :].astype(jnp.bfloat16)
                gsend[unit, 1, r, :, h * 128:h * 128 + 128] = xs[slot, h, r + 1, pl.ds(8, members, stride=33), :].astype(jnp.bfloat16)
            return carry
        lax.fori_loop(0, 4, edges, 0)
        ghost_copy(unit).start()

    def forecast(unit):
        patch, dslot = unit // ens_size, unit % ens_size
        slot = unit % 2
        out_slot = jnp.where(dslot < 3, (patch % 2) * 3 + dslot, 6)

        @pl.when((dslot < 3) & (patch >= 2))
        def _():
            wait_sent(patch - 2, dslot)
        ghost_copy(unit).wait_recv()

        def block(r, carry):
            for h in range(2):
                xs[slot, h, r + 1, pl.ds(7, members, stride=33), :] = grecv[unit, 0, r, :, h * 128:h * 128 + 128].astype(jnp.float32)
                xs[slot, h, r + 1, pl.ds(24, members, stride=33), :] = grecv[unit, 1, r, :, h * 128:h * 128 + 128].astype(jnp.float32)
            for m in range(members):
                b = 33 * m
                for h in range(2):
                    cur = xs[slot, h, r + 1, b + 8:b + 24, :]
                    north = xs[slot, h, r, b + 8:b + 24, :]
                    south = xs[slot, h, r + 2, b + 8:b + 24, :]
                    west = xs[slot, h, r + 1, b + 7:b + 23, :]
                    east = xs[slot, h, r + 1, b + 9:b + 25, :]
                    lap = north + south + west + east - 4.0 * cur
                    xl[16 * m:16 * m + 16, h * 128:h * 128 + 128] = cur.astype(jnp.bfloat16)
                    xl[16 * m:16 * m + 16, CP + h * 128:CP + h * 128 + 128] = lap.astype(jnp.bfloat16)
            hidden = jnp.dot(xl[...], wi[...], preferred_element_type=jnp.float32)
            gel = gelu(hidden).astype(jnp.bfloat16)
            inc = jnp.dot(gel, wo[...], preferred_element_type=jnp.float32)
            for m in range(members):
                for h in range(2):
                    ts[h, 17 * m:17 * m + 16, :] = xs[slot, h, r + 1, 33 * m + 8:33 * m + 24, :] + inc[16 * m:16 * m + 16, h * 128:h * 128 + 128]
            for col in range(columns):
                sb1[out_slot, r, col] = ts[0, pl.ds(col, members, stride=17), :].astype(jnp.bfloat16)
                t2[r, col] = ts[1, pl.ds(col, members, stride=17), :]
            return carry

        def pack(pair):
            left = jnp.zeros((members, 128), jnp.float32)
            for k in range(8):
                r, c0 = pair * 2 + k // 4, (k % 4) * 4
                v = [t2[r, c0 + i] for i in range(4)]
                for i in range(3):
                    sb2[out_slot, pair * 25 + k * 3 + i] = jnp.where(lane < 96, v[i], pltpu.roll(v[3], 96 - 32 * i, 1)).astype(jnp.bfloat16)
                for i in range(4):
                    left = left + pltpu.roll(jnp.where(lane >= 96, v[i], 0.0), (32 + 3 * (4 * k + i)) % 128, 1)
            sb2[out_slot, pair * 25 + 24] = left.astype(jnp.bfloat16)

        def half_unit(pair, carry):
            lax.fori_loop(pair * 2, pair * 2 + 2, block, 0)

            @pl.when(dslot < 3)
            def _():
                pack(pair)
                for copy in pair_copies(patch, dslot, pair):
                    copy.start()

            @pl.when(dslot == 3)
            def _():
                def own(r, c2):
                    for col in range(columns):
                        gath[patch, r, col, mine, 0:128] = sb1[6, r, col]
                        gath[patch, r, col, mine, 128:256] = t2[r, col].astype(jnp.bfloat16)
                    return c2
                lax.fori_loop(pair * 2, pair * 2 + 2, own, 0)
            return carry
        lax.fori_loop(0, 2, half_unit, 0)

    def unpack(patch, dslot):
        src = pl.ds(pl.multiple_of(dest_of(dslot) * members, members), members)
        box = patch * 3 + dslot

        def half(pair, carry):
            for copy in pair_copies(patch, dslot, pair):
                copy.wait_recv()
            left = rb[box, pair * 25 + 24].astype(jnp.float32)
            for k in range(8):
                r, c0 = pair * 2 + k // 4, (k % 4) * 4
                p = [rb[box, pair * 25 + k * 3 + i].astype(jnp.float32) for i in range(3)]
                tail = [jnp.where(lane < 99, pltpu.roll(left, (96 - 3 * (4 * k + i)) % 128, 1), 0.0) for i in range(4)]
                for i in range(3):
                    gath[patch, r, c0 + i, src, 128:256] = jnp.where(lane < 96, p[i], tail[i]).astype(jnp.bfloat16)
                last = jnp.where(lane < 64, jnp.where(lane < 32, pltpu.roll(p[0], 32, 1), pltpu.roll(p[1], 64, 1)),
                                 jnp.where(lane < 96, pltpu.roll(p[2], 96, 1), tail[3]))
                gath[patch, r, c0 + 3, src, 128:256] = last.astype(jnp.bfloat16)
            return carry
        lax.fori_loop(0, 2, half, 0)

    def analysis(patch):
        def arrive(dslot, carry):
            unpack(patch, dslot)
            return carry
        lax.fori_loop(0, 3, lambda i, c: arrive(2 - i, c), 0)
        eye = (lax.broadcasted_iota(jnp.int32, (total_m, total_m), 0) == lax.broadcasted_iota(jnp.int32, (total_m, total_m), 1)).astype(jnp.float32)
        csum = jnp.zeros((total_m, CP), jnp.float32)
        for half in range(2):
            lhs = jnp.concatenate([gath[patch, :, half * 8 + j].reshape(4 * total_m, CP) for j in range(8)], axis=1)
            yb = jnp.dot(lhs, wobs[...], preferred_element_type=jnp.float32)
            for r in range(4):
                g = half * 4 + r
                y = yb[r * total_m:(r + 1) * total_m]
                ybar = jnp.sum(y, axis=0, keepdims=True) * (1.0 / total_m)
                y = y - ybar
                c = y * obs_row[1, patch, g:g + 1, :]
                csum = csum + c * (obs_row[0, patch, g:g + 1, :] - ybar)
                yp[g] = y
                cm[g] = c
        a_mat = (total_m - 1.0) * eye
        for g in range(8):
            a_mat = a_mat + f32dot(cm[g], yp[g], NT)
        amat[patch % 2, :, 0:total_m] = a_mat
        amat[patch % 2, :, total_m:2 * total_m] = a_mat
        cvec[patch % 2] = jnp.broadcast_to(jnp.sum(csum, axis=1, keepdims=True), (total_m, 2 * total_m))

    def solve(patch):
        row = lax.broadcasted_iota(jnp.int32, (total_m, 2 * total_m), 0)
        col = lax.broadcasted_iota(jnp.int32, (total_m, 2 * total_m), 1)
        eye = ((row == col) | (row + total_m == col)).astype(jnp.float32)
        first = col < total_m
        left = first.astype(jnp.float32).astype(jnp.bfloat16)
        right = (col >= total_m).astype(jnp.float32).astype(jnp.bfloat16)
        mats = jnp.where(first, amat[0], amat[1])
        diag = jnp.sum(mats * eye, axis=0, keepdims=True)
        trace = jnp.where(first[0:1], jnp.sum(jnp.where(first[0:1], diag, 0.0), axis=1, keepdims=True),
                          jnp.sum(jnp.where(first[0:1], 0.0, diag), axis=1, keepdims=True))

        def mixer(z, y):
            return 1.5 * eye - 0.5 * packed_dot(z, y, left, right)

        def newton(step, carry):
            y, z = carry
            mix = mixer(z, y)
            return packed_dot(y, mix, left, right), packed_dot(mix, z, left, right)
        scaled = mats / trace
        mix = 1.5 * eye - 0.5 * scaled
        y, z = lax.fori_loop(1, NS_STEPS - 1, newton, (packed_dot(scaled, mix, left, right), mix))
        inv = packed_dot(mixer(z, y), z, left, right)
        root = inv / jnp.sqrt(trace)
        wbar = packed_dot(root, packed_dot(root, jnp.where(first, cvec[0], cvec[1]), left, right), left, right)
        trans = math.sqrt(total_m - 1.0) * root + wbar
        trans = trans + (1.0 - jnp.sum(trans, axis=0, keepdims=True)) * (1.0 / total_m)
        both = trans.T
        tt_ref[patch] = both[0:total_m]
        tt_ref[patch + 1] = both[total_m:2 * total_m]

        @pl.when(patch < done)
        def _():
            def apply(i, carry):
                lhs = stacked(tt_ref[patch + i // 4])
                for c in range(columns):
                    gath[patch + i // 4, i % 4, c] = transform(lhs, gath[patch + i // 4, i % 4, c])
                return carry
            lax.fori_loop(0, 8, apply, 0)

    def step(v, carry):
        @pl.when(v < units)
        def _():
            prepare(v)

        @pl.when((v >= 1) & (v <= units))
        def _():
            forecast(v - 1)

        @pl.when(v == 0)
        def _():
            setup()

        @pl.when((v >= 12) & (v % 4 == 0))
        def _():
            analysis(v // 4 - 3)

        @pl.when((v >= 12) & (v % 8 == 0))
        def _():
            solve(v // 4 - 4)
        return carry
    lax.fori_loop(0, units + 9, step, 0)

    def finish(patch, carry):
        @pl.when(patch >= patches - 2)
        def _():
            for dslot in range(3):
                wait_sent(patch, dslot)
        for dslot in range(4):
            ghost_copy(patch * 4 + dslot).wait_send()
        return carry
    lax.fori_loop(0, patches, finish, 0)


def update_kernel(done, tt_ref, g_ref, out_hbm, stage, sem):
    channels = out_hbm.shape[3]

    def copy(r):
        return pltpu.make_async_copy(stage.at[r], out_hbm.at[r], sem.at[r])

    def write(r, carry):
        for col in range(stage.shape[1]):
            stage[r, col] = g_ref[r // 4, r % 4, col, :, 0:channels]
        copy(r).start()
        return carry
    lax.fori_loop(0, 4 * done, write, 0)

    def last(r, carry):
        lhs = stacked(tt_ref[r // 4])
        for col in range(stage.shape[1]):
            stage[r, col] = transform(lhs, g_ref[r // 4, r % 4, col])[:, 0:channels]
        copy(r).start()
        return carry
    lax.fori_loop(4 * done, stage.shape[0], last, 0)

    def drain(r, carry):
        copy(r).wait()
        return carry
    lax.fori_loop(0, stage.shape[0], drain, 0)


def solution(mesh):
    ens_size = mesh.shape["ens"]
    obs_spec = P(None, None, "dom", None, None)

    def local_step(ens_state, w_in, w_out, obs_op, obs_val, obs_wt):
        members, rows, columns, channels = ens_state.shape
        total_m = members * ens_size
        dev_rows = rows // ens_size
        patches = dev_rows // 4
        units = patches * ens_size
        done = patches - 2
        dims = (members, rows, columns, channels, patches, dev_rows, ens_size, done)
        vmem = pl.BlockSpec(memory_space=pltpu.VMEM)
        anym = pl.BlockSpec(memory_space=pl.ANY)
        bf, f32 = jnp.bfloat16, jnp.float32
        dma = pltpu.SemaphoreType.DMA
        gathered, trans = pl.pallas_call(
            functools.partial(exchange_kernel, dims),
            out_shape=(pltpu.VMEM((patches, 4, columns, total_m, CP), bf),
                       pltpu.VMEM((patches, total_m, total_m), f32)),
            in_specs=[anym, vmem, vmem, vmem, anym, anym],
            out_specs=(vmem, vmem),
            scratch_shapes=[
                pltpu.VMEM((2, channels, columns, rows), bf),
                pltpu.VMEM((members, rows, columns, CP), bf),
                pltpu.VMEM((2, 2, 6, 544, 128), f32),
                pltpu.VMEM((2, 4, 544, 128), f32),
                pltpu.VMEM((members * columns, 2 * CP), bf),
                pltpu.VMEM((2, members * 17, 128), f32),
                pltpu.VMEM((4, columns, members, 128), f32),
                pltpu.VMEM((7, 4, columns, members, 128), bf),
                pltpu.VMEM((6, 50, members, 128), bf),
                pltpu.VMEM((patches * 3, 50, members, 128), bf),
                pltpu.VMEM((units, 2, 4, members, CP), bf),
                pltpu.VMEM((units, 2, 4, members, CP), bf),
                pltpu.VMEM((2 * CP, 512), bf),
                pltpu.VMEM((512, CP), bf),
                pltpu.VMEM((488, 512), f32),
                pltpu.VMEM((8 * CP, CP), bf),
                pltpu.VMEM((2, patches, 4, 1, columns, 32), f32),
                pltpu.VMEM((2, patches, 8, CP), f32),
                pltpu.VMEM((8, total_m, CP), f32),
                pltpu.VMEM((8, total_m, CP), f32),
                pltpu.VMEM((2, total_m, 2 * total_m), f32),
                pltpu.VMEM((2, total_m, 2 * total_m), f32),
                dma((2,)), dma((units,)), dma((units,)), dma((patches, 3, 4)), dma((patches, 3, 4)), dma((2,)),
            ],
            compiler_params=pltpu.CompilerParams(collective_id=0, has_side_effects=True, vmem_limit_bytes=46 * 1024 * 1024),
        )(ens_state.transpose(0, 3, 2, 1), w_in, w_out.T, obs_op.T, obs_val, obs_wt)
        return pl.pallas_call(
            functools.partial(update_kernel, done),
            out_shape=jax.ShapeDtypeStruct((dev_rows, columns, total_m, channels), bf),
            in_specs=[vmem, vmem],
            out_specs=anym,
            scratch_shapes=[pltpu.VMEM((dev_rows, columns, total_m, channels), bf), dma((dev_rows,))],
            compiler_params=pltpu.CompilerParams(vmem_limit_bytes=24 * 1024 * 1024),
        )(pltpu.with_memory_space_constraint(trans, pltpu.VMEM), pltpu.with_memory_space_constraint(gathered, pltpu.VMEM))

    return jax.shard_map(local_step, mesh=mesh, in_specs=(P("ens", None, "dom", None), P(), P(), P(), obs_spec, obs_spec), out_specs=P("ens", "dom", None, None), check_vma=False)
```

```python
import functools
import math
import jax
import jax.numpy as jnp
from jax import lax
from jax.experimental import pallas as pl
from jax.experimental.pallas import tpu as pltpu
from jax.sharding import PartitionSpec as P

NS_STEPS = 18
MESH = pl.DeviceIdType.MESH
CP = 256
NT = (((1,), (1,)), ((), ()))


NN = (((1,), (0,)), ((), ()))


def gelu(x):
    scale = math.sqrt(2.0 / math.pi)
    return (0.5 * x) * (1.0 + jnp.tanh(x * (scale + (scale * 0.044715) * (x * x))))


def split3(a):
    hi = a.astype(jnp.bfloat16)
    rem = a - hi.astype(jnp.float32)
    mid = rem.astype(jnp.bfloat16)
    low = (rem - mid.astype(jnp.float32)).astype(jnp.bfloat16)
    return hi, mid, low


def f32dot(a, b, dims=NN):
    ah, am, al = split3(a)
    bh, bm, bl = split3(b)
    n = a.shape[0]

    def dot(u, v):
        return lax.dot_general(u, v, dims, preferred_element_type=jnp.float32)
    by_hi = dot(jnp.concatenate([ah, am, al], axis=0), bh)
    by_mid = dot(jnp.concatenate([ah, am], axis=0), bm)
    by_low = dot(ah, bl)
    small = (by_low + by_hi[2 * n:]) + by_mid[n:]
    return (small + (by_mid[:n] + by_hi[n:2 * n])) + by_hi[:n]


def packed_dot(a, b, left, right):
    ah, am, al = split3(a)
    bh, bm, bl = split3(b)
    n = a.shape[0]

    def dot(u, v):
        blocks = jnp.concatenate([v * left, v * right], axis=0)
        return jnp.dot(u, blocks, preferred_element_type=jnp.float32)
    by_hi = dot(jnp.concatenate([ah, am, al], axis=0), bh)
    by_mid = dot(jnp.concatenate([ah, am], axis=0), bm)
    by_low = dot(ah, bl)
    small = (by_low + by_hi[2 * n:]) + by_mid[n:]
    return (small + (by_mid[:n] + by_hi[n:2 * n])) + by_hi[:n]


def stacked(t):
    hi, mid, low = (v.astype(jnp.float32) for v in split3(t))
    return jnp.concatenate([
        jnp.concatenate([hi, mid], axis=1),
        jnp.concatenate([low, jnp.zeros_like(low)], axis=1)], axis=0).astype(jnp.bfloat16)


def transform(lhs, g):
    n = lhs.shape[0] // 2
    res = jnp.dot(lhs, jnp.concatenate([g, g], axis=0), preferred_element_type=jnp.float32)
    return (res[n:] + res[:n]).astype(jnp.bfloat16)


def exchange_kernel(dims, xt_hbm, wi_ref, wo_ref, op_ref, yo_hbm, wt_hbm, gath, tt_ref,
                    xn, xb, xs, xa, xl, ts, t2, sb1, sb2, rb, gsend, grecv, wi, wo, wf, wobs, obs_raw, obs_row, yp, cm, amat, cvec,
                    xsem, gssem, grsem, ssem, rsem, osem):
    members, rows, columns, channels, patches, dev_rows, ens_size, done = dims
    units = patches * ens_size
    total_m = members * ens_size
    me = lax.axis_index("ens")
    mydom = lax.axis_index("dom")
    my_x, my_core = me // 2, me % 2
    mine = pl.ds(pl.multiple_of(me * members, members), members)

    def dest_of(dslot):
        dx = (my_x + 1 - dslot // 2) % 2
        dc = (my_core + (dslot + 1) // 2) % 2
        return dx * 2 + dc

    def x_copy(m):
        return pltpu.make_async_copy(xt_hbm.at[m], xn.at[m % 2], xsem.at[m % 2])

    def ghost_copy(unit):
        return pltpu.make_async_remote_copy(
            src_ref=gsend.at[unit % 8], dst_ref=grecv.at[unit], send_sem=gssem.at[unit], recv_sem=grsem.at[unit],
            device_id={"dom": 1 - mydom}, device_id_type=MESH)

    def pair_copies(patch, dslot, pair):
        dev = {"ens": dest_of(dslot)}
        slot, box = (patch % 4) * 3 + dslot, patch * 3 + dslot
        two, tiles = pl.ds(pair * 2, 2), pl.ds(pair * 25, 25)
        first = pltpu.make_async_remote_copy(
            src_ref=sb1.at[slot, two], dst_ref=gath.at[patch, two, :, mine, pl.ds(0, 128)],
            send_sem=ssem.at[patch, dslot, pair * 2], recv_sem=rsem.at[patch, dslot, pair * 2],
            device_id=dev, device_id_type=MESH)
        second = pltpu.make_async_remote_copy(
            src_ref=sb2.at[slot, tiles], dst_ref=rb.at[box, tiles],
            send_sem=ssem.at[patch, dslot, pair * 2 + 1], recv_sem=rsem.at[patch, dslot, pair * 2 + 1],
            device_id=dev, device_id_type=MESH)
        return first, second

    def wait_sent(patch, dslot):
        for pair in range(2):
            for copy in pair_copies(patch, dslot, pair):
                copy.wait_send()

    obs_copies = [pltpu.make_async_copy(ref.at[pl.ds(me * patches, patches)], obs_raw.at[i], osem.at[i]) for i, ref in enumerate((yo_hbm, wt_hbm))]

    x_copy(0).start()
    x_copy(1).start()
    for copy in obs_copies:
        copy.start()
    barrier = pltpu.get_barrier_semaphore()
    for dslot in range(3):
        pl.semaphore_signal(barrier, inc=1, device_id={"ens": dest_of(dslot)}, device_id_type=MESH)
    pl.semaphore_signal(barrier, inc=1, device_id={"dom": 1 - mydom}, device_id_type=MESH)

    wf[...] = jnp.zeros_like(wf)
    wf[0:channels, :] = wo_ref[...].astype(jnp.float32)
    wo[...] = wf[0:CP, :].T.astype(jnp.bfloat16)
    wf[0:2 * channels, :] = wi_ref[...].astype(jnp.float32)
    keep = lax.broadcasted_iota(jnp.int32, (CP, 512), 0) < channels
    wi[0:CP, :] = jnp.where(keep, wf[0:CP, :], 0.0).astype(jnp.bfloat16)
    wi[CP:2 * CP, :] = wf[channels:channels + CP, :].astype(jnp.bfloat16)
    turn = (lax.broadcasted_iota(jnp.int32, (128, 128), 0) == lax.broadcasted_iota(jnp.int32, (128, 128), 1)).astype(jnp.float32).astype(jnp.bfloat16)

    wide = ([[xs.at[0, h, j] for j in range(4)] for h in range(2)],
            [[xs.at[j // 2, h, 4 + j % 2] for j in range(4)] for h in range(2)])
    turned = ([[xs.at[1, h, j] for j in range(4)] for h in range(2)],
              [[xa.at[h, j] for j in range(4)] for h in range(2)])

    def widen(odd, c):
        wide[odd][c // 128][c // 32 % 4][17 * (c % 32):17 * (c % 32) + 16, :] = xn[odd, c].astype(jnp.float32)

    def turn_column(odd, col):
        part = jnp.concatenate([wide[odd][h][j][pl.ds(col, 32, stride=17), :] for h in range(2) for j in range(4)], axis=0)
        out = lax.dot_general(turn, part.astype(jnp.bfloat16), NT, preferred_element_type=jnp.float32)
        for h in range(2):
            for j in range(4):
                turned[odd][h][j][pl.ds(col, 32, stride=17), :] = out[32 * j:32 * j + 32, h * 128:h * 128 + 128]

    def narrow(odd, m, row):
        for h in range(2):
            xb[m, row, :, h * 128:h * 128 + 128] = turned[odd][h][row // 32][17 * (row % 32):17 * (row % 32) + 16, :].astype(jnp.bfloat16)

    def relayout(t, carry):
        for odd in range(2):
            m = 2 * t + odd

            @pl.when(m + 2 < members)
            def _():
                x_copy(m + 2).start()

            @pl.when(m + 1 < members)
            def _():
                x_copy(m + 1).wait()
            for col in range(columns):
                turn_column(odd, col)
                for c in range(channels * col // columns, channels * (col + 1) // columns):
                    widen(1 - odd, c)
                for row in range(rows * col // columns, rows * (col + 1) // columns):
                    narrow(1 - odd, jnp.maximum(m - 1, 0), row)
        return carry
    for ref in (wide[0][1][3], wide[1][1][3]):
        ref[17 * (channels % 32):544, :] = jnp.zeros((544 - 17 * (channels % 32), 128), jnp.float32)
    x_copy(0).wait()
    for c in range(channels):
        widen(0, c)
    lax.fori_loop(0, members // 2, relayout, 0)

    for row in range(rows):
        narrow(1, members - 1, row)
    pl.semaphore_wait(barrier, 4)

    lane = lax.broadcasted_iota(jnp.int32, (members, 128), 1)

    def setup():
        wf[0:128, 0:CP] = jnp.zeros((128, CP), jnp.float32)
        wf[0:32, 0:channels] = op_ref[...].astype(jnp.float32)
        opt = wf[0:128, 0:CP].T.astype(jnp.bfloat16)
        for j in range(8):
            place = (lax.broadcasted_iota(jnp.int32, (128, CP), 1) == lax.broadcasted_iota(jnp.int32, (128, CP), 0) + 32 * j)
            wobs[j * CP:(j + 1) * CP, :] = jnp.dot(opt, place.astype(jnp.bfloat16), preferred_element_type=jnp.float32).astype(jnp.bfloat16)
        for copy in obs_copies:
            copy.wait()
        sub8 = lax.broadcasted_iota(jnp.int32, (8, 128), 0)
        lane8 = lax.broadcasted_iota(jnp.int32, (8, 128), 1) // 32
        wf[0:8, 0:128] = jnp.zeros((8, 128), jnp.float32)

        def rows_of(patch, carry):
            for i in range(2):
                for g in range(8):
                    wf[0:8, 0:32] = obs_raw[i, patch, g % 4, 0, (g // 4) * 8:(g // 4) * 8 + 8, :]
                    v = wf[0:8, 0:128]
                    v = v + pltpu.roll(v, 32, 1)
                    v = v + pltpu.roll(v, 64, 1)
                    for q in range(2):
                        obs_row[i, patch, g:g + 1, q * 128:q * 128 + 128] = jnp.sum(jnp.where(sub8 == lane8 + 4 * q, v, 0.0), axis=0, keepdims=True)
            return carry
        lax.fori_loop(0, patches, rows_of, 0)

    def prepare(unit):
        slot = unit % 2
        patch, dslot = unit // ens_size, unit % ens_size
        first = dest_of(dslot) * dev_rows + patch * 4

        def convert(r, carry):
            row = jnp.minimum(jnp.maximum(first + r - 1, 0), rows - 1)
            for m in range(members):
                for h in range(2):
                    xs[slot, h, r, 33 * m + 8:33 * m + 24, :] = xb[m, row, :, h * 128:h * 128 + 128].astype(jnp.float32)
            return carry
        lax.fori_loop(0, 6, convert, 0)

        @pl.when(unit >= 8)
        def _():
            ghost_copy(unit - 8).wait_send()

        def edges(r, carry):
            for h in range(2):
                gsend[unit % 8, 0, r, :, h * 128:h * 128 + 128] = xs[slot, h, r + 1, pl.ds(23, members, stride=33), :].astype(jnp.bfloat16)
                gsend[unit % 8, 1, r, :, h * 128:h * 128 + 128] = xs[slot, h, r + 1, pl.ds(8, members, stride=33), :].astype(jnp.bfloat16)
            return carry
        lax.fori_loop(0, 4, edges, 0)
        ghost_copy(unit).start()

    def forecast(unit):
        patch, dslot = unit // ens_size, unit % ens_size
        slot = unit % 2
        out_slot = jnp.where(dslot < 3, (patch % 4) * 3 + dslot, 12)

        @pl.when((dslot < 3) & (patch >= 4))
        def _():
            wait_sent(patch - 4, dslot)
        ghost_copy(unit).wait_recv()

        def block(r, carry):
            for h in range(2):
                xs[slot, h, r + 1, pl.ds(7, members, stride=33), :] = grecv[unit, 0, r, :, h * 128:h * 128 + 128].astype(jnp.float32)
                xs[slot, h, r + 1, pl.ds(24, members, stride=33), :] = grecv[unit, 1, r, :, h * 128:h * 128 + 128].astype(jnp.float32)
            for m in range(members):
                b = 33 * m
                for h in range(2):
                    cur = xs[slot, h, r + 1, b + 8:b + 24, :]
                    north = xs[slot, h, r, b + 8:b + 24, :]
                    south = xs[slot, h, r + 2, b + 8:b + 24, :]
                    west = xs[slot, h, r + 1, b + 7:b + 23, :]
                    east = xs[slot, h, r + 1, b + 9:b + 25, :]
                    lap = north + south + west + east - 4.0 * cur
                    xl[16 * m:16 * m + 16, h * 128:h * 128 + 128] = cur.astype(jnp.bfloat16)
                    xl[16 * m:16 * m + 16, CP + h * 128:CP + h * 128 + 128] = lap.astype(jnp.bfloat16)
            hidden = jnp.dot(xl[...], wi[...], preferred_element_type=jnp.float32)
            gel = gelu(hidden).astype(jnp.bfloat16)
            inc = jnp.dot(gel, wo[...], preferred_element_type=jnp.float32)
            for m in range(members):
                for h in range(2):
                    ts[h, 17 * m:17 * m + 16, :] = xs[slot, h, r + 1, 33 * m + 8:33 * m + 24, :] + inc[16 * m:16 * m + 16, h * 128:h * 128 + 128]
            for col in range(columns):
                sb1[out_slot, r, col] = ts[0, pl.ds(col, members, stride=17), :].astype(jnp.bfloat16)
                t2[r, col] = ts[1, pl.ds(col, members, stride=17), :]
            return carry

        def pack(pair):
            left = jnp.zeros((members, 128), jnp.float32)
            for k in range(8):
                r, c0 = pair * 2 + k // 4, (k % 4) * 4
                v = [t2[r, c0 + i] for i in range(4)]
                for i in range(3):
                    sb2[out_slot, pair * 25 + k * 3 + i] = jnp.where(lane < 96, v[i], pltpu.roll(v[3], 96 - 32 * i, 1)).astype(jnp.bfloat16)
                for i in range(4):
                    left = left + pltpu.roll(jnp.where(lane >= 96, v[i], 0.0), (32 + 3 * (4 * k + i)) % 128, 1)
            sb2[out_slot, pair * 25 + 24] = left.astype(jnp.bfloat16)

        def half_unit(pair, carry):
            lax.fori_loop(pair * 2, pair * 2 + 2, block, 0)

            @pl.when(dslot < 3)
            def _():
                pack(pair)
                for copy in pair_copies(patch, dslot, pair):
                    copy.start()

            @pl.when(dslot == 3)
            def _():
                def own(r, c2):
                    for col in range(columns):
                        gath[patch, r, col, mine, 0:128] = sb1[12, r, col]
                        gath[patch, r, col, mine, 128:256] = t2[r, col].astype(jnp.bfloat16)
                    return c2
                lax.fori_loop(pair * 2, pair * 2 + 2, own, 0)
            return carry
        lax.fori_loop(0, 2, half_unit, 0)

    def unpack(patch, dslot):
        src = pl.ds(pl.multiple_of(dest_of(dslot) * members, members), members)
        box = patch * 3 + dslot

        def half(pair, carry):
            for copy in pair_copies(patch, dslot, pair):
                copy.wait_recv()
            left = rb[box, pair * 25 + 24].astype(jnp.float32)
            for k in range(8):
                r, c0 = pair * 2 + k // 4, (k % 4) * 4
                p = [rb[box, pair * 25 + k * 3 + i].astype(jnp.float32) for i in range(3)]
                tail = [jnp.where(lane < 99, pltpu.roll(left, (96 - 3 * (4 * k + i)) % 128, 1), 0.0) for i in range(4)]
                for i in range(3):
                    gath[patch, r, c0 + i, src, 128:256] = jnp.where(lane < 96, p[i], tail[i]).astype(jnp.bfloat16)
                last = jnp.where(lane < 64, jnp.where(lane < 32, pltpu.roll(p[0], 32, 1), pltpu.roll(p[1], 64, 1)),
                                 jnp.where(lane < 96, pltpu.roll(p[2], 96, 1), tail[3]))
                gath[patch, r, c0 + 3, src, 128:256] = last.astype(jnp.bfloat16)
            return carry
        lax.fori_loop(0, 2, half, 0)

    def analysis(patch):
        def arrive(dslot, carry):
            unpack(patch, dslot)
            return carry
        lax.fori_loop(0, 3, lambda i, c: arrive(2 - i, c), 0)
        eye = (lax.broadcasted_iota(jnp.int32, (total_m, total_m), 0) == lax.broadcasted_iota(jnp.int32, (total_m, total_m), 1)).astype(jnp.float32)
        csum = jnp.zeros((total_m, CP), jnp.float32)
        for half in range(2):
            lhs = jnp.concatenate([gath[patch, :, half * 8 + j].reshape(4 * total_m, CP) for j in range(8)], axis=1)
            yb = jnp.dot(lhs, wobs[...], preferred_element_type=jnp.float32)
            for r in range(4):
                g = half * 4 + r
                y = yb[r * total_m:(r + 1) * total_m]
                ybar = jnp.sum(y, axis=0, keepdims=True) * (1.0 / total_m)
                y = y - ybar
                c = y * obs_row[1, patch, g:g + 1, :]
                csum = csum + c * (obs_row[0, patch, g:g + 1, :] - ybar)
                yp[g] = y
                cm[g] = c
        a_mat = (total_m - 1.0) * eye
        for g in range(8):
            a_mat = a_mat + f32dot(cm[g], yp[g], NT)
        amat[patch % 2, :, 0:total_m] = a_mat
        amat[patch % 2, :, total_m:2 * total_m] = a_mat
        cvec[patch % 2] = jnp.broadcast_to(jnp.sum(csum, axis=1, keepdims=True), (total_m, 2 * total_m))

    def solve(patch):
        row = lax.broadcasted_iota(jnp.int32, (total_m, 2 * total_m), 0)
        col = lax.broadcasted_iota(jnp.int32, (total_m, 2 * total_m), 1)
        eye = ((row == col) | (row + total_m == col)).astype(jnp.float32)
        first = col < total_m
        left = first.astype(jnp.float32).astype(jnp.bfloat16)
        right = (col >= total_m).astype(jnp.float32).astype(jnp.bfloat16)
        mats = jnp.where(first, amat[0], amat[1])
        diag = jnp.sum(mats * eye, axis=0, keepdims=True)
        trace = jnp.where(first[0:1], jnp.sum(jnp.where(first[0:1], diag, 0.0), axis=1, keepdims=True),
                          jnp.sum(jnp.where(first[0:1], 0.0, diag), axis=1, keepdims=True))

        def mixer(z, y):
            return 1.5 * eye - 0.5 * packed_dot(z, y, left, right)

        def newton(step, carry):
            y, z = carry
            mix = mixer(z, y)
            return packed_dot(y, mix, left, right), packed_dot(mix, z, left, right)
        scaled = mats / trace
        mix = 1.5 * eye - 0.5 * scaled
        y, z = lax.fori_loop(1, NS_STEPS - 1, newton, (packed_dot(scaled, mix, left, right), mix))
        inv = packed_dot(mixer(z, y), z, left, right)
        root = inv / jnp.sqrt(trace)
        wbar = packed_dot(root, packed_dot(root, jnp.where(first, cvec[0], cvec[1]), left, right), left, right)
        trans = math.sqrt(total_m - 1.0) * root + wbar
        trans = trans + (1.0 - jnp.sum(trans, axis=0, keepdims=True)) * (1.0 / total_m)
        both = trans.T
        tt_ref[patch] = both[0:total_m]
        tt_ref[patch + 1] = both[total_m:2 * total_m]

        @pl.when(patch < done)
        def _():
            def apply(i, carry):
                lhs = stacked(tt_ref[patch + i // 4])
                for c in range(columns):
                    gath[patch + i // 4, i % 4, c] = transform(lhs, gath[patch + i // 4, i % 4, c])
                return carry
            lax.fori_loop(0, 8, apply, 0)

    def step(v, carry):
        @pl.when(v < units)
        def _():
            prepare(v)

        @pl.when((v >= 1) & (v <= units))
        def _():
            forecast(v - 1)

        @pl.when(v == 0)
        def _():
            setup()

        @pl.when((v >= 16) & (v % 4 == 0))
        def _():
            analysis(v // 4 - 4)

        @pl.when((v >= 16) & (v % 8 == 4))
        def _():
            solve(v // 4 - 5)
        return carry
    lax.fori_loop(0, units + 13, step, 0)

    def finish(patch, carry):
        @pl.when(patch >= patches - 4)
        def _():
            for dslot in range(3):
                wait_sent(patch, dslot)
        @pl.when(patch >= patches - 2)
        def _():
            for dslot in range(4):
                ghost_copy(patch * 4 + dslot).wait_send()
        return carry
    lax.fori_loop(0, patches, finish, 0)


def update_kernel(done, tt_ref, g_ref, out_hbm, stage, sem):
    channels = out_hbm.shape[3]

    def copy(r):
        return pltpu.make_async_copy(stage.at[r], out_hbm.at[r], sem.at[r])

    def write(r, carry):
        for col in range(stage.shape[1]):
            stage[r, col] = g_ref[r // 4, r % 4, col, :, 0:channels]
        copy(r).start()
        return carry
    lax.fori_loop(0, 4 * done, write, 0)

    def last(r, carry):
        lhs = stacked(tt_ref[r // 4])
        for col in range(stage.shape[1]):
            stage[r, col] = transform(lhs, g_ref[r // 4, r % 4, col])[:, 0:channels]
        copy(r).start()
        return carry
    lax.fori_loop(4 * done, stage.shape[0], last, 0)

    def drain(r, carry):
        copy(r).wait()
        return carry
    lax.fori_loop(0, stage.shape[0], drain, 0)


def solution(mesh):
    ens_size = mesh.shape["ens"]
    obs_spec = P(None, None, "dom", None, None)

    def local_step(ens_state, w_in, w_out, obs_op, obs_val, obs_wt):
        members, rows, columns, channels = ens_state.shape
        total_m = members * ens_size
        dev_rows = rows // ens_size
        patches = dev_rows // 4
        units = patches * ens_size
        done = patches - 2
        dims = (members, rows, columns, channels, patches, dev_rows, ens_size, done)
        vmem = pl.BlockSpec(memory_space=pltpu.VMEM)
        anym = pl.BlockSpec(memory_space=pl.ANY)
        bf, f32 = jnp.bfloat16, jnp.float32
        dma = pltpu.SemaphoreType.DMA
        gathered, trans = pl.pallas_call(
            functools.partial(exchange_kernel, dims),
            out_shape=(pltpu.VMEM((patches, 4, columns, total_m, CP), bf),
                       pltpu.VMEM((patches, total_m, total_m), f32)),
            in_specs=[anym, vmem, vmem, vmem, anym, anym],
            out_specs=(vmem, vmem),
            scratch_shapes=[
                pltpu.VMEM((2, channels, columns, rows), bf),
                pltpu.VMEM((members, rows, columns, CP), bf),
                pltpu.VMEM((2, 2, 6, 544, 128), f32),
                pltpu.VMEM((2, 4, 544, 128), f32),
                pltpu.VMEM((members * columns, 2 * CP), bf),
                pltpu.VMEM((2, members * 17, 128), f32),
                pltpu.VMEM((4, columns, members, 128), f32),
                pltpu.VMEM((13, 4, columns, members, 128), bf),
                pltpu.VMEM((12, 50, members, 128), bf),
                pltpu.VMEM((patches * 3, 50, members, 128), bf),
                pltpu.VMEM((8, 2, 4, members, CP), bf),
                pltpu.VMEM((units, 2, 4, members, CP), bf),
                pltpu.VMEM((2 * CP, 512), bf),
                pltpu.VMEM((512, CP), bf),
                pltpu.VMEM((488, 512), f32),
                pltpu.VMEM((8 * CP, CP), bf),
                pltpu.VMEM((2, patches, 4, 1, columns, 32), f32),
                pltpu.VMEM((2, patches, 8, CP), f32),
                pltpu.VMEM((8, total_m, CP), f32),
                pltpu.VMEM((8, total_m, CP), f32),
                pltpu.VMEM((2, total_m, 2 * total_m), f32),
                pltpu.VMEM((2, total_m, 2 * total_m), f32),
                dma((2,)), dma((units,)), dma((units,)), dma((patches, 3, 4)), dma((patches, 3, 4)), dma((2,)),
            ],
            compiler_params=pltpu.CompilerParams(collective_id=0, has_side_effects=True, vmem_limit_bytes=46 * 1024 * 1024),
        )(ens_state.transpose(0, 3, 2, 1), w_in, w_out.T, obs_op.T, obs_val, obs_wt)
        return pl.pallas_call(
            functools.partial(update_kernel, done),
            out_shape=jax.ShapeDtypeStruct((dev_rows, columns, total_m, channels), bf),
            in_specs=[vmem, vmem],
            out_specs=anym,
            scratch_shapes=[pltpu.VMEM((dev_rows, columns, total_m, channels), bf), dma((dev_rows,))],
            compiler_params=pltpu.CompilerParams(vmem_limit_bytes=24 * 1024 * 1024),
        )(pltpu.with_memory_space_constraint(trans, pltpu.VMEM), pltpu.with_memory_space_constraint(gathered, pltpu.VMEM))

    return jax.shard_map(local_step, mesh=mesh, in_specs=(P("ens", None, "dom", None), P(), P(), P(), obs_spec, obs_spec), out_specs=P("ens", "dom", None, None), check_vma=False)
```

```python
import functools
import math
import jax
import jax.numpy as jnp
from jax import lax
from jax.experimental import pallas as pl
from jax.experimental.pallas import tpu as pltpu
from jax.sharding import PartitionSpec as P

NS_STEPS = 18
MESH = pl.DeviceIdType.MESH
CP = 256
NT = (((1,), (1,)), ((), ()))


NN = (((1,), (0,)), ((), ()))


def gelu(x):
    scale = math.sqrt(2.0 / math.pi)
    return (0.5 * x) * (1.0 + jnp.tanh(x * (scale + (scale * 0.044715) * (x * x))))


def split3(a):
    hi = a.astype(jnp.bfloat16)
    rem = a - hi.astype(jnp.float32)
    mid = rem.astype(jnp.bfloat16)
    low = (rem - mid.astype(jnp.float32)).astype(jnp.bfloat16)
    return hi, mid, low


def f32dot(a, b, dims=NN):
    ah, am, al = split3(a)
    bh, bm, bl = split3(b)
    n = a.shape[0]

    def dot(u, v):
        return lax.dot_general(u, v, dims, preferred_element_type=jnp.float32)
    by_hi = dot(jnp.concatenate([ah, am, al], axis=0), bh)
    by_mid = dot(jnp.concatenate([ah, am], axis=0), bm)
    by_low = dot(ah, bl)
    small = (by_low + by_hi[2 * n:]) + by_mid[n:]
    return (small + (by_mid[:n] + by_hi[n:2 * n])) + by_hi[:n]


def packed_dot(a, b, left, right):
    ah, am, al = split3(a)
    bh, bm, bl = split3(b)
    n = a.shape[0]

    def dot(u, v):
        blocks = jnp.concatenate([v * left, v * right], axis=0)
        return jnp.dot(u, blocks, preferred_element_type=jnp.float32)
    by_hi = dot(jnp.concatenate([ah, am, al], axis=0), bh)
    by_mid = dot(jnp.concatenate([ah, am], axis=0), bm)
    by_low = dot(ah, bl)
    small = (by_low + by_hi[2 * n:]) + by_mid[n:]
    return (small + (by_mid[:n] + by_hi[n:2 * n])) + by_hi[:n]


def stacked(t):
    hi, mid, low = (v.astype(jnp.float32) for v in split3(t))
    return jnp.concatenate([
        jnp.concatenate([hi, mid], axis=1),
        jnp.concatenate([low, jnp.zeros_like(low)], axis=1)], axis=0).astype(jnp.bfloat16)


def transform(lhs, g):
    n = lhs.shape[0] // 2
    res = jnp.dot(lhs, jnp.concatenate([g, g], axis=0), preferred_element_type=jnp.float32)
    return (res[n:] + res[:n]).astype(jnp.bfloat16)


def exchange_kernel(dims, xt_hbm, wi_ref, wo_ref, op_ref, yo_hbm, wt_hbm, gath, tt_ref,
                    xn, xb, xs, xa, xl, ts, t2, sb1, sb2, rb, gsend, grecv, wi, wo, wf, wobs, obs_raw, obs_row, yp, cm, amat, cvec,
                    xsem, gssem, grsem, ssem, rsem, osem):
    members, rows, columns, channels, patches, dev_rows, ens_size, done = dims
    units = patches * ens_size
    total_m = members * ens_size
    me = lax.axis_index("ens")
    mydom = lax.axis_index("dom")
    my_x, my_core = me // 2, me % 2
    mine = pl.ds(pl.multiple_of(me * members, members), members)

    def dest_of(dslot):
        dx = (my_x + 1 - dslot // 2) % 2
        dc = (my_core + (dslot + 1) // 2) % 2
        return dx * 2 + dc

    def x_copy(m):
        return pltpu.make_async_copy(xt_hbm.at[m], xn.at[m % 2], xsem.at[m % 2])

    def ghost_copy(unit):
        return pltpu.make_async_remote_copy(
            src_ref=gsend.at[unit % 8], dst_ref=grecv.at[unit], send_sem=gssem.at[unit], recv_sem=grsem.at[unit],
            device_id={"dom": 1 - mydom}, device_id_type=MESH)

    def pair_copies(patch, dslot, pair):
        dev = {"ens": dest_of(dslot)}
        slot, box = (patch % 2) * 3 + dslot, patch * 3 + dslot
        two, tiles = pl.ds(pair * 2, 2), pl.ds(pair * 25, 25)
        first = pltpu.make_async_remote_copy(
            src_ref=sb1.at[slot, two], dst_ref=gath.at[patch, two, :, mine, pl.ds(0, 128)],
            send_sem=ssem.at[patch, dslot, pair * 2], recv_sem=rsem.at[patch, dslot, pair * 2],
            device_id=dev, device_id_type=MESH)
        second = pltpu.make_async_remote_copy(
            src_ref=sb2.at[slot, tiles], dst_ref=rb.at[box, tiles],
            send_sem=ssem.at[patch, dslot, pair * 2 + 1], recv_sem=rsem.at[patch, dslot, pair * 2 + 1],
            device_id=dev, device_id_type=MESH)
        return first, second

    def wait_sent(patch, dslot):
        for pair in range(2):
            for copy in pair_copies(patch, dslot, pair):
                copy.wait_send()

    obs_copies = [pltpu.make_async_copy(ref.at[pl.ds(me * patches, patches)], obs_raw.at[i], osem.at[i]) for i, ref in enumerate((yo_hbm, wt_hbm))]

    x_copy(0).start()
    x_copy(1).start()
    for copy in obs_copies:
        copy.start()
    barrier = pltpu.get_barrier_semaphore()
    for dslot in range(3):
        pl.semaphore_signal(barrier, inc=1, device_id={"ens": dest_of(dslot)}, device_id_type=MESH)
    pl.semaphore_signal(barrier, inc=1, device_id={"dom": 1 - mydom}, device_id_type=MESH)

    wf[...] = jnp.zeros_like(wf)
    wf[0:channels, :] = wo_ref[...].astype(jnp.float32)
    wo[...] = wf[0:CP, :].T.astype(jnp.bfloat16)
    wf[0:2 * channels, :] = wi_ref[...].astype(jnp.float32)
    keep = lax.broadcasted_iota(jnp.int32, (CP, 512), 0) < channels
    wi[0:CP, :] = jnp.where(keep, wf[0:CP, :], 0.0).astype(jnp.bfloat16)
    wi[CP:2 * CP, :] = wf[channels:channels + CP, :].astype(jnp.bfloat16)
    turn = (lax.broadcasted_iota(jnp.int32, (128, 128), 0) == lax.broadcasted_iota(jnp.int32, (128, 128), 1)).astype(jnp.float32).astype(jnp.bfloat16)

    wide = ([[xs.at[0, h, j] for j in range(4)] for h in range(2)],
            [[xs.at[j // 2, h, 4 + j % 2] for j in range(4)] for h in range(2)])
    turned = ([[xs.at[1, h, j] for j in range(4)] for h in range(2)],
              [[xa.at[h, j] for j in range(4)] for h in range(2)])

    def widen(odd, c):
        wide[odd][c // 128][c // 32 % 4][17 * (c % 32):17 * (c % 32) + 16, :] = xn[odd, c].astype(jnp.float32)

    def turn_column(odd, col):
        part = jnp.concatenate([wide[odd][h][j][pl.ds(col, 32, stride=17), :] for h in range(2) for j in range(4)], axis=0)
        out = lax.dot_general(turn, part.astype(jnp.bfloat16), NT, preferred_element_type=jnp.float32)
        for h in range(2):
            for j in range(4):
                turned[odd][h][j][pl.ds(col, 32, stride=17), :] = out[32 * j:32 * j + 32, h * 128:h * 128 + 128]

    def narrow(odd, m, row):
        for h in range(2):
            xb[m, row, :, h * 128:h * 128 + 128] = turned[odd][h][row // 32][17 * (row % 32):17 * (row % 32) + 16, :].astype(jnp.bfloat16)

    def relayout(t, carry):
        for odd in range(2):
            m = 2 * t + odd

            @pl.when(m + 2 < members)
            def _():
                x_copy(m + 2).start()

            @pl.when(m + 1 < members)
            def _():
                x_copy(m + 1).wait()
            for col in range(columns):
                turn_column(odd, col)
                for c in range(channels * col // columns, channels * (col + 1) // columns):
                    widen(1 - odd, c)
                for row in range(rows * col // columns, rows * (col + 1) // columns):
                    narrow(1 - odd, jnp.maximum(m - 1, 0), row)
        return carry
    for ref in (wide[0][1][3], wide[1][1][3]):
        ref[17 * (channels % 32):544, :] = jnp.zeros((544 - 17 * (channels % 32), 128), jnp.float32)
    x_copy(0).wait()
    for c in range(channels):
        widen(0, c)
    lax.fori_loop(0, members // 2, relayout, 0)

    for row in range(rows):
        narrow(1, members - 1, row)
    pl.semaphore_wait(barrier, 4)

    lane = lax.broadcasted_iota(jnp.int32, (members, 128), 1)

    def setup():
        wf[0:128, 0:CP] = jnp.zeros((128, CP), jnp.float32)
        wf[0:32, 0:channels] = op_ref[...].astype(jnp.float32)
        opt = wf[0:128, 0:CP].T.astype(jnp.bfloat16)
        for j in range(8):
            place = (lax.broadcasted_iota(jnp.int32, (128, CP), 1) == lax.broadcasted_iota(jnp.int32, (128, CP), 0) + 32 * j)
            wobs[j * CP:(j + 1) * CP, :] = jnp.dot(opt, place.astype(jnp.bfloat16), preferred_element_type=jnp.float32).astype(jnp.bfloat16)
        for copy in obs_copies:
            copy.wait()
        sub8 = lax.broadcasted_iota(jnp.int32, (8, 128), 0)
        lane8 = lax.broadcasted_iota(jnp.int32, (8, 128), 1) // 32
        wf[0:8, 0:128] = jnp.zeros((8, 128), jnp.float32)

        def rows_of(patch, carry):
            for i in range(2):
                for g in range(8):
                    wf[0:8, 0:32] = obs_raw[i, patch, g % 4, 0, (g // 4) * 8:(g // 4) * 8 + 8, :]
                    v = wf[0:8, 0:128]
                    v = v + pltpu.roll(v, 32, 1)
                    v = v + pltpu.roll(v, 64, 1)
                    for q in range(2):
                        obs_row[i, patch, g:g + 1, q * 128:q * 128 + 128] = jnp.sum(jnp.where(sub8 == lane8 + 4 * q, v, 0.0), axis=0, keepdims=True)
            return carry
        lax.fori_loop(0, patches, rows_of, 0)

    def prepare(unit):
        slot = unit % 2
        patch, dslot = unit // ens_size, unit % ens_size
        first = dest_of(dslot) * dev_rows + patch * 4

        def convert(r, carry):
            row = jnp.minimum(jnp.maximum(first + r - 1, 0), rows - 1)
            for m in range(members):
                for h in range(2):
                    xs[slot, h, r, 33 * m + 8:33 * m + 24, :] = xb[m, row, :, h * 128:h * 128 + 128].astype(jnp.float32)
            return carry
        lax.fori_loop(0, 6, convert, 0)

        @pl.when(unit >= 8)
        def _():
            ghost_copy(unit - 8).wait_send()

        def edges(r, carry):
            for h in range(2):
                gsend[unit % 8, 0, r, :, h * 128:h * 128 + 128] = xs[slot, h, r + 1, pl.ds(23, members, stride=33), :].astype(jnp.bfloat16)
                gsend[unit % 8, 1, r, :, h * 128:h * 128 + 128] = xs[slot, h, r + 1, pl.ds(8, members, stride=33), :].astype(jnp.bfloat16)
            return carry
        lax.fori_loop(0, 4, edges, 0)
        ghost_copy(unit).start()

    def forecast(unit):
        patch, dslot = unit // ens_size, unit % ens_size
        slot = unit % 2
        out_slot = jnp.where(dslot < 3, (patch % 2) * 3 + dslot, 6)

        @pl.when((dslot < 3) & (patch >= 2))
        def _():
            wait_sent(patch - 2, dslot)
        ghost_copy(unit).wait_recv()

        def block(r, carry):
            for h in range(2):
                xs[slot, h, r + 1, pl.ds(7, members, stride=33), :] = grecv[unit, 0, r, :, h * 128:h * 128 + 128].astype(jnp.float32)
                xs[slot, h, r + 1, pl.ds(24, members, stride=33), :] = grecv[unit, 1, r, :, h * 128:h * 128 + 128].astype(jnp.float32)
            for m in range(members):
                b = 33 * m
                for h in range(2):
                    cur = xs[slot, h, r + 1, b + 8:b + 24, :]
                    north = xs[slot, h, r, b + 8:b + 24, :]
                    south = xs[slot, h, r + 2, b + 8:b + 24, :]
                    west = xs[slot, h, r + 1, b + 7:b + 23, :]
                    east = xs[slot, h, r + 1, b + 9:b + 25, :]
                    lap = north + south + west + east - 4.0 * cur
                    xl[16 * m:16 * m + 16, h * 128:h * 128 + 128] = cur.astype(jnp.bfloat16)
                    xl[16 * m:16 * m + 16, CP + h * 128:CP + h * 128 + 128] = lap.astype(jnp.bfloat16)
            hidden = jnp.dot(xl[...], wi[...], preferred_element_type=jnp.float32)
            gel = gelu(hidden).astype(jnp.bfloat16)
            inc = jnp.dot(gel, wo[...], preferred_element_type=jnp.float32)
            for m in range(members):
                for h in range(2):
                    ts[h, 17 * m:17 * m + 16, :] = xs[slot, h, r + 1, 33 * m + 8:33 * m + 24, :] + inc[16 * m:16 * m + 16, h * 128:h * 128 + 128]
            for col in range(columns):
                sb1[out_slot, r, col] = ts[0, pl.ds(col, members, stride=17), :].astype(jnp.bfloat16)
                t2[r, col] = ts[1, pl.ds(col, members, stride=17), :]
            return carry

        def pack(pair):
            left = jnp.zeros((members, 128), jnp.float32)
            for k in range(8):
                r, c0 = pair * 2 + k // 4, (k % 4) * 4
                v = [t2[r, c0 + i] for i in range(4)]
                for i in range(3):
                    sb2[out_slot, pair * 25 + k * 3 + i] = jnp.where(lane < 96, v[i], pltpu.roll(v[3], 96 - 32 * i, 1)).astype(jnp.bfloat16)
                for i in range(4):
                    left = left + pltpu.roll(jnp.where(lane >= 96, v[i], 0.0), (32 + 3 * (4 * k + i)) % 128, 1)
            sb2[out_slot, pair * 25 + 24] = left.astype(jnp.bfloat16)

        def half_unit(pair, carry):
            lax.fori_loop(pair * 2, pair * 2 + 2, block, 0)

            @pl.when(dslot < 3)
            def _():
                pack(pair)
                for copy in pair_copies(patch, dslot, pair):
                    copy.start()

            @pl.when(dslot == 3)
            def _():
                def own(r, c2):
                    for col in range(columns):
                        gath[patch, r, col, mine, 0:128] = sb1[6, r, col]
                        gath[patch, r, col, mine, 128:256] = t2[r, col].astype(jnp.bfloat16)
                    return c2
                lax.fori_loop(pair * 2, pair * 2 + 2, own, 0)
            return carry
        lax.fori_loop(0, 2, half_unit, 0)

    def unpack(patch, dslot):
        src = pl.ds(pl.multiple_of(dest_of(dslot) * members, members), members)
        box = patch * 3 + dslot

        def half(pair, carry):
            for copy in pair_copies(patch, dslot, pair):
                copy.wait_recv()
            left = rb[box, pair * 25 + 24].astype(jnp.float32)
            for k in range(8):
                r, c0 = pair * 2 + k // 4, (k % 4) * 4
                p = [rb[box, pair * 25 + k * 3 + i].astype(jnp.float32) for i in range(3)]
                tail = [jnp.where(lane < 99, pltpu.roll(left, (96 - 3 * (4 * k + i)) % 128, 1), 0.0) for i in range(4)]
                for i in range(3):
                    gath[patch, r, c0 + i, src, 128:256] = jnp.where(lane < 96, p[i], tail[i]).astype(jnp.bfloat16)
                last = jnp.where(lane < 64, jnp.where(lane < 32, pltpu.roll(p[0], 32, 1), pltpu.roll(p[1], 64, 1)),
                                 jnp.where(lane < 96, pltpu.roll(p[2], 96, 1), tail[3]))
                gath[patch, r, c0 + 3, src, 128:256] = last.astype(jnp.bfloat16)
            return carry
        lax.fori_loop(0, 2, half, 0)

    def analysis(patch):
        def arrive(dslot, carry):
            unpack(patch, dslot)
            return carry
        lax.fori_loop(0, 3, lambda i, c: arrive(2 - i, c), 0)
        eye = (lax.broadcasted_iota(jnp.int32, (total_m, total_m), 0) == lax.broadcasted_iota(jnp.int32, (total_m, total_m), 1)).astype(jnp.float32)
        csum = jnp.zeros((total_m, CP), jnp.float32)
        for half in range(2):
            lhs = jnp.concatenate([gath[patch, :, half * 8 + j].reshape(4 * total_m, CP) for j in range(8)], axis=1)
            yb = jnp.dot(lhs, wobs[...], preferred_element_type=jnp.float32)
            for r in range(4):
                g = half * 4 + r
                y = yb[r * total_m:(r + 1) * total_m]
                ybar = jnp.sum(y, axis=0, keepdims=True) * (1.0 / total_m)
                y = y - ybar
                c = y * obs_row[1, patch, g:g + 1, :]
                csum = csum + c * (obs_row[0, patch, g:g + 1, :] - ybar)
                yp[g] = y
                cm[g] = c
        a_mat = (total_m - 1.0) * eye
        for g in range(8):
            a_mat = a_mat + f32dot(cm[g], yp[g], NT)
        amat[patch % 2, :, 0:total_m] = a_mat
        amat[patch % 2, :, total_m:2 * total_m] = a_mat
        cvec[patch % 2] = jnp.broadcast_to(jnp.sum(csum, axis=1, keepdims=True), (total_m, 2 * total_m))

    def solve(patch):
        row = lax.broadcasted_iota(jnp.int32, (total_m, 2 * total_m), 0)
        col = lax.broadcasted_iota(jnp.int32, (total_m, 2 * total_m), 1)
        eye = ((row == col) | (row + total_m == col)).astype(jnp.float32)
        first = col < total_m
        left = first.astype(jnp.float32).astype(jnp.bfloat16)
        right = (col >= total_m).astype(jnp.float32).astype(jnp.bfloat16)
        mats = jnp.where(first, amat[0], amat[1])
        diag = jnp.sum(mats * eye, axis=0, keepdims=True)
        trace = jnp.where(first[0:1], jnp.sum(jnp.where(first[0:1], diag, 0.0), axis=1, keepdims=True),
                          jnp.sum(jnp.where(first[0:1], 0.0, diag), axis=1, keepdims=True))

        def mixer(z, y):
            return 1.5 * eye - 0.5 * packed_dot(z, y, left, right)

        def newton(step, carry):
            y, z = carry
            mix = mixer(z, y)
            return packed_dot(y, mix, left, right), packed_dot(mix, z, left, right)
        scaled = mats / trace
        mix = 1.5 * eye - 0.5 * scaled
        y, z = lax.fori_loop(1, NS_STEPS - 1, newton, (packed_dot(scaled, mix, left, right), mix))
        inv = packed_dot(mixer(z, y), z, left, right)
        root = inv / jnp.sqrt(trace)
        wbar = packed_dot(root, packed_dot(root, jnp.where(first, cvec[0], cvec[1]), left, right), left, right)
        trans = math.sqrt(total_m - 1.0) * root + wbar
        trans = trans + (1.0 - jnp.sum(trans, axis=0, keepdims=True)) * (1.0 / total_m)
        both = trans.T
        tt_ref[patch] = both[0:total_m]
        tt_ref[patch + 1] = both[total_m:2 * total_m]

        @pl.when(patch < done)
        def _():
            def apply(i, carry):
                lhs = stacked(tt_ref[patch + i // 4])
                for c in range(columns):
                    gath[patch + i // 4, i % 4, c] = transform(lhs, gath[patch + i // 4, i % 4, c])
                return carry
            lax.fori_loop(0, 8, apply, 0)

    def step(v, carry):
        @pl.when(v < units)
        def _():
            prepare(v)

        @pl.when((v >= 1) & (v <= units))
        def _():
            forecast(v - 1)

        @pl.when(v == 0)
        def _():
            setup()

        @pl.when(v == units + 1)
        def _():
            for unit in range(units - 8, units):
                ghost_copy(unit).wait_send()

        @pl.when((v >= 12) & (v % 4 == 0))
        def _():
            analysis(v // 4 - 3)

        @pl.when((v >= 12) & (v % 8 == 0))
        def _():
            solve(v // 4 - 4)
        return carry
    lax.fori_loop(0, units + 9, step, 0)

    for patch in range(patches - 2, patches):
        for dslot in range(3):
            wait_sent(patch, dslot)


def update_kernel(done, tt_ref, g_ref, out_hbm, stage, sem):
    channels = out_hbm.shape[3]

    def copy(r):
        return pltpu.make_async_copy(stage.at[r], out_hbm.at[r], sem.at[r])

    def write(r, carry):
        for col in range(stage.shape[1]):
            stage[r, col] = g_ref[r // 4, r % 4, col, :, 0:channels]
        copy(r).start()
        return carry
    lax.fori_loop(0, 4 * done, write, 0)

    def last(r, carry):
        lhs = stacked(tt_ref[r // 4])
        for col in range(stage.shape[1]):
            stage[r, col] = transform(lhs, g_ref[r // 4, r % 4, col])[:, 0:channels]
        copy(r).start()
        return carry
    lax.fori_loop(4 * done, stage.shape[0], last, 0)

    def drain(r, carry):
        copy(r).wait()
        return carry
    lax.fori_loop(0, stage.shape[0], drain, 0)


def solution(mesh):
    ens_size = mesh.shape["ens"]
    obs_spec = P(None, None, "dom", None, None)

    def local_step(ens_state, w_in, w_out, obs_op, obs_val, obs_wt):
        members, rows, columns, channels = ens_state.shape
        total_m = members * ens_size
        dev_rows = rows // ens_size
        patches = dev_rows // 4
        units = patches * ens_size
        done = patches - 2
        dims = (members, rows, columns, channels, patches, dev_rows, ens_size, done)
        vmem = pl.BlockSpec(memory_space=pltpu.VMEM)
        anym = pl.BlockSpec(memory_space=pl.ANY)
        bf, f32 = jnp.bfloat16, jnp.float32
        dma = pltpu.SemaphoreType.DMA
        gathered, trans = pl.pallas_call(
            functools.partial(exchange_kernel, dims),
            out_shape=(pltpu.VMEM((patches, 4, columns, total_m, CP), bf),
                       pltpu.VMEM((patches, total_m, total_m), f32)),
            in_specs=[anym, vmem, vmem, vmem, anym, anym],
            out_specs=(vmem, vmem),
            scratch_shapes=[
                pltpu.VMEM((2, channels, columns, rows), bf),
                pltpu.VMEM((members, rows, columns, CP), bf),
                pltpu.VMEM((2, 2, 6, 544, 128), f32),
                pltpu.VMEM((2, 4, 544, 128), f32),
                pltpu.VMEM((members * columns, 2 * CP), bf),
                pltpu.VMEM((2, members * 17, 128), f32),
                pltpu.VMEM((4, columns, members, 128), f32),
                pltpu.VMEM((7, 4, columns, members, 128), bf),
                pltpu.VMEM((6, 50, members, 128), bf),
                pltpu.VMEM((patches * 3, 50, members, 128), bf),
                pltpu.VMEM((8, 2, 4, members, CP), bf),
                pltpu.VMEM((units, 2, 4, members, CP), bf),
                pltpu.VMEM((2 * CP, 512), bf),
                pltpu.VMEM((512, CP), bf),
                pltpu.VMEM((488, 512), f32),
                pltpu.VMEM((8 * CP, CP), bf),
                pltpu.VMEM((2, patches, 4, 1, columns, 32), f32),
                pltpu.VMEM((2, patches, 8, CP), f32),
                pltpu.VMEM((8, total_m, CP), f32),
                pltpu.VMEM((8, total_m, CP), f32),
                pltpu.VMEM((2, total_m, 2 * total_m), f32),
                pltpu.VMEM((2, total_m, 2 * total_m), f32),
                dma((2,)), dma((units,)), dma((units,)), dma((patches, 3, 4)), dma((patches, 3, 4)), dma((2,)),
            ],
            compiler_params=pltpu.CompilerParams(collective_id=0, has_side_effects=True, vmem_limit_bytes=46 * 1024 * 1024),
        )(ens_state.transpose(0, 3, 2, 1), w_in, w_out.T, obs_op.T, obs_val, obs_wt)
        return pl.pallas_call(
            functools.partial(update_kernel, done),
            out_shape=jax.ShapeDtypeStruct((dev_rows, columns, total_m, channels), bf),
            in_specs=[vmem, vmem],
            out_specs=anym,
            scratch_shapes=[pltpu.VMEM((dev_rows, columns, total_m, channels), bf), dma((dev_rows,))],
            compiler_params=pltpu.CompilerParams(vmem_limit_bytes=24 * 1024 * 1024),
        )(pltpu.with_memory_space_constraint(trans, pltpu.VMEM), pltpu.with_memory_space_constraint(gathered, pltpu.VMEM))

    return jax.shard_map(local_step, mesh=mesh, in_specs=(P("ens", None, "dom", None), P(), P(), P(), obs_spec, obs_spec), out_specs=P("ens", "dom", None, None), check_vma=False)
```

```python
import functools
import math
import jax
import jax.numpy as jnp
from jax import lax
from jax.experimental import pallas as pl
from jax.experimental.pallas import tpu as pltpu
from jax.sharding import PartitionSpec as P

NS_STEPS = 18
MESH = pl.DeviceIdType.MESH
CP = 256
NT = (((1,), (1,)), ((), ()))


NN = (((1,), (0,)), ((), ()))


def gelu(x):
    scale = math.sqrt(2.0 / math.pi)
    return (0.5 * x) * (1.0 + jnp.tanh(x * (scale + (scale * 0.044715) * (x * x))))


def split3(a):
    hi = a.astype(jnp.bfloat16)
    rem = a - hi.astype(jnp.float32)
    mid = rem.astype(jnp.bfloat16)
    low = (rem - mid.astype(jnp.float32)).astype(jnp.bfloat16)
    return hi, mid, low


def f32dot(a, b, dims=NN):
    ah, am, al = split3(a)
    bh, bm, bl = split3(b)
    n = a.shape[0]

    def dot(u, v):
        return lax.dot_general(u, v, dims, preferred_element_type=jnp.float32)
    by_hi = dot(jnp.concatenate([ah, am, al], axis=0), bh)
    by_mid = dot(jnp.concatenate([ah, am], axis=0), bm)
    by_low = dot(ah, bl)
    small = (by_low + by_hi[2 * n:]) + by_mid[n:]
    return (small + (by_mid[:n] + by_hi[n:2 * n])) + by_hi[:n]


def packed_dot(a, b, left, right):
    ah, am, al = split3(a)
    bh, bm, bl = split3(b)
    n = a.shape[0]

    def dot(u, v):
        blocks = jnp.concatenate([v * left, v * right], axis=0)
        return jnp.dot(u, blocks, preferred_element_type=jnp.float32)
    by_hi = dot(jnp.concatenate([ah, am, al], axis=0), bh)
    by_mid = dot(jnp.concatenate([ah, am], axis=0), bm)
    by_low = dot(ah, bl)
    small = (by_low + by_hi[2 * n:]) + by_mid[n:]
    return (small + (by_mid[:n] + by_hi[n:2 * n])) + by_hi[:n]


def stacked(t):
    hi, mid, low = (v.astype(jnp.float32) for v in split3(t))
    return jnp.concatenate([
        jnp.concatenate([hi, mid], axis=1),
        jnp.concatenate([low, jnp.zeros_like(low)], axis=1)], axis=0).astype(jnp.bfloat16)


def transform(lhs, g):
    n = lhs.shape[0] // 2
    res = jnp.dot(lhs, jnp.concatenate([g, g], axis=0), preferred_element_type=jnp.float32)
    return (res[n:] + res[:n]).astype(jnp.bfloat16)


def exchange_kernel(dims, xt_hbm, wi_ref, wo_ref, op_ref, yo_hbm, wt_hbm, gath, tt_ref,
                    xn, xb, xs, xa, xl, ts, t2, sb1, sb2, rb, gsend, grecv, wi, wo, wf, wobs, obs_raw, obs_row, yp, cm, amat, cvec,
                    xsem, gssem, grsem, ssem, rsem, osem):
    members, rows, columns, channels, patches, dev_rows, ens_size, done = dims
    units = patches * ens_size
    total_m = members * ens_size
    me = lax.axis_index("ens")
    mydom = lax.axis_index("dom")
    my_x, my_core = me // 2, me % 2
    mine = pl.ds(pl.multiple_of(me * members, members), members)

    def dest_of(dslot):
        dx = (my_x + 1 - dslot // 2) % 2
        dc = (my_core + (dslot + 1) // 2) % 2
        return dx * 2 + dc

    def x_copy(m):
        return pltpu.make_async_copy(xt_hbm.at[m], xn.at[m % 2], xsem.at[m % 2])

    def ghost_copy(unit, pair):
        two = pl.ds(pair * 2, 2)
        return pltpu.make_async_remote_copy(
            src_ref=gsend.at[unit % 8, :, two], dst_ref=grecv.at[unit, :, two],
            send_sem=gssem.at[unit, pair], recv_sem=grsem.at[unit, pair],
            device_id={"dom": 1 - mydom}, device_id_type=MESH)

    def pair_copies(patch, dslot, pair):
        dev = {"ens": dest_of(dslot)}
        slot, box = (patch % 2) * 3 + dslot, patch * 3 + dslot
        two, tiles = pl.ds(pair * 2, 2), pl.ds(pair * 25, 25)
        first = pltpu.make_async_remote_copy(
            src_ref=sb1.at[slot, two], dst_ref=gath.at[patch, two, :, mine, pl.ds(0, 128)],
            send_sem=ssem.at[patch, dslot, pair * 2], recv_sem=rsem.at[patch, dslot, pair * 2],
            device_id=dev, device_id_type=MESH)
        second = pltpu.make_async_remote_copy(
            src_ref=sb2.at[slot, tiles], dst_ref=rb.at[box, tiles],
            send_sem=ssem.at[patch, dslot, pair * 2 + 1], recv_sem=rsem.at[patch, dslot, pair * 2 + 1],
            device_id=dev, device_id_type=MESH)
        return first, second

    def wait_sent(patch, dslot):
        for pair in range(2):
            for copy in pair_copies(patch, dslot, pair):
                copy.wait_send()

    obs_copies = [pltpu.make_async_copy(ref.at[pl.ds(me * patches, patches)], obs_raw.at[i], osem.at[i]) for i, ref in enumerate((yo_hbm, wt_hbm))]

    x_copy(0).start()
    x_copy(1).start()
    for copy in obs_copies:
        copy.start()
    barrier = pltpu.get_barrier_semaphore()
    for dslot in range(3):
        pl.semaphore_signal(barrier, inc=1, device_id={"ens": dest_of(dslot)}, device_id_type=MESH)
    pl.semaphore_signal(barrier, inc=1, device_id={"dom": 1 - mydom}, device_id_type=MESH)

    wf[...] = jnp.zeros_like(wf)
    wf[0:channels, :] = wo_ref[...].astype(jnp.float32)
    wo[...] = wf[0:CP, :].T.astype(jnp.bfloat16)
    wf[0:2 * channels, :] = wi_ref[...].astype(jnp.float32)
    keep = lax.broadcasted_iota(jnp.int32, (CP, 512), 0) < channels
    wi[0:CP, :] = jnp.where(keep, wf[0:CP, :], 0.0).astype(jnp.bfloat16)
    wi[CP:2 * CP, :] = wf[channels:channels + CP, :].astype(jnp.bfloat16)
    turn = (lax.broadcasted_iota(jnp.int32, (128, 128), 0) == lax.broadcasted_iota(jnp.int32, (128, 128), 1)).astype(jnp.float32).astype(jnp.bfloat16)

    wide = ([[xs.at[0, h, j] for j in range(4)] for h in range(2)],
            [[xs.at[j // 2, h, 4 + j % 2] for j in range(4)] for h in range(2)])
    turned = ([[xs.at[1, h, j] for j in range(4)] for h in range(2)],
              [[xa.at[h, j] for j in range(4)] for h in range(2)])

    def widen(odd, c):
        wide[odd][c // 128][c // 32 % 4][17 * (c % 32):17 * (c % 32) + 16, :] = xn[odd, c].astype(jnp.float32)

    def turn_column(odd, col):
        part = jnp.concatenate([wide[odd][h][j][pl.ds(col, 32, stride=17), :] for h in range(2) for j in range(4)], axis=0)
        out = lax.dot_general(turn, part.astype(jnp.bfloat16), NT, preferred_element_type=jnp.float32)
        for h in range(2):
            for j in range(4):
                turned[odd][h][j][pl.ds(col, 32, stride=17), :] = out[32 * j:32 * j + 32, h * 128:h * 128 + 128]

    def narrow(odd, m, row):
        for h in range(2):
            xb[m, row, :, h * 128:h * 128 + 128] = turned[odd][h][row // 32][17 * (row % 32):17 * (row % 32) + 16, :].astype(jnp.bfloat16)

    def relayout(t, carry):
        for odd in range(2):
            m = 2 * t + odd

            @pl.when(m + 2 < members)
            def _():
                x_copy(m + 2).start()

            @pl.when(m + 1 < members)
            def _():
                x_copy(m + 1).wait()
            for col in range(columns):
                turn_column(odd, col)
                for c in range(channels * col // columns, channels * (col + 1) // columns):
                    widen(1 - odd, c)
                for row in range(rows * col // columns, rows * (col + 1) // columns):
                    narrow(1 - odd, jnp.maximum(m - 1, 0), row)
        return carry
    for ref in (wide[0][1][3], wide[1][1][3]):
        ref[17 * (channels % 32):544, :] = jnp.zeros((544 - 17 * (channels % 32), 128), jnp.float32)
    x_copy(0).wait()
    for c in range(channels):
        widen(0, c)
    lax.fori_loop(0, members // 2, relayout, 0)

    for row in range(rows):
        narrow(1, members - 1, row)
    pl.semaphore_wait(barrier, 4)

    lane = lax.broadcasted_iota(jnp.int32, (members, 128), 1)

    def setup():
        wf[0:128, 0:CP] = jnp.zeros((128, CP), jnp.float32)
        wf[0:32, 0:channels] = op_ref[...].astype(jnp.float32)
        opt = wf[0:128, 0:CP].T.astype(jnp.bfloat16)
        for j in range(8):
            place = (lax.broadcasted_iota(jnp.int32, (128, CP), 1) == lax.broadcasted_iota(jnp.int32, (128, CP), 0) + 32 * j)
            wobs[j * CP:(j + 1) * CP, :] = jnp.dot(opt, place.astype(jnp.bfloat16), preferred_element_type=jnp.float32).astype(jnp.bfloat16)
        for copy in obs_copies:
            copy.wait()
        sub8 = lax.broadcasted_iota(jnp.int32, (8, 128), 0)
        lane8 = lax.broadcasted_iota(jnp.int32, (8, 128), 1) // 32
        wf[0:8, 0:128] = jnp.zeros((8, 128), jnp.float32)

        def rows_of(patch, carry):
            for i in range(2):
                for g in range(8):
                    wf[0:8, 0:32] = obs_raw[i, patch, g % 4, 0, (g // 4) * 8:(g // 4) * 8 + 8, :]
                    v = wf[0:8, 0:128]
                    v = v + pltpu.roll(v, 32, 1)
                    v = v + pltpu.roll(v, 64, 1)
                    for q in range(2):
                        obs_row[i, patch, g:g + 1, q * 128:q * 128 + 128] = jnp.sum(jnp.where(sub8 == lane8 + 4 * q, v, 0.0), axis=0, keepdims=True)
            return carry
        lax.fori_loop(0, patches, rows_of, 0)

    def prepare(unit):
        slot = unit % 2
        patch, dslot = unit // ens_size, unit % ens_size
        first = dest_of(dslot) * dev_rows + patch * 4

        def convert(r, carry):
            row = jnp.minimum(jnp.maximum(first + r - 1, 0), rows - 1)
            for m in range(members):
                for h in range(2):
                    xs[slot, h, r, 33 * m + 8:33 * m + 24, :] = xb[m, row, :, h * 128:h * 128 + 128].astype(jnp.float32)
            return carry
        lax.fori_loop(0, 6, convert, 0)

        @pl.when(unit >= 8)
        def _():
            for pair in range(2):
                ghost_copy(unit - 8, pair).wait_send()

        def edges(r, carry):
            for h in range(2):
                gsend[unit % 8, 0, r, :, h * 128:h * 128 + 128] = xs[slot, h, r + 1, pl.ds(23, members, stride=33), :].astype(jnp.bfloat16)
                gsend[unit % 8, 1, r, :, h * 128:h * 128 + 128] = xs[slot, h, r + 1, pl.ds(8, members, stride=33), :].astype(jnp.bfloat16)
            return carry
        for pair in range(2):
            lax.fori_loop(pair * 2, pair * 2 + 2, edges, 0)
            ghost_copy(unit, pair).start()

    def forecast(unit):
        patch, dslot = unit // ens_size, unit % ens_size
        slot = unit % 2
        out_slot = jnp.where(dslot < 3, (patch % 2) * 3 + dslot, 6)

        @pl.when((dslot < 3) & (patch >= 2))
        def _():
            wait_sent(patch - 2, dslot)

        def block(r, carry):
            for h in range(2):
                xs[slot, h, r + 1, pl.ds(7, members, stride=33), :] = grecv[unit, 0, r, :, h * 128:h * 128 + 128].astype(jnp.float32)
                xs[slot, h, r + 1, pl.ds(24, members, stride=33), :] = grecv[unit, 1, r, :, h * 128:h * 128 + 128].astype(jnp.float32)
            for m in range(members):
                b = 33 * m
                for h in range(2):
                    cur = xs[slot, h, r + 1, b + 8:b + 24, :]
                    north = xs[slot, h, r, b + 8:b + 24, :]
                    south = xs[slot, h, r + 2, b + 8:b + 24, :]
                    west = xs[slot, h, r + 1, b + 7:b + 23, :]
                    east = xs[slot, h, r + 1, b + 9:b + 25, :]
                    lap = north + south + west + east - 4.0 * cur
                    xl[16 * m:16 * m + 16, h * 128:h * 128 + 128] = cur.astype(jnp.bfloat16)
                    xl[16 * m:16 * m + 16, CP + h * 128:CP + h * 128 + 128] = lap.astype(jnp.bfloat16)
            hidden = jnp.dot(xl[...], wi[...], preferred_element_type=jnp.float32)
            gel = gelu(hidden).astype(jnp.bfloat16)
            inc = jnp.dot(gel, wo[...], preferred_element_type=jnp.float32)
            for m in range(members):
                for h in range(2):
                    ts[h, 17 * m:17 * m + 16, :] = xs[slot, h, r + 1, 33 * m + 8:33 * m + 24, :] + inc[16 * m:16 * m + 16, h * 128:h * 128 + 128]
            for col in range(columns):
                sb1[out_slot, r, col] = ts[0, pl.ds(col, members, stride=17), :].astype(jnp.bfloat16)
                t2[r, col] = ts[1, pl.ds(col, members, stride=17), :]
            return carry

        def pack(pair):
            left = jnp.zeros((members, 128), jnp.float32)
            for k in range(8):
                r, c0 = pair * 2 + k // 4, (k % 4) * 4
                v = [t2[r, c0 + i] for i in range(4)]
                for i in range(3):
                    sb2[out_slot, pair * 25 + k * 3 + i] = jnp.where(lane < 96, v[i], pltpu.roll(v[3], 96 - 32 * i, 1)).astype(jnp.bfloat16)
                for i in range(4):
                    left = left + pltpu.roll(jnp.where(lane >= 96, v[i], 0.0), (32 + 3 * (4 * k + i)) % 128, 1)
            sb2[out_slot, pair * 25 + 24] = left.astype(jnp.bfloat16)

        def half_unit(pair, carry):
            ghost_copy(unit, pair).wait_recv()
            lax.fori_loop(pair * 2, pair * 2 + 2, block, 0)

            @pl.when(dslot < 3)
            def _():
                pack(pair)
                for copy in pair_copies(patch, dslot, pair):
                    copy.start()

            @pl.when(dslot == 3)
            def _():
                def own(r, c2):
                    for col in range(columns):
                        gath[patch, r, col, mine, 0:128] = sb1[6, r, col]
                        gath[patch, r, col, mine, 128:256] = t2[r, col].astype(jnp.bfloat16)
                    return c2
                lax.fori_loop(pair * 2, pair * 2 + 2, own, 0)
            return carry
        lax.fori_loop(0, 2, half_unit, 0)

    def unpack(patch, dslot):
        src = pl.ds(pl.multiple_of(dest_of(dslot) * members, members), members)
        box = patch * 3 + dslot

        def half(pair, carry):
            for copy in pair_copies(patch, dslot, pair):
                copy.wait_recv()
            left = rb[box, pair * 25 + 24].astype(jnp.float32)
            for k in range(8):
                r, c0 = pair * 2 + k // 4, (k % 4) * 4
                p = [rb[box, pair * 25 + k * 3 + i].astype(jnp.float32) for i in range(3)]
                tail = [jnp.where(lane < 99, pltpu.roll(left, (96 - 3 * (4 * k + i)) % 128, 1), 0.0) for i in range(4)]
                for i in range(3):
                    gath[patch, r, c0 + i, src, 128:256] = jnp.where(lane < 96, p[i], tail[i]).astype(jnp.bfloat16)
                last = jnp.where(lane < 64, jnp.where(lane < 32, pltpu.roll(p[0], 32, 1), pltpu.roll(p[1], 64, 1)),
                                 jnp.where(lane < 96, pltpu.roll(p[2], 96, 1), tail[3]))
                gath[patch, r, c0 + 3, src, 128:256] = last.astype(jnp.bfloat16)
            return carry
        lax.fori_loop(0, 2, half, 0)

    def analysis(patch):
        def arrive(dslot, carry):
            unpack(patch, dslot)
            return carry
        lax.fori_loop(0, 3, lambda i, c: arrive(2 - i, c), 0)
        eye = (lax.broadcasted_iota(jnp.int32, (total_m, total_m), 0) == lax.broadcasted_iota(jnp.int32, (total_m, total_m), 1)).astype(jnp.float32)
        csum = jnp.zeros((total_m, CP), jnp.float32)
        for half in range(2):
            lhs = jnp.concatenate([gath[patch, :, half * 8 + j].reshape(4 * total_m, CP) for j in range(8)], axis=1)
            yb = jnp.dot(lhs, wobs[...], preferred_element_type=jnp.float32)
            for r in range(4):
                g = half * 4 + r
                y = yb[r * total_m:(r + 1) * total_m]
                ybar = jnp.sum(y, axis=0, keepdims=True) * (1.0 / total_m)
                y = y - ybar
                c = y * obs_row[1, patch, g:g + 1, :]
                csum = csum + c * (obs_row[0, patch, g:g + 1, :] - ybar)
                yp[g] = y
                cm[g] = c
        a_mat = (total_m - 1.0) * eye
        for g in range(8):
            a_mat = a_mat + f32dot(cm[g], yp[g], NT)
        amat[patch % 2, :, 0:total_m] = a_mat
        amat[patch % 2, :, total_m:2 * total_m] = a_mat
        cvec[patch % 2] = jnp.broadcast_to(jnp.sum(csum, axis=1, keepdims=True), (total_m, 2 * total_m))

    def solve(patch):
        row = lax.broadcasted_iota(jnp.int32, (total_m, 2 * total_m), 0)
        col = lax.broadcasted_iota(jnp.int32, (total_m, 2 * total_m), 1)
        eye = ((row == col) | (row + total_m == col)).astype(jnp.float32)
        first = col < total_m
        left = first.astype(jnp.float32).astype(jnp.bfloat16)
        right = (col >= total_m).astype(jnp.float32).astype(jnp.bfloat16)
        mats = jnp.where(first, amat[0], amat[1])
        diag = jnp.sum(mats * eye, axis=0, keepdims=True)
        trace = jnp.where(first[0:1], jnp.sum(jnp.where(first[0:1], diag, 0.0), axis=1, keepdims=True),
                          jnp.sum(jnp.where(first[0:1], 0.0, diag), axis=1, keepdims=True))

        def mixer(z, y):
            return 1.5 * eye - 0.5 * packed_dot(z, y, left, right)

        def newton(step, carry):
            y, z = carry
            mix = mixer(z, y)
            return packed_dot(y, mix, left, right), packed_dot(mix, z, left, right)
        scaled = mats / trace
        mix = 1.5 * eye - 0.5 * scaled
        y, z = lax.fori_loop(1, NS_STEPS - 1, newton, (packed_dot(scaled, mix, left, right), mix))
        inv = packed_dot(mixer(z, y), z, left, right)
        root = inv / jnp.sqrt(trace)
        wbar = packed_dot(root, packed_dot(root, jnp.where(first, cvec[0], cvec[1]), left, right), left, right)
        trans = math.sqrt(total_m - 1.0) * root + wbar
        trans = trans + (1.0 - jnp.sum(trans, axis=0, keepdims=True)) * (1.0 / total_m)
        both = trans.T
        tt_ref[patch] = both[0:total_m]
        tt_ref[patch + 1] = both[total_m:2 * total_m]

        @pl.when(patch < done)
        def _():
            def apply(i, carry):
                lhs = stacked(tt_ref[patch + i // 4])
                for c in range(columns):
                    gath[patch + i // 4, i % 4, c] = transform(lhs, gath[patch + i // 4, i % 4, c])
                return carry
            lax.fori_loop(0, 8, apply, 0)

    def step(v, carry):
        @pl.when(v < units)
        def _():
            prepare(v)

        @pl.when((v >= 1) & (v <= units))
        def _():
            forecast(v - 1)

        @pl.when(v == 0)
        def _():
            setup()

        @pl.when(v == units + 1)
        def _():
            for unit in range(units - 8, units):
                for pair in range(2):
                    ghost_copy(unit, pair).wait_send()

        @pl.when((v >= 12) & (v % 4 == 0))
        def _():
            analysis(v // 4 - 3)

        @pl.when((v >= 12) & (v % 8 == 0))
        def _():
            solve(v // 4 - 4)
        return carry
    lax.fori_loop(0, units + 9, step, 0)

    for patch in range(patches - 2, patches):
        for dslot in range(3):
            wait_sent(patch, dslot)


def update_kernel(done, tt_ref, g_ref, out_hbm, stage, sem):
    channels = out_hbm.shape[3]

    def copy(r):
        return pltpu.make_async_copy(stage.at[r], out_hbm.at[r], sem.at[r])

    def write(r, carry):
        for col in range(stage.shape[1]):
            stage[r, col] = g_ref[r // 4, r % 4, col, :, 0:channels]
        copy(r).start()
        return carry
    lax.fori_loop(0, 4 * done, write, 0)

    def last(r, carry):
        lhs = stacked(tt_ref[r // 4])
        for col in range(stage.shape[1]):
            stage[r, col] = transform(lhs, g_ref[r // 4, r % 4, col])[:, 0:channels]
        copy(r).start()
        return carry
    lax.fori_loop(4 * done, stage.shape[0], last, 0)

    def drain(r, carry):
        copy(r).wait()
        return carry
    lax.fori_loop(0, stage.shape[0], drain, 0)


def solution(mesh):
    ens_size = mesh.shape["ens"]
    obs_spec = P(None, None, "dom", None, None)

    def local_step(ens_state, w_in, w_out, obs_op, obs_val, obs_wt):
        members, rows, columns, channels = ens_state.shape
        total_m = members * ens_size
        dev_rows = rows // ens_size
        patches = dev_rows // 4
        units = patches * ens_size
        done = patches - 2
        dims = (members, rows, columns, channels, patches, dev_rows, ens_size, done)
        vmem = pl.BlockSpec(memory_space=pltpu.VMEM)
        anym = pl.BlockSpec(memory_space=pl.ANY)
        bf, f32 = jnp.bfloat16, jnp.float32
        dma = pltpu.SemaphoreType.DMA
        gathered, trans = pl.pallas_call(
            functools.partial(exchange_kernel, dims),
            out_shape=(pltpu.VMEM((patches, 4, columns, total_m, CP), bf),
                       pltpu.VMEM((patches, total_m, total_m), f32)),
            in_specs=[anym, vmem, vmem, vmem, anym, anym],
            out_specs=(vmem, vmem),
            scratch_shapes=[
                pltpu.VMEM((2, channels, columns, rows), bf),
                pltpu.VMEM((members, rows, columns, CP), bf),
                pltpu.VMEM((2, 2, 6, 544, 128), f32),
                pltpu.VMEM((2, 4, 544, 128), f32),
                pltpu.VMEM((members * columns, 2 * CP), bf),
                pltpu.VMEM((2, members * 17, 128), f32),
                pltpu.VMEM((4, columns, members, 128), f32),
                pltpu.VMEM((7, 4, columns, members, 128), bf),
                pltpu.VMEM((6, 50, members, 128), bf),
                pltpu.VMEM((patches * 3, 50, members, 128), bf),
                pltpu.VMEM((8, 2, 4, members, CP), bf),
                pltpu.VMEM((units, 2, 4, members, CP), bf),
                pltpu.VMEM((2 * CP, 512), bf),
                pltpu.VMEM((512, CP), bf),
                pltpu.VMEM((488, 512), f32),
                pltpu.VMEM((8 * CP, CP), bf),
                pltpu.VMEM((2, patches, 4, 1, columns, 32), f32),
                pltpu.VMEM((2, patches, 8, CP), f32),
                pltpu.VMEM((8, total_m, CP), f32),
                pltpu.VMEM((8, total_m, CP), f32),
                pltpu.VMEM((2, total_m, 2 * total_m), f32),
                pltpu.VMEM((2, total_m, 2 * total_m), f32),
                dma((2,)), dma((units, 2)), dma((units, 2)), dma((patches, 3, 4)), dma((patches, 3, 4)), dma((2,)),
            ],
            compiler_params=pltpu.CompilerParams(collective_id=0, has_side_effects=True, vmem_limit_bytes=46 * 1024 * 1024),
        )(ens_state.transpose(0, 3, 2, 1), w_in, w_out.T, obs_op.T, obs_val, obs_wt)
        return pl.pallas_call(
            functools.partial(update_kernel, done),
            out_shape=jax.ShapeDtypeStruct((dev_rows, columns, total_m, channels), bf),
            in_specs=[vmem, vmem],
            out_specs=anym,
            scratch_shapes=[pltpu.VMEM((dev_rows, columns, total_m, channels), bf), dma((dev_rows,))],
            compiler_params=pltpu.CompilerParams(vmem_limit_bytes=24 * 1024 * 1024),
        )(pltpu.with_memory_space_constraint(trans, pltpu.VMEM), pltpu.with_memory_space_constraint(gathered, pltpu.VMEM))

    return jax.shard_map(local_step, mesh=mesh, in_specs=(P("ens", None, "dom", None), P(), P(), P(), obs_spec, obs_spec), out_specs=P("ens", "dom", None, None), check_vma=False)
```

```python
import functools
import math
import jax
import jax.numpy as jnp
from jax import lax
from jax.experimental import pallas as pl
from jax.experimental.pallas import tpu as pltpu
from jax.sharding import PartitionSpec as P

NS_STEPS = 18
MESH = pl.DeviceIdType.MESH
CP = 256
NT = (((1,), (1,)), ((), ()))


NN = (((1,), (0,)), ((), ()))


def gelu(x):
    scale = math.sqrt(2.0 / math.pi)
    return (0.5 * x) * (1.0 + jnp.tanh(x * (scale + (scale * 0.044715) * (x * x))))


def split3(a):
    hi = a.astype(jnp.bfloat16)
    rem = a - hi.astype(jnp.float32)
    mid = rem.astype(jnp.bfloat16)
    low = (rem - mid.astype(jnp.float32)).astype(jnp.bfloat16)
    return hi, mid, low


def f32dot(a, b, dims=NN):
    ah, am, al = split3(a)
    bh, bm, bl = split3(b)
    n = a.shape[0]

    def dot(u, v):
        return lax.dot_general(u, v, dims, preferred_element_type=jnp.float32)
    by_hi = dot(jnp.concatenate([ah, am, al], axis=0), bh)
    by_mid = dot(jnp.concatenate([ah, am], axis=0), bm)
    by_low = dot(ah, bl)
    small = (by_low + by_hi[2 * n:]) + by_mid[n:]
    return (small + (by_mid[:n] + by_hi[n:2 * n])) + by_hi[:n]


def packed_dot(a, b, left, right):
    ah, am, al = split3(a)
    bh, bm, bl = split3(b)
    n = a.shape[0]

    def dot(u, v):
        blocks = jnp.concatenate([v * left, v * right], axis=0)
        return jnp.dot(u, blocks, preferred_element_type=jnp.float32)
    by_hi = dot(jnp.concatenate([ah, am, al], axis=0), bh)
    by_mid = dot(jnp.concatenate([ah, am], axis=0), bm)
    by_low = dot(ah, bl)
    small = (by_low + by_hi[2 * n:]) + by_mid[n:]
    return (small + (by_mid[:n] + by_hi[n:2 * n])) + by_hi[:n]


def stacked(t):
    hi, mid, low = (v.astype(jnp.float32) for v in split3(t))
    return jnp.concatenate([
        jnp.concatenate([hi, mid], axis=1),
        jnp.concatenate([low, jnp.zeros_like(low)], axis=1)], axis=0).astype(jnp.bfloat16)


def transform(lhs, g):
    n = lhs.shape[0] // 2
    res = jnp.dot(lhs, jnp.concatenate([g, g], axis=0), preferred_element_type=jnp.float32)
    return (res[n:] + res[:n]).astype(jnp.bfloat16)


def exchange_kernel(dims, xt_hbm, wi_ref, wo_ref, op_ref, yo_hbm, wt_hbm, gath, tt_ref,
                    xn, xb, xs, xa, xl, ts, t2, sb1, sb2, rb, gsend, grecv, wi, wo, wf, wobs, obs_raw, obs_row, yp, cm, amat, cvec,
                    xsem, gssem, grsem, ssem, rsem, osem):
    members, rows, columns, channels, patches, dev_rows, ens_size, done = dims
    units = patches * ens_size
    total_m = members * ens_size
    me = lax.axis_index("ens")
    mydom = lax.axis_index("dom")
    my_x, my_core = me // 2, me % 2
    mine = pl.ds(pl.multiple_of(me * members, members), members)

    def dest_of(dslot):
        dx = (my_x + 1 - dslot // 2) % 2
        dc = (my_core + (dslot + 1) // 2) % 2
        return dx * 2 + dc

    def x_copy(m):
        return pltpu.make_async_copy(xt_hbm.at[m], xn.at[m % 2], xsem.at[m % 2])

    def ghost_copy(unit):
        return pltpu.make_async_remote_copy(
            src_ref=gsend.at[unit % 8], dst_ref=grecv.at[unit], send_sem=gssem.at[unit], recv_sem=grsem.at[unit],
            device_id={"dom": 1 - mydom}, device_id_type=MESH)

    def pair_copies(patch, dslot, pair):
        dev = {"ens": dest_of(dslot)}
        slot, box = (patch % 2) * 3 + dslot, patch * 3 + dslot
        two, tiles = pl.ds(pair * 2, 2), pl.ds(pair * 25, 25)
        first = pltpu.make_async_remote_copy(
            src_ref=sb1.at[slot, two], dst_ref=gath.at[patch, two, :, mine, pl.ds(0, 128)],
            send_sem=ssem.at[patch, dslot, pair * 2], recv_sem=rsem.at[patch, dslot, pair * 2],
            device_id=dev, device_id_type=MESH)
        second = pltpu.make_async_remote_copy(
            src_ref=sb2.at[slot, tiles], dst_ref=rb.at[box, tiles],
            send_sem=ssem.at[patch, dslot, pair * 2 + 1], recv_sem=rsem.at[patch, dslot, pair * 2 + 1],
            device_id=dev, device_id_type=MESH)
        return first, second

    def wait_sent(patch, dslot):
        for pair in range(2):
            for copy in pair_copies(patch, dslot, pair):
                copy.wait_send()

    obs_copies = [pltpu.make_async_copy(ref.at[pl.ds(me * patches, patches)], obs_raw.at[i], osem.at[i]) for i, ref in enumerate((yo_hbm, wt_hbm))]

    x_copy(0).start()
    x_copy(1).start()
    for copy in obs_copies:
        copy.start()
    barrier = pltpu.get_barrier_semaphore()
    for dslot in range(3):
        pl.semaphore_signal(barrier, inc=1, device_id={"ens": dest_of(dslot)}, device_id_type=MESH)
    pl.semaphore_signal(barrier, inc=1, device_id={"dom": 1 - mydom}, device_id_type=MESH)

    wf[...] = jnp.zeros_like(wf)
    wf[0:channels, :] = wo_ref[...].astype(jnp.float32)
    wo[...] = wf[0:CP, :].T.astype(jnp.bfloat16)
    wf[0:2 * channels, :] = wi_ref[...].astype(jnp.float32)
    keep = lax.broadcasted_iota(jnp.int32, (CP, 512), 0) < channels
    wi[0:CP, :] = jnp.where(keep, wf[0:CP, :], 0.0).astype(jnp.bfloat16)
    wi[CP:2 * CP, :] = wf[channels:channels + CP, :].astype(jnp.bfloat16)
    turn = (lax.broadcasted_iota(jnp.int32, (128, 128), 0) == lax.broadcasted_iota(jnp.int32, (128, 128), 1)).astype(jnp.float32).astype(jnp.bfloat16)

    wide = ([[xs.at[0, h, j] for j in range(4)] for h in range(2)],
            [[xs.at[j // 2, h, 4 + j % 2] for j in range(4)] for h in range(2)])
    turned = ([[xs.at[1, h, j] for j in range(4)] for h in range(2)],
              [[xa.at[h, j] for j in range(4)] for h in range(2)])

    def widen(odd, c):
        wide[odd][c // 128][c // 32 % 4][17 * (c % 32):17 * (c % 32) + 16, :] = xn[odd, c].astype(jnp.float32)

    def turn_column(odd, col):
        part = jnp.concatenate([wide[odd][h][j][pl.ds(col, 32, stride=17), :] for h in range(2) for j in range(4)], axis=0)
        out = lax.dot_general(turn, part.astype(jnp.bfloat16), NT, preferred_element_type=jnp.float32)
        for h in range(2):
            for j in range(4):
                turned[odd][h][j][pl.ds(col, 32, stride=17), :] = out[32 * j:32 * j + 32, h * 128:h * 128 + 128]

    def narrow(odd, m, row):
        for h in range(2):
            xb[m, row, :, h * 128:h * 128 + 128] = turned[odd][h][row // 32][17 * (row % 32):17 * (row % 32) + 16, :].astype(jnp.bfloat16)

    def relayout(t, carry):
        for odd in range(2):
            m = 2 * t + odd

            @pl.when(m + 2 < members)
            def _():
                x_copy(m + 2).start()

            @pl.when(m + 1 < members)
            def _():
                x_copy(m + 1).wait()
            for col in range(columns):
                turn_column(odd, col)
                for row in range(rows * col // columns, rows * (col + 1) // columns):
                    narrow(1 - odd, jnp.maximum(m - 1, 0), row)
            for c in range(channels):
                widen(1 - odd, c)
        return carry
    for ref in (wide[0][1][3], wide[1][1][3]):
        ref[17 * (channels % 32):544, :] = jnp.zeros((544 - 17 * (channels % 32), 128), jnp.float32)
    x_copy(0).wait()
    for c in range(channels):
        widen(0, c)
    lax.fori_loop(0, members // 2, relayout, 0)

    for row in range(rows):
        narrow(1, members - 1, row)
    pl.semaphore_wait(barrier, 4)

    lane = lax.broadcasted_iota(jnp.int32, (members, 128), 1)

    def setup():
        wf[0:128, 0:CP] = jnp.zeros((128, CP), jnp.float32)
        wf[0:32, 0:channels] = op_ref[...].astype(jnp.float32)
        opt = wf[0:128, 0:CP].T.astype(jnp.bfloat16)
        for j in range(8):
            place = (lax.broadcasted_iota(jnp.int32, (128, CP), 1) == lax.broadcasted_iota(jnp.int32, (128, CP), 0) + 32 * j)
            wobs[j * CP:(j + 1) * CP, :] = jnp.dot(opt, place.astype(jnp.bfloat16), preferred_element_type=jnp.float32).astype(jnp.bfloat16)
        for copy in obs_copies:
            copy.wait()
        sub8 = lax.broadcasted_iota(jnp.int32, (8, 128), 0)
        lane8 = lax.broadcasted_iota(jnp.int32, (8, 128), 1) // 32
        wf[0:8, 0:128] = jnp.zeros((8, 128), jnp.float32)

        def rows_of(patch, carry):
            for i in range(2):
                for g in range(8):
                    wf[0:8, 0:32] = obs_raw[i, patch, g % 4, 0, (g // 4) * 8:(g // 4) * 8 + 8, :]
                    v = wf[0:8, 0:128]
                    v = v + pltpu.roll(v, 32, 1)
                    v = v + pltpu.roll(v, 64, 1)
                    for q in range(2):
                        obs_row[i, patch, g:g + 1, q * 128:q * 128 + 128] = jnp.sum(jnp.where(sub8 == lane8 + 4 * q, v, 0.0), axis=0, keepdims=True)
            return carry
        lax.fori_loop(0, patches, rows_of, 0)

    def prepare(unit):
        slot = unit % 2
        patch, dslot = unit // ens_size, unit % ens_size
        first = dest_of(dslot) * dev_rows + patch * 4

        def convert(r, carry):
            row = jnp.minimum(jnp.maximum(first + r - 1, 0), rows - 1)
            for m in range(members):
                for h in range(2):
                    xs[slot, h, r, 33 * m + 8:33 * m + 24, :] = xb[m, row, :, h * 128:h * 128 + 128].astype(jnp.float32)
            return carry
        lax.fori_loop(0, 6, convert, 0)

        @pl.when(unit >= 8)
        def _():
            ghost_copy(unit - 8).wait_send()

        def edges(r, carry):
            for h in range(2):
                gsend[unit % 8, 0, r, :, h * 128:h * 128 + 128] = xs[slot, h, r + 1, pl.ds(23, members, stride=33), :].astype(jnp.bfloat16)
                gsend[unit % 8, 1, r, :, h * 128:h * 128 + 128] = xs[slot, h, r + 1, pl.ds(8, members, stride=33), :].astype(jnp.bfloat16)
            return carry
        lax.fori_loop(0, 4, edges, 0)
        ghost_copy(unit).start()

    def forecast(unit):
        patch, dslot = unit // ens_size, unit % ens_size
        slot = unit % 2
        out_slot = jnp.where(dslot < 3, (patch % 2) * 3 + dslot, 6)

        @pl.when((dslot < 3) & (patch >= 2))
        def _():
            wait_sent(patch - 2, dslot)
        ghost_copy(unit).wait_recv()

        def block(r, carry):
            for h in range(2):
                xs[slot, h, r + 1, pl.ds(7, members, stride=33), :] = grecv[unit, 0, r, :, h * 128:h * 128 + 128].astype(jnp.float32)
                xs[slot, h, r + 1, pl.ds(24, members, stride=33), :] = grecv[unit, 1, r, :, h * 128:h * 128 + 128].astype(jnp.float32)
            for m in range(members):
                b = 33 * m
                for h in range(2):
                    cur = xs[slot, h, r + 1, b + 8:b + 24, :]
                    north = xs[slot, h, r, b + 8:b + 24, :]
                    south = xs[slot, h, r + 2, b + 8:b + 24, :]
                    west = xs[slot, h, r + 1, b + 7:b + 23, :]
                    east = xs[slot, h, r + 1, b + 9:b + 25, :]
                    lap = north + south + west + east - 4.0 * cur
                    xl[16 * m:16 * m + 16, h * 128:h * 128 + 128] = cur.astype(jnp.bfloat16)
                    xl[16 * m:16 * m + 16, CP + h * 128:CP + h * 128 + 128] = lap.astype(jnp.bfloat16)
            hidden = jnp.dot(xl[...], wi[...], preferred_element_type=jnp.float32)
            gel = gelu(hidden).astype(jnp.bfloat16)
            inc = jnp.dot(gel, wo[...], preferred_element_type=jnp.float32)
            for m in range(members):
                for h in range(2):
                    ts[h, 17 * m:17 * m + 16, :] = xs[slot, h, r + 1, 33 * m + 8:33 * m + 24, :] + inc[16 * m:16 * m + 16, h * 128:h * 128 + 128]
            for col in range(columns):
                sb1[out_slot, r, col] = ts[0, pl.ds(col, members, stride=17), :].astype(jnp.bfloat16)
                t2[r, col] = ts[1, pl.ds(col, members, stride=17), :]
            return carry

        def pack(pair):
            left = jnp.zeros((members, 128), jnp.float32)
            for k in range(8):
                r, c0 = pair * 2 + k // 4, (k % 4) * 4
                v = [t2[r, c0 + i] for i in range(4)]
                for i in range(3):
                    sb2[out_slot, pair * 25 + k * 3 + i] = jnp.where(lane < 96, v[i], pltpu.roll(v[3], 96 - 32 * i, 1)).astype(jnp.bfloat16)
                for i in range(4):
                    left = left + pltpu.roll(jnp.where(lane >= 96, v[i], 0.0), (32 + 3 * (4 * k + i)) % 128, 1)
            sb2[out_slot, pair * 25 + 24] = left.astype(jnp.bfloat16)

        def half_unit(pair, carry):
            lax.fori_loop(pair * 2, pair * 2 + 2, block, 0)

            @pl.when(dslot < 3)
            def _():
                pack(pair)
                for copy in pair_copies(patch, dslot, pair):
                    copy.start()

            @pl.when(dslot == 3)
            def _():
                def own(r, c2):
                    for col in range(columns):
                        gath[patch, r, col, mine, 0:128] = sb1[6, r, col]
                        gath[patch, r, col, mine, 128:256] = t2[r, col].astype(jnp.bfloat16)
                    return c2
                lax.fori_loop(pair * 2, pair * 2 + 2, own, 0)
            return carry
        lax.fori_loop(0, 2, half_unit, 0)

    def unpack(patch, dslot):
        src = pl.ds(pl.multiple_of(dest_of(dslot) * members, members), members)
        box = patch * 3 + dslot

        def half(pair, carry):
            for copy in pair_copies(patch, dslot, pair):
                copy.wait_recv()
            left = rb[box, pair * 25 + 24].astype(jnp.float32)
            for k in range(8):
                r, c0 = pair * 2 + k // 4, (k % 4) * 4
                p = [rb[box, pair * 25 + k * 3 + i].astype(jnp.float32) for i in range(3)]
                tail = [jnp.where(lane < 99, pltpu.roll(left, (96 - 3 * (4 * k + i)) % 128, 1), 0.0) for i in range(4)]
                for i in range(3):
                    gath[patch, r, c0 + i, src, 128:256] = jnp.where(lane < 96, p[i], tail[i]).astype(jnp.bfloat16)
                last = jnp.where(lane < 64, jnp.where(lane < 32, pltpu.roll(p[0], 32, 1), pltpu.roll(p[1], 64, 1)),
                                 jnp.where(lane < 96, pltpu.roll(p[2], 96, 1), tail[3]))
                gath[patch, r, c0 + 3, src, 128:256] = last.astype(jnp.bfloat16)
            return carry
        lax.fori_loop(0, 2, half, 0)

    def analysis(patch):
        def arrive(dslot, carry):
            unpack(patch, dslot)
            return carry
        lax.fori_loop(0, 3, lambda i, c: arrive(2 - i, c), 0)
        eye = (lax.broadcasted_iota(jnp.int32, (total_m, total_m), 0) == lax.broadcasted_iota(jnp.int32, (total_m, total_m), 1)).astype(jnp.float32)
        csum = jnp.zeros((total_m, CP), jnp.float32)
        for half in range(2):
            lhs = jnp.concatenate([gath[patch, :, half * 8 + j].reshape(4 * total_m, CP) for j in range(8)], axis=1)
            yb = jnp.dot(lhs, wobs[...], preferred_element_type=jnp.float32)
            for r in range(4):
                g = half * 4 + r
                y = yb[r * total_m:(r + 1) * total_m]
                ybar = jnp.sum(y, axis=0, keepdims=True) * (1.0 / total_m)
                y = y - ybar
                c = y * obs_row[1, patch, g:g + 1, :]
                csum = csum + c * (obs_row[0, patch, g:g + 1, :] - ybar)
                yp[g] = y
                cm[g] = c
        a_mat = (total_m - 1.0) * eye
        for g in range(8):
            a_mat = a_mat + f32dot(cm[g], yp[g], NT)
        amat[patch % 2, :, 0:total_m] = a_mat
        amat[patch % 2, :, total_m:2 * total_m] = a_mat
        cvec[patch % 2] = jnp.broadcast_to(jnp.sum(csum, axis=1, keepdims=True), (total_m, 2 * total_m))

    def solve(patch):
        row = lax.broadcasted_iota(jnp.int32, (total_m, 2 * total_m), 0)
        col = lax.broadcasted_iota(jnp.int32, (total_m, 2 * total_m), 1)
        eye = ((row == col) | (row + total_m == col)).astype(jnp.float32)
        first = col < total_m
        left = first.astype(jnp.float32).astype(jnp.bfloat16)
        right = (col >= total_m).astype(jnp.float32).astype(jnp.bfloat16)
        mats = jnp.where(first, amat[0], amat[1])
        diag = jnp.sum(mats * eye, axis=0, keepdims=True)
        trace = jnp.where(first[0:1], jnp.sum(jnp.where(first[0:1], diag, 0.0), axis=1, keepdims=True),
                          jnp.sum(jnp.where(first[0:1], 0.0, diag), axis=1, keepdims=True))

        def mixer(z, y):
            return 1.5 * eye - 0.5 * packed_dot(z, y, left, right)

        def newton(step, carry):
            y, z = carry
            mix = mixer(z, y)
            return packed_dot(y, mix, left, right), packed_dot(mix, z, left, right)
        scaled = mats / trace
        mix = 1.5 * eye - 0.5 * scaled
        y, z = lax.fori_loop(1, NS_STEPS - 1, newton, (packed_dot(scaled, mix, left, right), mix))
        inv = packed_dot(mixer(z, y), z, left, right)
        root = inv / jnp.sqrt(trace)
        wbar = packed_dot(root, packed_dot(root, jnp.where(first, cvec[0], cvec[1]), left, right), left, right)
        trans = math.sqrt(total_m - 1.0) * root + wbar
        trans = trans + (1.0 - jnp.sum(trans, axis=0, keepdims=True)) * (1.0 / total_m)
        both = trans.T
        tt_ref[patch] = both[0:total_m]
        tt_ref[patch + 1] = both[total_m:2 * total_m]

        @pl.when(patch < done)
        def _():
            def apply(i, carry):
                lhs = stacked(tt_ref[patch + i // 4])
                for c in range(columns):
                    gath[patch + i // 4, i % 4, c] = transform(lhs, gath[patch + i // 4, i % 4, c])
                return carry
            lax.fori_loop(0, 8, apply, 0)

    def step(v, carry):
        @pl.when(v < units)
        def _():
            prepare(v)

        @pl.when((v >= 1) & (v <= units))
        def _():
            forecast(v - 1)

        @pl.when(v == 0)
        def _():
            setup()

        @pl.when(v == units + 1)
        def _():
            for unit in range(units - 8, units):
                ghost_copy(unit).wait_send()

        @pl.when((v >= 12) & (v % 4 == 0))
        def _():
            analysis(v // 4 - 3)

        @pl.when((v >= 12) & (v % 8 == 0))
        def _():
            solve(v // 4 - 4)
        return carry
    lax.fori_loop(0, units + 9, step, 0)

    for patch in range(patches - 2, patches):
        for dslot in range(3):
            wait_sent(patch, dslot)


def update_kernel(done, tt_ref, g_ref, out_hbm, stage, sem):
    channels = out_hbm.shape[3]

    def copy(r):
        return pltpu.make_async_copy(stage.at[r], out_hbm.at[r], sem.at[r])

    def write(r, carry):
        for col in range(stage.shape[1]):
            stage[r, col] = g_ref[r // 4, r % 4, col, :, 0:channels]
        copy(r).start()
        return carry
    lax.fori_loop(0, 4 * done, write, 0)

    def last(r, carry):
        lhs = stacked(tt_ref[r // 4])
        for col in range(stage.shape[1]):
            stage[r, col] = transform(lhs, g_ref[r // 4, r % 4, col])[:, 0:channels]
        copy(r).start()
        return carry
    lax.fori_loop(4 * done, stage.shape[0], last, 0)

    def drain(r, carry):
        copy(r).wait()
        return carry
    lax.fori_loop(0, stage.shape[0], drain, 0)


def solution(mesh):
    ens_size = mesh.shape["ens"]
    obs_spec = P(None, None, "dom", None, None)

    def local_step(ens_state, w_in, w_out, obs_op, obs_val, obs_wt):
        members, rows, columns, channels = ens_state.shape
        total_m = members * ens_size
        dev_rows = rows // ens_size
        patches = dev_rows // 4
        units = patches * ens_size
        done = patches - 2
        dims = (members, rows, columns, channels, patches, dev_rows, ens_size, done)
        vmem = pl.BlockSpec(memory_space=pltpu.VMEM)
        anym = pl.BlockSpec(memory_space=pl.ANY)
        bf, f32 = jnp.bfloat16, jnp.float32
        dma = pltpu.SemaphoreType.DMA
        gathered, trans = pl.pallas_call(
            functools.partial(exchange_kernel, dims),
            out_shape=(pltpu.VMEM((patches, 4, columns, total_m, CP), bf),
                       pltpu.VMEM((patches, total_m, total_m), f32)),
            in_specs=[anym, vmem, vmem, vmem, anym, anym],
            out_specs=(vmem, vmem),
            scratch_shapes=[
                pltpu.VMEM((2, channels, columns, rows), bf),
                pltpu.VMEM((members, rows, columns, CP), bf),
                pltpu.VMEM((2, 2, 6, 544, 128), f32),
                pltpu.VMEM((2, 4, 544, 128), f32),
                pltpu.VMEM((members * columns, 2 * CP), bf),
                pltpu.VMEM((2, members * 17, 128), f32),
                pltpu.VMEM((4, columns, members, 128), f32),
                pltpu.VMEM((7, 4, columns, members, 128), bf),
                pltpu.VMEM((6, 50, members, 128), bf),
                pltpu.VMEM((patches * 3, 50, members, 128), bf),
                pltpu.VMEM((8, 2, 4, members, CP), bf),
                pltpu.VMEM((units, 2, 4, members, CP), bf),
                pltpu.VMEM((2 * CP, 512), bf),
                pltpu.VMEM((512, CP), bf),
                pltpu.VMEM((488, 512), f32),
                pltpu.VMEM((8 * CP, CP), bf),
                pltpu.VMEM((2, patches, 4, 1, columns, 32), f32),
                pltpu.VMEM((2, patches, 8, CP), f32),
                pltpu.VMEM((8, total_m, CP), f32),
                pltpu.VMEM((8, total_m, CP), f32),
                pltpu.VMEM((2, total_m, 2 * total_m), f32),
                pltpu.VMEM((2, total_m, 2 * total_m), f32),
                dma((2,)), dma((units,)), dma((units,)), dma((patches, 3, 4)), dma((patches, 3, 4)), dma((2,)),
            ],
            compiler_params=pltpu.CompilerParams(collective_id=0, has_side_effects=True, vmem_limit_bytes=46 * 1024 * 1024),
        )(ens_state.transpose(0, 3, 2, 1), w_in, w_out.T, obs_op.T, obs_val, obs_wt)
        return pl.pallas_call(
            functools.partial(update_kernel, done),
            out_shape=jax.ShapeDtypeStruct((dev_rows, columns, total_m, channels), bf),
            in_specs=[vmem, vmem],
            out_specs=anym,
            scratch_shapes=[pltpu.VMEM((dev_rows, columns, total_m, channels), bf), dma((dev_rows,))],
            compiler_params=pltpu.CompilerParams(vmem_limit_bytes=24 * 1024 * 1024),
        )(pltpu.with_memory_space_constraint(trans, pltpu.VMEM), pltpu.with_memory_space_constraint(gathered, pltpu.VMEM))

    return jax.shard_map(local_step, mesh=mesh, in_specs=(P("ens", None, "dom", None), P(), P(), P(), obs_spec, obs_spec), out_specs=P("ens", "dom", None, None), check_vma=False)
```
